128 devices in a mesh: row: 8 (over z, core), col: 16 (over y, x).
Axes of the slice: x: 4, y: 4, z: 4, core: 2. Of those that a mesh axis runs over, the one named last changes fastest.
Arguments:
- right_side: float32 [512, 4096], P('row', 'col'), may hold values from -20 to 20
- initial_guess: float32 [512, 4096], P('row', 'col'), may hold values from -3 to 3
- kernel: float32 [31, 31], replicated, may hold values from 0 to 1, as said below
Outputs:
- template: float32 [512, 4096], P('row', 'col')
- residual: float32 [512, 4096], P('row', 'col')
The draws below stay inside these ranges and needn't reach their ends.
Inputs may be any that keep to these rules, and one draw needn't show every extreme that they name: `kernel`: entries are positive and sum to one.
All inputs are finite; a program needn't handle non-finite values.
Results may differ from the reference program's by a relative error of at most 0.0003.
Values sent between devices are 32-bit elements; how exact they have to be, the bound alone decides.
A program may use at most 128 MiB of HBM per device.

```python
import jax
import jax.numpy as jnp

KW = 31
ITERS = 3
NX = 512
NY = 4096


def draw_right_side(key, part):
    rough = jax.random.normal(jax.random.fold_in(key, 11), (NX, NY), jnp.float32)
    column_pos = jnp.arange(NY, dtype=jnp.float32) / max(NY - 1, 1)
    ramp = jnp.exp(jnp.log(3.0) * column_pos)[None, :]
    values = rough * ramp
    return jnp.clip(values, -20.0, 20.0)


def draw_kernel(key, part):
    center = (KW - 1) / 2.0
    offsets = jnp.arange(KW, dtype=jnp.float32) - center
    radius_sq = offsets[:, None] ** 2 + offsets[None, :] ** 2
    profile = jnp.exp(-radius_sq / 98.0)
    factor = jax.random.uniform(jax.random.fold_in(key, 21), (KW, KW), jnp.float32, 0.5, 1.5)
    weights = profile * factor
    return weights / jnp.sum(weights)


def shard_levels(own_key, shape, shards, least, largest):
    def one(position, blocks):
        draws = jax.random.uniform(jax.random.fold_in(jax.random.fold_in(own_key, 6), position), (blocks,), jnp.float32, least / len(shards), largest / len(shards))
        return jnp.repeat(jnp.exp(draws), shape[position] // blocks).reshape((-1,) + (1,) * (len(shape) - position - 1))

    gain = one(*shards[0])
    for cut in shards[1:]:
        gain = gain * one(*cut)
    return gain


def scatter_about(rng, dims, deviation, bound, split=(), kind=jnp.bfloat16):
    level = shard_levels(rng, dims, split, -0.22, 0.18) if split else 1.0
    result = jax.random.normal(rng, dims, jnp.float32) * deviation * level
    return jnp.minimum(jnp.maximum(result, -bound), bound).astype(kind)


def setup_inputs(seed: int = 0) -> dict:
    splits = jax.random.split(jax.random.key(seed), 4)
    return {
        "right_side": draw_right_side(jax.random.fold_in(splits[3], 71), 0),
        "initial_guess": scatter_about(splits[1], (NX, NY), 0.5, 3.0, ((0, 8), (1, 16)), jnp.float32),
        "kernel": draw_kernel(jax.random.fold_in(splits[3], 71), 0),
    }


penalty = 0.05


def convolve(source, taps):
    half_width = taps.shape[0] // 2
    tile_rows, tile_cols = source.shape
    extent = (tile_rows + 2 * half_width, tile_cols + 2 * half_width)
    spectrum = jnp.fft.rfft2(source, s=extent) * jnp.fft.rfft2(taps, s=extent)
    complete = jnp.fft.irfft2(spectrum, s=extent)
    return complete[half_width:half_width + tile_rows, half_width:half_width + tile_cols].astype(source.dtype)


def laplacian(source):
    padded = jnp.pad(source, 1)
    return 4.0 * source - padded[2:, 1:-1] - padded[:-2, 1:-1] - padded[1:-1, 2:] - padded[1:-1, :-2]


def operate(source, kernel):
    blurred = convolve(source, kernel[::-1, ::-1])
    return convolve(blurred, kernel) + penalty * laplacian(source)


def reference(right_side, initial_guess, kernel):
    template = initial_guess
    residual = right_side - operate(template, kernel)
    direction = residual
    norm_now = jnp.sum(residual * residual)
    for iteration in range(ITERS):
        applied = operate(direction, kernel)
        step_size = norm_now / jnp.sum(direction * applied)
        template = template + step_size * direction
        residual = residual - step_size * applied
        norm_next = jnp.sum(residual * residual)
        direction = residual + (norm_next / norm_now) * direction
        norm_now = norm_next
    return template, residual
```

```python
import jax
import jax.numpy as jnp
from jax import lax
from jax.experimental import pallas as pl
from jax.experimental.pallas import tpu as pltpu
from jax.sharding import PartitionSpec as P

PENALTY = 0.05
F32, BF16 = jnp.float32, jnp.bfloat16
B = 16
LANES = B * B
PITCH = 24
ROWS = 13
FLAT = ROWS * PITCH
DIRECTIONS = ((-1, 0), (1, 0), (0, -1), (0, 1), (-1, -1), (-1, 1), (1, -1), (1, 1))
MESH = pl.DeviceIdType.MESH


def iota(shape, dim):
    return lax.broadcasted_iota(jnp.int32, shape, dim)


def roll(x, shift, axis):
    return pltpu.roll(x, shift % x.shape[axis], axis)


def split(x):
    high = x.astype(BF16)
    return high, (x - high.astype(F32)).astype(BF16)


def swap_blocks(x):
    top, bottom = [], []
    for i in range(4):
        upper, lower = x[16 * i : 16 * i + 8], x[16 * i + 8 : 16 * i + 16]
        top += [upper[:, :128], upper[:, 128:]]
        bottom += [lower[:, :128], lower[:, 128:]]
    y = jnp.concatenate(top + bottom, axis=0)
    row, lane = iota(y.shape, 0), iota(y.shape, 1)
    for t in range(3):
        step = 1 << t
        row_bit, lane_bit = (row >> t) & 1, (lane >> (t + 4)) & 1
        from_below = roll(roll(y, -step, 0), B * step, 1)
        from_above = roll(roll(y, step, 0), -B * step, 1)
        y = jnp.where(row_bit == lane_bit, y, jnp.where(row_bit == 0, from_below, from_above))
    return jnp.concatenate([y[:64], y[64:]], axis=1)


def build_weights(kernel_ref, padded_ref, shifted_ref, weights):
    padded_ref[...] = jnp.zeros_like(padded_ref)
    padded_ref[0:31, 0:31] = kernel_ref[...]
    taps = roll(padded_ref[...], 1, 1).T
    taps = taps[0:48]
    high, low = split(taps)
    flip = (iota((48, 48), 0) + iota((48, 48), 1) == 32).astype(F32).astype(BF16)
    flipped = [jnp.dot(flip, part, preferred_element_type=F32).astype(BF16) for part in (high, low)]
    lane_block = iota((128, 1024), 1) // B
    tap_row = iota((128, 1024), 0)
    spread = (tap_row == 46 - lane_block).astype(F32).astype(BF16)
    spread_flipped = (tap_row == lane_block - 16).astype(F32).astype(BF16)
    for number, (parts, selector) in enumerate((((high, low), spread), (tuple(flipped), spread_flipped))):
        base = jnp.dot(jnp.concatenate(parts, axis=0), selector, preferred_element_type=F32)
        column = iota(base.shape, 1) % B
        for t in range(4):
            base = jnp.where((column >> t) & 1 == 1, roll(base, 1 << t, 0), base)
        for shift in range(8):
            shifted_ref[shift] = roll(base, -B * shift, 1).astype(BF16)
        for part in range(2):
            weight = weights[2 * number + part]
            for di in (-1, 0, 1):
                for r in range(B):
                    start = 31 - 16 * di - r
                    lanes = 128 * (start // 8)
                    for dj in range(3):
                        rows = 48 * part + 16 * dj
                        weight[
                            LANES * (di + 1) + B * r : LANES * (di + 1) + B * r + B,
                            LANES * dj : LANES * dj + LANES,
                        ] = shifted_ref[start % 8, rows : rows + 16, lanes : lanes + LANES]


def correlate(source, high_weight, low_weight, first, count):
    highs, lows = [], []
    for di in (-1, 0, 1):
        high, low = split(source[pl.ds(first + PITCH * di, count), :])
        highs.append(high)
        lows.append(low)
    left = jnp.concatenate(highs + lows + highs, axis=1)
    right = jnp.concatenate([high_weight[...], high_weight[...], low_weight[...]], axis=0)
    y = jnp.dot(left, right, preferred_element_type=F32)
    return y[:, LANES : 2 * LANES] + roll(y[:, :LANES], 1, 0) + roll(y[:, 2 * LANES :], -1, 0)


def smooth(source, first, count):
    x = source[pl.ds(first, count), :]
    above = source[pl.ds(first - PITCH, count), :]
    below = source[pl.ds(first + PITCH, count), :]
    wide = source[pl.ds(first - 8, count + 16), :]
    before = roll(wide, 1, 0)[8 : 8 + count]
    after = roll(wide, -1, 0)[8 : 8 + count]
    lane = iota(x.shape, 1)
    column = lane % B
    upper = roll(jnp.where(lane >= LANES - B, above, x), B, 1)
    lower = roll(jnp.where(lane < B, below, x), -B, 1)
    leftward = jnp.where(column == 0, roll(before, -(B - 1), 1), roll(x, 1, 1))
    rightward = jnp.where(column == B - 1, roll(after, B - 1, 1), roll(x, -1, 1))
    return PENALTY * (4.0 * x - upper - lower - leftward - rightward)


def own(value, first):
    return jnp.concatenate(
        [value[PITCH * r + 8 - first : PITCH * r + 24 - first] for r in range(4, 8)], axis=0
    )


def pack_sides(middle, left_ref, right_ref):
    sublane = iota((8, LANES), 0)
    for pair in range(2):
        first, second = 4 + 2 * pair, 5 + 2 * pair
        left_ref[pair] = jnp.where(sublane < 4, middle[first, 0:8], roll(middle[second, 0:8], 4, 0))
        right_ref[pair] = jnp.where(sublane < 4, roll(middle[first, 8:16], 4, 0), middle[second, 8:16])


def unpack(middle, from_left, from_right, flat, masked):
    sublane = iota((8, LANES), 0)
    for r in range(ROWS):
        right = jnp.zeros((8, LANES), F32)
        left = right
        if r >= 1:
            right = from_right[(r - 1) // 2]
            if (r - 1) % 2:
                right = roll(right, 4, 0)
        if r < 12:
            left = from_left[r // 2]
            if r % 2 == 0:
                left = roll(left, 4, 0)
        start = PITCH * r
        flat[start : start + 8] = masked(jnp.where(sublane < 4, right, left), start, 8)
        if r < 12:
            flat[start + 8 : start + 24] = masked(middle[r], start + 8, 16)
        else:
            flat[start + 8 : start + 24] = jnp.zeros((16, LANES), F32)


def image_kernel(
    grid, b_ref, guess_ref, kernel_ref, template_ref, residual_ref,
    x_mid, v_mid, b_mid, x_left, x_right, v_left, v_right, b_left, b_right,
    x_from_left, x_from_right, v_from_left, v_from_right, b_from_left, b_from_right,
    xf, vf, bf, rf, t1, t2, mask_ref, padded_ref, shifted_ref, k_high, k_low, kt_high, kt_low,
    r0_own, v1_own, kr0_own, kv1_own, lr0_own, lv1_own,
    first_slots, second_slots,
    x_send, x_recv, b_send, b_recv, v_send, v_recv, first_send, first_recv, second_send, second_recv,
):
    n_rows, n_cols = grid
    row, col = lax.axis_index("row"), lax.axis_index("col")

    def at(dr, dc):
        return lax.rem(row + dr + n_rows, n_rows), lax.rem(col + dc + n_cols, n_cols)

    barrier = pltpu.get_barrier_semaphore()
    partners = [at(d, 0) for d in range(1, n_rows)] + [at(0, d) for d in range(1, n_cols)]
    partners += [at(dr, dc) for dr, dc in DIRECTIONS[4:]]
    for partner in partners:
        pl.semaphore_signal(barrier, inc=1, device_id=partner, device_id_type=MESH)

    def remote(source, target, send, recv, device):
        return pltpu.make_async_remote_copy(
            src_ref=source, dst_ref=target, send_sem=send, recv_sem=recv, device_id=device, device_id_type=MESH
        )

    def field_copies(middle, left, right, from_left, from_right, send, recv):
        copies = []
        for number, (dr, dc) in enumerate(DIRECTIONS):
            if dc == 0:
                source = middle.at[pl.ds(4, 4)]
                target = middle.at[pl.ds(4 - 4 * dr, 4)]
            else:
                source = right if dc == 1 else left
                target = (from_left if dc == 1 else from_right).at[pl.ds(2 - 2 * dr, 2)]
            copies.append(remote(source, target, send.at[number], recv.at[number], at(dr, dc)))
        return copies

    def spread(middle, first, x):
        for i in range(4):
            middle[first + i] = x[16 * i : 16 * i + 16]

    spread(x_mid, 4, swap_blocks(guess_ref[...]))
    pack_sides(x_mid, x_left, x_right)
    spread(b_mid, 2, swap_blocks(b_ref[...]))
    sublane = iota((8, LANES), 0)
    left_part = right_part = jnp.zeros((8, LANES), F32)
    for i in range(4):
        here = sublane // 2 == i
        left_part = jnp.where(here, roll(b_mid[2 + i, 0:8], 2 * i, 0), left_part)
        right_part = jnp.where(here, roll(b_mid[2 + i, 8:16], 2 * i + 2, 0), right_part)
    b_left[...] = left_part
    b_right[...] = right_part

    pl.semaphore_wait(barrier, n_rows - 1 + n_cols - 1 + 4)

    x_copies = field_copies(x_mid, x_left, x_right, x_from_left, x_from_right, x_send, x_recv)
    b_copies = []
    for number, (dr, dc) in enumerate(DIRECTIONS):
        if dc == 0:
            source = b_mid.at[pl.ds(2 if dr == -1 else 4, 2)]
            target = b_mid.at[pl.ds(6 if dr == -1 else 0, 2)]
        else:
            source = b_right if dc == 1 else b_left
            target = (b_from_left if dc == 1 else b_from_right).at[1 - dr]
        b_copies.append(remote(source, target, b_send.at[number], b_recv.at[number], at(dr, dc)))
    for copy in x_copies + b_copies:
        copy.start()

    build_weights(kernel_ref, padded_ref, shifted_ref, (k_high, k_low, kt_high, kt_low))
    flat = iota((FLAT, LANES), 0)
    slot = flat % PITCH
    block_row = row * 4 + flat // PITCH - 4 - (slot < 4).astype(jnp.int32)
    block_col = col * 16 + slot - 8 + 24 * (slot < 4).astype(jnp.int32)
    inside = (block_row >= 0) & (block_row < 4 * n_rows) & (block_col >= 0) & (block_col < 16 * n_cols)
    mask_ref[...] = inside.astype(F32)

    def masked(value, first, count):
        return jnp.where(mask_ref[pl.ds(first, count), :] > 0.5, value, 0.0)

    def apply_twice(source, second):
        t1[pl.ds(24, 256), :] = masked(correlate(source, k_high, k_low, 24, 256), 24, 256)
        blurred_source = own(t1[pl.ds(96, 112), :], 96)
        smooth_source = smooth(source, 48, 208)
        applied = correlate(t1, kt_high, kt_low, 48, 208) + smooth_source
        second[pl.ds(48, 208), :] = masked(bf[pl.ds(48, 208), :] - applied if source is xf else applied, 48, 208)
        blurred = correlate(second, k_high, k_low, 72, 160)
        t2[pl.ds(72, 160), :] = masked(blurred, 72, 160)
        return blurred_source, own(smooth_source, 48), own(blurred, 72), own(smooth(second, 96, 112), 96)

    for copy in x_copies:
        copy.wait_recv()
    unpack(x_mid, x_from_left, x_from_right, xf, masked)
    for copy in b_copies:
        copy.wait_recv()
    for r in range(2, 11):
        right = left = jnp.zeros((8, LANES), F32)
        if r >= 3:
            right = roll(b_from_right[(r - 1) // 4], -2 * ((r - 1) % 4), 0)
        if r < 10:
            left = roll(b_from_left[r // 4], 6 - 2 * (r % 4), 0)
        bf[PITCH * r : PITCH * r + 8] = jnp.where(sublane < 4, right, left)
        if r < 10:
            bf[PITCH * r + 8 : PITCH * r + 24] = b_mid[r - 2]

    _, _, kr0, lr0 = apply_twice(xf, rf)
    v1 = own(correlate(t2, kt_high, kt_low, 96, 112), 96) + lr0
    spread(v_mid, 4, v1)
    pack_sides(v_mid, v_left, v_right)
    v_copies = field_copies(v_mid, v_left, v_right, v_from_left, v_from_right, v_send, v_recv)
    for copy in v_copies:
        copy.start()
    r0_own[...] = own(rf[pl.ds(96, 112), :], 96)
    v1_own[...] = v1
    kr0_own[...] = kr0
    lr0_own[...] = lr0

    for copy in v_copies:
        copy.wait_recv()
    unpack(v_mid, v_from_left, v_from_right, vf, masked)
    kv1, lv1, kv2, lv2 = apply_twice(vf, rf)
    v2 = own(rf[pl.ds(96, 112), :], 96)

    def powers(zero, one, two):
        return two, one - two, zero - 2.0 * one + two

    r0, v1 = r0_own[...], v1_own[...]
    p = powers(r0, v1, v2)
    kp = powers(kr0_own[...], kv1, kv2)
    lp = powers(lr0_own[...], lv1, lv2)

    def lanes_of(x):
        total = x[0:8]
        for i in range(1, 8):
            total = total + x[8 * i : 8 * i + 8]
        total = total[:, :128] + total[:, 128:]
        return jnp.sum(total, axis=0, keepdims=True)

    moments = [lanes_of(p[2] * p[2])]
    for i, j in ((2, 2), (1, 2), (1, 1), (0, 1), (0, 0)):
        moments.append(lanes_of(kp[i] * kp[j] + p[i] * lp[j]))
    slot8 = iota((8, 128), 0)
    packed = jnp.zeros((8, 128), F32)
    for i, moment in enumerate(moments):
        packed = jnp.where(slot8 == i, moment, packed)

    def gather(slots, me, count, target, send, recv):
        return [
            remote(slots.at[me], slots.at[me], send.at[d - 1], recv.at[d - 1], target(d)) for d in range(1, count)
        ]

    first_slots[row] = packed
    first_copies = gather(first_slots, row, n_rows, lambda d: at(d, 0), first_send, first_recv)
    for copy in first_copies:
        copy.start()
    v3 = own(correlate(t2, kt_high, kt_low, 96, 112), 96) + lv2
    ap = powers(v1, v2, v3)
    for copy in first_copies:
        copy.wait_recv()
    total = first_slots[0]
    for i in range(1, n_rows):
        total = total + first_slots[i]
    second_slots[col] = total
    second_copies = gather(second_slots, col, n_cols, lambda d: at(0, d), second_send, second_recv)
    for copy in second_copies:
        copy.start()
    for copy in second_copies:
        copy.wait_recv()
    total = second_slots[0]
    for i in range(1, n_cols):
        total = total + second_slots[i]
    total = jnp.sum(total, axis=1, keepdims=True)
    b0, c1, c2, c3, c4, c5 = [total[i : i + 1, :] for i in range(6)]
    c = (None, c1, c2, c3, c4, c5)
    b = (b0, c1 + c2, c2 + c3, c3 + c4, c4 + c5)

    def square(q, m, base):
        return (
            q[0] * q[0] * m[base]
            + 2.0 * (q[0] * q[1]) * m[base + 1]
            + (q[1] * q[1] + 2.0 * (q[0] * q[2])) * m[base + 2]
            + 2.0 * (q[1] * q[2]) * m[base + 3]
            + q[2] * q[2] * m[base + 4]
        )

    def raised(q):
        return q[0], q[0] + q[1], q[1]

    one = (1.0, 2.0, 1.0)
    norm = square(one, b, 0)
    alpha0 = norm / square(one, c, 1)
    r1 = (1.0, 1.0 - alpha0)
    following = square(raised(r1), b, 0)
    beta0 = following / norm
    norm = following
    p1 = (r1[0] + beta0, r1[1] + beta0)
    p1_raised = raised(p1)
    alpha1 = norm / square(p1_raised, c, 1)
    r1_raised = raised(r1)
    r2 = (r1_raised[0], r1_raised[1] - alpha1 * p1[0], r1_raised[2] - alpha1 * p1[1])
    following = square(r2, b, 0)
    beta1 = following / norm
    p2 = tuple(r2[i] + beta1 * p1_raised[i] for i in range(3))
    alpha2 = following / square(p2, c, 1)
    steps = [alpha0 * one[i] + alpha1 * p1_raised[i] + alpha2 * p2[i] for i in range(3)]

    template = own(xf[pl.ds(96, 112), :], 96) + steps[0] * p[2] + steps[1] * p[1] + steps[2] * p[0]
    residual = r2[0] * p[2] + r2[1] * p[1] + r2[2] * p[0]
    residual = residual - alpha2 * (p2[0] * ap[2] + p2[1] * ap[1] + p2[2] * ap[0])
    template_ref[...] = swap_blocks(template)
    residual_ref[...] = swap_blocks(residual)
    for copy in x_copies + b_copies + v_copies + first_copies + second_copies:
        copy.wait_send()


def on_device(grid, right_side, initial_guess, kernel):
    n_rows, n_cols = grid
    middle = pltpu.VMEM((12, 16, LANES), F32)
    b_middle = pltpu.VMEM((8, 16, LANES), F32)
    side = pltpu.VMEM((2, 8, LANES), F32)
    halo = pltpu.VMEM((6, 8, LANES), F32)
    b_side = pltpu.VMEM((8, LANES), F32)
    b_halo = pltpu.VMEM((3, 8, LANES), F32)
    flat = pltpu.VMEM((FLAT, LANES), F32)
    weight = pltpu.VMEM((3 * LANES, 3 * LANES), BF16)
    tile = pltpu.VMEM((64, LANES), F32)
    dma = pltpu.SemaphoreType.DMA
    shape = jax.ShapeDtypeStruct((64, LANES), F32)
    vmem = pl.BlockSpec(memory_space=pltpu.VMEM)

    def body(*refs):
        image_kernel(grid, *refs)

    return pl.pallas_call(
        body,
        out_shape=(shape, shape),
        in_specs=[vmem] * 3,
        out_specs=(vmem, vmem),
        scratch_shapes=[
            middle, middle, b_middle, side, side, side, side, b_side, b_side,
            halo, halo, halo, halo, b_halo, b_halo,
            flat, flat, flat, flat, flat, flat, flat,
            pltpu.VMEM((128, 128), F32), pltpu.VMEM((8, 96, 1024), BF16),
            weight, weight, weight, weight,
            tile, tile, tile, tile, tile, tile,
            pltpu.VMEM((n_rows, 8, 128), F32), pltpu.VMEM((n_cols, 8, 128), F32),
            dma((8,)), dma((8,)), dma((8,)), dma((8,)), dma((8,)), dma((8,)),
            dma((n_rows - 1,)), dma((n_rows - 1,)), dma((n_cols - 1,)), dma((n_cols - 1,)),
        ],
        compiler_params=pltpu.CompilerParams(
            collective_id=0, has_side_effects=True, vmem_limit_bytes=48 * 1024 * 1024
        ),
    )(right_side, initial_guess, kernel)


def solution(mesh):
    grid = (mesh.shape["row"], mesh.shape["col"])
    tiles = P("row", "col")
    return jax.shard_map(
        lambda *arrays: on_device(grid, *arrays),
        mesh=mesh,
        in_specs=(tiles, tiles, P()),
        out_specs=(tiles, tiles),
        check_vma=False,
    )
```

```python
import jax
import jax.numpy as jnp
from jax import lax
from jax.experimental import pallas as pl
from jax.experimental.pallas import tpu as pltpu
from jax.sharding import PartitionSpec as P

PENALTY = 0.05
F32, BF16 = jnp.float32, jnp.bfloat16
B = 16
LANES = B * B
PITCH = 24
ROWS = 13
FLAT = ROWS * PITCH
DIRECTIONS = ((-1, 0), (1, 0), (0, -1), (0, 1), (-1, -1), (-1, 1), (1, -1), (1, 1))
MESH = pl.DeviceIdType.MESH


def iota(shape, dim):
    return lax.broadcasted_iota(jnp.int32, shape, dim)


def roll(x, shift, axis):
    return pltpu.roll(x, shift % x.shape[axis], axis)


def rounded(x):
    return x.astype(BF16).astype(F32)


def put(pair, first, value):
    rows = pl.ds(first, value.shape[0])
    pair[0][rows, :] = value
    pair[1][rows, :] = value - rounded(value)


def swap_blocks(x):
    top, bottom = [], []
    for i in range(4):
        upper, lower = x[16 * i : 16 * i + 8], x[16 * i + 8 : 16 * i + 16]
        top += [upper[:, :128], upper[:, 128:]]
        bottom += [lower[:, :128], lower[:, 128:]]
    y = jnp.concatenate(top + bottom, axis=0)
    row, lane = iota(y.shape, 0), iota(y.shape, 1)
    for t in range(3):
        step = 1 << t
        row_bit, lane_bit = (row >> t) & 1, (lane >> (t + 4)) & 1
        from_below = roll(roll(y, -step, 0), B * step, 1)
        from_above = roll(roll(y, step, 0), -B * step, 1)
        y = jnp.where(row_bit == lane_bit, y, jnp.where(row_bit == 0, from_below, from_above))
    return jnp.concatenate([y[:64], y[64:]], axis=1)


def pick_lanes(x, lanes):
    return jnp.take_along_axis(x, lanes, axis=1, mode="promise_in_bounds")


def build_weights(taps_ref, shifted_ref, weights):
    taps = taps_ref[...]
    lane = iota((128, 128), 1)
    empty = (lane < 1) | (lane > 31)
    ahead = jnp.where(empty, 0.0, roll(taps, 1, 1)).T[0:48]
    flipped = jnp.where(empty, 0.0, pick_lanes(taps, jnp.clip(31 - lane, 0, 127))).T[0:48]
    group = iota((48, 128), 1) // B
    for number, source in enumerate((ahead, flipped)):
        pieces = []
        for tile in range(8):
            block = 8 * tile + group
            wanted = 46 - block if number == 0 else block - 16
            valid = (wanted >= 0) & (wanted <= 30)
            pieces.append(jnp.where(valid, pick_lanes(source, jnp.clip(wanted, 0, 30)), 0.0))
        base = jnp.concatenate(pieces, axis=1)
        column = iota(base.shape, 1) % B
        for t in range(4):
            base = jnp.where((column >> t) & 1 == 1, roll(base, 1 << t, 0), base)
        for shift in range(8):
            moved = roll(base, -B * shift, 1)
            high = moved.astype(BF16)
            shifted_ref[shift, 0:48] = high
            shifted_ref[shift, 48:96] = (moved - high.astype(F32)).astype(BF16)
        for part in range(2):
            weight = weights[2 * number + part]
            for di in (-1, 0, 1):
                for r in range(B):
                    start = 31 - 16 * di - r
                    lanes = 128 * (start // 8)
                    for dj in range(3):
                        rows = 48 * part + 16 * dj
                        weight[
                            LANES * (di + 1) + B * r : LANES * (di + 1) + B * r + B,
                            LANES * dj : LANES * dj + LANES,
                        ] = shifted_ref[start % 8, rows : rows + 16, lanes : lanes + LANES]


FIRST_UNIT = [(di, 0, low) for low in (False, True) for di in (-1, 0, 1)] + [(-1, -1, False), (0, -1, False)]
SECOND_UNIT = [(di, 1, low) for low in (False, True) for di in (-1, 0, 1)]
SECOND_UNIT += [(1, -1, False), (-1, -1, True), (0, -1, True), (1, -1, True)]


def correlate(field, high_weight, low_weight, first, count):
    def body(middle, right, left0, left1):
        queues = []
        for unit, products in enumerate((FIRST_UNIT, SECOND_UNIT)):
            queue = []
            for number, (di, dj, low) in enumerate(products):
                queue.append((unit, number % 2, di, dj, low, ((left0, left1)[unit], middle, right)[dj + 1]))
            queues.append(queue)
        for step in range(max(map(len, queues))):
            for queue in queues:
                if step < len(queue):
                    unit, register, di, dj, low, total = queue[step]
                    weight = low_weight if low else high_weight
                    tile = weight[LANES * (di + 1) : LANES * (di + 2), LANES * (dj + 1) : LANES * (dj + 2)]
                    pltpu.matmul_push_rhs(tile, staging_register=register, mxu_index=unit)
                    rows = pl.ds(first + PITCH * di, count)
                    pltpu.matmul_acc_lhs(total, field[0][rows, :], load_staged_rhs=register)
                    if not low:
                        pltpu.matmul_acc_lhs(total, field[1][rows, :])
        value = pltpu.matmul_pop(middle) + roll(pltpu.matmul_pop(right), -1, 0)
        return value + roll(pltpu.matmul_pop(left0) + pltpu.matmul_pop(left1), 1, 0)

    totals = [pltpu.ACC(unit)((count, LANES), F32) for unit in (0, 1, 0, 1)]
    return pl.run_scoped(body, *totals)


def smooth(source, first, count):
    x = source[pl.ds(first, count), :]
    above = source[pl.ds(first - PITCH, count), :]
    below = source[pl.ds(first + PITCH, count), :]
    wide = source[pl.ds(first - 8, count + 16), :]
    before = roll(wide, 1, 0)[8 : 8 + count]
    after = roll(wide, -1, 0)[8 : 8 + count]
    lane = iota(x.shape, 1)
    column = lane % B
    upper = roll(jnp.where(lane >= LANES - B, above, x), B, 1)
    lower = roll(jnp.where(lane < B, below, x), -B, 1)
    leftward = jnp.where(column == 0, roll(before, -(B - 1), 1), roll(x, 1, 1))
    rightward = jnp.where(column == B - 1, roll(after, B - 1, 1), roll(x, -1, 1))
    return PENALTY * (4.0 * x - upper - lower - leftward - rightward)


def own(value, first):
    return jnp.concatenate(
        [value[PITCH * r + 8 - first : PITCH * r + 24 - first] for r in range(4, 8)], axis=0
    )


def pack_sides(middle, left_ref, right_ref):
    sublane = iota((8, LANES), 0)
    for pair in range(2):
        first, second = 4 + 2 * pair, 5 + 2 * pair
        left_ref[pair] = jnp.where(sublane < 4, middle[first, 0:8], roll(middle[second, 0:8], 4, 0))
        right_ref[pair] = jnp.where(sublane < 4, roll(middle[first, 8:16], 4, 0), middle[second, 8:16])


def unpack(middle, from_left, from_right, flat, masked):
    sublane = iota((8, LANES), 0)
    for r in range(ROWS):
        right = jnp.zeros((8, LANES), F32)
        left = right
        if r >= 1:
            right = from_right[(r - 1) // 2]
            if (r - 1) % 2:
                right = roll(right, 4, 0)
        if r < 12:
            left = from_left[r // 2]
            if r % 2 == 0:
                left = roll(left, 4, 0)
        start = PITCH * r
        put(flat, start, masked(jnp.where(sublane < 4, right, left), start, 8))
        if r < 12:
            put(flat, start + 8, masked(middle[r], start + 8, 16))
        else:
            put(flat, start + 8, jnp.zeros((16, LANES), F32))


def image_kernel(
    grid, b_ref, guess_ref, kernel_ref, template_ref, residual_ref,
    x_mid, v_mid, b_mid, x_left, x_right, v_left, v_right, b_left, b_right,
    x_from_left, x_from_right, v_from_left, v_from_right, b_from_left, b_from_right,
    xf, xf_low, vf, vf_low, bf, rf, rf_low, t1, t1_low, t2, t2_low, mask_ref, taps_ref, shifted_ref, k_high, k_low, kt_high, kt_low,
    r0_own, v1_own, kr0_own, kv1_own, lr0_own, lv1_own,
    first_slots, second_slots, guess_tile, b_tile, taps_in, in_sems,
    x_send, x_recv, b_send, b_recv, v_send, v_recv, first_send, first_recv, second_send, second_recv,
):
    n_rows, n_cols = grid
    loads = (
        pltpu.make_async_copy(guess_ref, guess_tile, in_sems.at[0]),
        pltpu.make_async_copy(b_ref, b_tile, in_sems.at[1]),
        pltpu.make_async_copy(kernel_ref, taps_in, in_sems.at[2]),
    )
    row, col = lax.axis_index("row"), lax.axis_index("col")

    def at(dr, dc):
        return lax.rem(row + dr + n_rows, n_rows), lax.rem(col + dc + n_cols, n_cols)

    barrier = pltpu.get_barrier_semaphore()
    partners = [at(d, 0) for d in range(1, n_rows)] + [at(0, d) for d in range(1, n_cols)]
    partners += [at(dr, dc) for dr, dc in DIRECTIONS[4:]]
    for partner in partners:
        pl.semaphore_signal(barrier, inc=1, device_id=partner, device_id_type=MESH)

    taps_ref[...] = jnp.zeros_like(taps_ref)
    for load in loads:
        load.start()

    def remote(source, target, send, recv, device):
        return pltpu.make_async_remote_copy(
            src_ref=source, dst_ref=target, send_sem=send, recv_sem=recv, device_id=device, device_id_type=MESH
        )

    def field_copies(middle, left, right, from_left, from_right, send, recv):
        copies = []
        for number, (dr, dc) in enumerate(DIRECTIONS):
            if dc == 0:
                source = middle.at[pl.ds(4, 4)]
                target = middle.at[pl.ds(4 - 4 * dr, 4)]
            else:
                source = right if dc == 1 else left
                target = (from_left if dc == 1 else from_right).at[pl.ds(2 - 2 * dr, 2)]
            copies.append(remote(source, target, send.at[number], recv.at[number], at(dr, dc)))
        return copies

    def spread(middle, first, x):
        for i in range(4):
            middle[first + i] = x[16 * i : 16 * i + 16]

    loads[0].wait()
    spread(x_mid, 4, swap_blocks(guess_tile[...]))
    pack_sides(x_mid, x_left, x_right)
    loads[1].wait()
    spread(b_mid, 2, swap_blocks(b_tile[...]))
    sublane = iota((8, LANES), 0)
    left_part = right_part = jnp.zeros((8, LANES), F32)
    for i in range(4):
        here = sublane // 2 == i
        left_part = jnp.where(here, roll(b_mid[2 + i, 0:8], 2 * i, 0), left_part)
        right_part = jnp.where(here, roll(b_mid[2 + i, 8:16], 2 * i + 2, 0), right_part)
    b_left[...] = left_part
    b_right[...] = right_part

    pl.semaphore_wait(barrier, n_rows - 1 + n_cols - 1 + 4)

    x_copies = field_copies(x_mid, x_left, x_right, x_from_left, x_from_right, x_send, x_recv)
    b_copies = []
    for number, (dr, dc) in enumerate(DIRECTIONS):
        if dc == 0:
            source = b_mid.at[pl.ds(2 if dr == -1 else 4, 2)]
            target = b_mid.at[pl.ds(6 if dr == -1 else 0, 2)]
        else:
            source = b_right if dc == 1 else b_left
            target = (b_from_left if dc == 1 else b_from_right).at[1 - dr]
        b_copies.append(remote(source, target, b_send.at[number], b_recv.at[number], at(dr, dc)))
    for copy in x_copies + b_copies:
        copy.start()

    loads[2].wait()
    taps_ref[0:31, 0:31] = taps_in[...]
    build_weights(taps_ref, shifted_ref, (k_high, k_low, kt_high, kt_low))
    flat = iota((FLAT, LANES), 0)
    slot = flat % PITCH
    block_row = row * 4 + flat // PITCH - 4 - (slot < 4).astype(jnp.int32)
    block_col = col * 16 + slot - 8 + 24 * (slot < 4).astype(jnp.int32)
    inside = (block_row >= 0) & (block_row < 4 * n_rows) & (block_col >= 0) & (block_col < 16 * n_cols)
    mask_ref[...] = inside.astype(F32)

    def masked(value, first, count):
        return jnp.where(mask_ref[pl.ds(first, count), :] > 0.5, value, 0.0)

    def apply_twice(source, second):
        put((t1, t1_low), 24, masked(correlate(source, k_high, k_low, 24, 256), 24, 256))
        blurred_source = own(t1[pl.ds(96, 112), :], 96)
        smooth_source = smooth(source[0], 48, 208)
        applied = correlate((t1, t1_low), kt_high, kt_low, 48, 208) + smooth_source
        put(second, 48, masked(bf[pl.ds(48, 208), :] - applied if source[0] is xf else applied, 48, 208))
        blurred = masked(correlate(second, k_high, k_low, 72, 160), 72, 160)
        put((t2, t2_low), 72, blurred)
        return blurred_source, own(smooth_source, 48), own(blurred, 72), own(smooth(second[0], 96, 112), 96)

    for copy in x_copies:
        copy.wait_recv()
    unpack(x_mid, x_from_left, x_from_right, (xf, xf_low), masked)
    for copy in b_copies:
        copy.wait_recv()
    for r in range(2, 11):
        right = left = jnp.zeros((8, LANES), F32)
        if r >= 3:
            right = roll(b_from_right[(r - 1) // 4], -2 * ((r - 1) % 4), 0)
        if r < 10:
            left = roll(b_from_left[r // 4], 6 - 2 * (r % 4), 0)
        bf[PITCH * r : PITCH * r + 8] = jnp.where(sublane < 4, right, left)
        if r < 10:
            bf[PITCH * r + 8 : PITCH * r + 24] = b_mid[r - 2]

    _, _, kr0, lr0 = apply_twice((xf, xf_low), (rf, rf_low))
    v1 = own(correlate((t2, t2_low), kt_high, kt_low, 96, 112), 96) + lr0
    spread(v_mid, 4, v1)
    pack_sides(v_mid, v_left, v_right)
    v_copies = field_copies(v_mid, v_left, v_right, v_from_left, v_from_right, v_send, v_recv)
    for copy in v_copies:
        copy.start()
    r0_own[...] = own(rf[pl.ds(96, 112), :], 96)
    v1_own[...] = v1
    kr0_own[...] = kr0
    lr0_own[...] = lr0

    for copy in v_copies:
        copy.wait_recv()
    unpack(v_mid, v_from_left, v_from_right, (vf, vf_low), masked)
    kv1, lv1, kv2, lv2 = apply_twice((vf, vf_low), (rf, rf_low))
    v2 = own(rf[pl.ds(96, 112), :], 96)

    def powers(zero, one, two):
        return two, one - two, zero - 2.0 * one + two

    r0, v1 = r0_own[...], v1_own[...]
    p = powers(r0, v1, v2)
    kp = powers(kr0_own[...], kv1, kv2)
    lp = powers(lr0_own[...], lv1, lv2)

    def lanes_of(x):
        total = x[0:8]
        for i in range(1, 8):
            total = total + x[8 * i : 8 * i + 8]
        total = total[:, :128] + total[:, 128:]
        return jnp.sum(total, axis=0, keepdims=True)

    moments = [lanes_of(p[2] * p[2])]
    for i, j in ((2, 2), (1, 2), (1, 1), (0, 1), (0, 0)):
        moments.append(lanes_of(kp[i] * kp[j] + p[i] * lp[j]))
    slot8 = iota((8, 128), 0)
    packed = jnp.zeros((8, 128), F32)
    for i, moment in enumerate(moments):
        packed = jnp.where(slot8 == i, moment, packed)

    def gather(slots, me, count, target, send, recv):
        return [
            remote(slots.at[me], slots.at[me], send.at[d - 1], recv.at[d - 1], target(d)) for d in range(1, count)
        ]

    first_slots[row] = packed
    first_copies = gather(first_slots, row, n_rows, lambda d: at(d, 0), first_send, first_recv)
    for copy in first_copies:
        copy.start()
    v3 = own(correlate((t2, t2_low), kt_high, kt_low, 96, 112), 96) + lv2
    ap = powers(v1, v2, v3)
    for copy in first_copies:
        copy.wait_recv()
    total = first_slots[0]
    for i in range(1, n_rows):
        total = total + first_slots[i]
    second_slots[col] = total
    second_copies = gather(second_slots, col, n_cols, lambda d: at(0, d), second_send, second_recv)
    for copy in second_copies:
        copy.start()
    for copy in second_copies:
        copy.wait_recv()
    total = second_slots[0]
    for i in range(1, n_cols):
        total = total + second_slots[i]
    total = jnp.sum(total, axis=1, keepdims=True)
    b0, c1, c2, c3, c4, c5 = [total[i : i + 1, :] for i in range(6)]
    c = (None, c1, c2, c3, c4, c5)
    b = (b0, c1 + c2, c2 + c3, c3 + c4, c4 + c5)

    def square(q, m, base):
        return (
            q[0] * q[0] * m[base]
            + 2.0 * (q[0] * q[1]) * m[base + 1]
            + (q[1] * q[1] + 2.0 * (q[0] * q[2])) * m[base + 2]
            + 2.0 * (q[1] * q[2]) * m[base + 3]
            + q[2] * q[2] * m[base + 4]
        )

    def raised(q):
        return q[0], q[0] + q[1], q[1]

    one = (1.0, 2.0, 1.0)
    norm = square(one, b, 0)
    alpha0 = norm / square(one, c, 1)
    r1 = (1.0, 1.0 - alpha0)
    following = square(raised(r1), b, 0)
    beta0 = following / norm
    norm = following
    p1 = (r1[0] + beta0, r1[1] + beta0)
    p1_raised = raised(p1)
    alpha1 = norm / square(p1_raised, c, 1)
    r1_raised = raised(r1)
    r2 = (r1_raised[0], r1_raised[1] - alpha1 * p1[0], r1_raised[2] - alpha1 * p1[1])
    following = square(r2, b, 0)
    beta1 = following / norm
    p2 = tuple(r2[i] + beta1 * p1_raised[i] for i in range(3))
    alpha2 = following / square(p2, c, 1)
    steps = [alpha0 * one[i] + alpha1 * p1_raised[i] + alpha2 * p2[i] for i in range(3)]

    template = own(xf[pl.ds(96, 112), :], 96) + steps[0] * p[2] + steps[1] * p[1] + steps[2] * p[0]
    residual = r2[0] * p[2] + r2[1] * p[1] + r2[2] * p[0]
    residual = residual - alpha2 * (p2[0] * ap[2] + p2[1] * ap[1] + p2[2] * ap[0])
    template_ref[...] = swap_blocks(template)
    residual_ref[...] = swap_blocks(residual)
    for copy in x_copies + b_copies + v_copies + first_copies + second_copies:
        copy.wait_send()


def on_device(grid, right_side, initial_guess, kernel):
    n_rows, n_cols = grid
    middle = pltpu.VMEM((12, 16, LANES), F32)
    b_middle = pltpu.VMEM((8, 16, LANES), F32)
    side = pltpu.VMEM((2, 8, LANES), F32)
    halo = pltpu.VMEM((6, 8, LANES), F32)
    b_side = pltpu.VMEM((8, LANES), F32)
    b_halo = pltpu.VMEM((3, 8, LANES), F32)
    flat = pltpu.VMEM((FLAT, LANES), F32)
    weight = pltpu.VMEM((3 * LANES, 3 * LANES), BF16)
    tile = pltpu.VMEM((64, LANES), F32)
    dma = pltpu.SemaphoreType.DMA
    shape = jax.ShapeDtypeStruct((64, LANES), F32)
    vmem = pl.BlockSpec(memory_space=pltpu.VMEM)

    def body(*refs):
        image_kernel(grid, *refs)

    return pl.pallas_call(
        body,
        out_shape=(shape, shape),
        in_specs=[pl.BlockSpec(memory_space=pl.ANY)] * 3,
        out_specs=(vmem, vmem),
        scratch_shapes=[
            middle, middle, b_middle, side, side, side, side, b_side, b_side,
            halo, halo, halo, halo, b_halo, b_halo,
            flat, flat, flat, flat, flat, flat, flat, flat, flat, flat, flat, flat,
            pltpu.VMEM((128, 128), F32), pltpu.VMEM((8, 96, 1024), BF16),
            weight, weight, weight, weight,
            tile, tile, tile, tile, tile, tile,
            pltpu.VMEM((n_rows, 8, 128), F32), pltpu.VMEM((n_cols, 8, 128), F32), tile, tile, pltpu.VMEM((31, 31), F32), dma((3,)),
            dma((8,)), dma((8,)), dma((8,)), dma((8,)), dma((8,)), dma((8,)),
            dma((n_rows - 1,)), dma((n_rows - 1,)), dma((n_cols - 1,)), dma((n_cols - 1,)),
        ],
        compiler_params=pltpu.CompilerParams(
            collective_id=0, has_side_effects=True, vmem_limit_bytes=60 * 1024 * 1024
        ),
    )(right_side, initial_guess, kernel)


def solution(mesh):
    grid = (mesh.shape["row"], mesh.shape["col"])
    tiles = P("row", "col")
    return jax.shard_map(
        lambda *arrays: on_device(grid, *arrays),
        mesh=mesh,
        in_specs=(tiles, tiles, P()),
        out_specs=(tiles, tiles),
        check_vma=False,
    )
```

```python
import jax
import jax.numpy as jnp
from jax import lax
from jax.experimental import pallas as pl
from jax.experimental.pallas import tpu as pltpu
from jax.sharding import PartitionSpec as P

PENALTY = 0.05
F32, BF16 = jnp.float32, jnp.bfloat16
B = 16
LANES = B * B
PITCH = 24
ROWS = 13
FLAT = ROWS * PITCH
DIRECTIONS = ((-1, 0), (1, 0), (0, -1), (0, 1), (-1, -1), (-1, 1), (1, -1), (1, 1))
MESH = pl.DeviceIdType.MESH


def iota(shape, dim):
    return lax.broadcasted_iota(jnp.int32, shape, dim)


def roll(x, shift, axis):
    return pltpu.roll(x, shift % x.shape[axis], axis)


def rounded(x):
    return x.astype(BF16).astype(F32)


def put(pair, first, value):
    rows = pl.ds(first, value.shape[0])
    pair[0][rows, :] = value
    pair[1][rows, :] = value - rounded(value)


def swap_blocks(x):
    top, bottom = [], []
    for i in range(4):
        upper, lower = x[16 * i : 16 * i + 8], x[16 * i + 8 : 16 * i + 16]
        top += [upper[:, :128], upper[:, 128:]]
        bottom += [lower[:, :128], lower[:, 128:]]
    y = jnp.concatenate(top + bottom, axis=0)
    row, lane = iota(y.shape, 0), iota(y.shape, 1)
    for t in range(3):
        step = 1 << t
        row_bit, lane_bit = (row >> t) & 1, (lane >> (t + 4)) & 1
        from_below = roll(roll(y, -step, 0), B * step, 1)
        from_above = roll(roll(y, step, 0), -B * step, 1)
        y = jnp.where(row_bit == lane_bit, y, jnp.where(row_bit == 0, from_below, from_above))
    return jnp.concatenate([y[:64], y[64:]], axis=1)


def pick_lanes(x, lanes):
    return jnp.take_along_axis(x, lanes, axis=1, mode="promise_in_bounds")


def build_weights(taps_ref, shifted_ref, weights):
    taps = taps_ref[...]
    lane = iota((128, 128), 1)
    empty = (lane < 1) | (lane > 31)
    ahead = jnp.where(empty, 0.0, roll(taps, 1, 1)).T[0:48]
    flipped = jnp.where(empty, 0.0, pick_lanes(taps, jnp.clip(31 - lane, 0, 127))).T[0:48]
    group = iota((48, 128), 1) // B
    for number, source in enumerate((ahead, flipped)):
        pieces = []
        for tile in range(8):
            block = 8 * tile + group
            wanted = 46 - block if number == 0 else block - 16
            valid = (wanted >= 0) & (wanted <= 30)
            pieces.append(jnp.where(valid, pick_lanes(source, jnp.clip(wanted, 0, 30)), 0.0))
        base = jnp.concatenate(pieces, axis=1)
        column = iota(base.shape, 1) % B
        for t in range(4):
            base = jnp.where((column >> t) & 1 == 1, roll(base, 1 << t, 0), base)
        for shift in range(8):
            moved = roll(base, -B * shift, 1)
            high = moved.astype(BF16)
            shifted_ref[shift, 0:48] = high
            shifted_ref[shift, 48:96] = (moved - high.astype(F32)).astype(BF16)
        for part in range(2):
            weight = weights[2 * number + part]
            for di in (-1, 0, 1):
                for r in range(B):
                    start = 31 - 16 * di - r
                    lanes = 128 * (start // 8)
                    for dj in range(3):
                        rows = 48 * part + 16 * dj
                        weight[
                            LANES * (di + 1) + B * r : LANES * (di + 1) + B * r + B,
                            LANES * dj : LANES * dj + LANES,
                        ] = shifted_ref[start % 8, rows : rows + 16, lanes : lanes + LANES]


FIRST_UNIT = [(di, 0, low) for low in (False, True) for di in (-1, 0, 1)] + [(-1, -1, False), (0, -1, False)]
SECOND_UNIT = [(di, 1, low) for low in (False, True) for di in (-1, 0, 1)]
SECOND_UNIT += [(1, -1, False), (-1, -1, True), (0, -1, True), (1, -1, True)]


def correlate(field, high_weight, low_weight, first, count):
    def body(middle, right, left0, left1):
        queues = []
        for unit, products in enumerate((FIRST_UNIT, SECOND_UNIT)):
            queue = []
            for number, (di, dj, low) in enumerate(products):
                queue.append((unit, number % 2, di, dj, low, ((left0, left1)[unit], middle, right)[dj + 1]))
            queues.append(queue)
        for step in range(max(map(len, queues))):
            for queue in queues:
                if step < len(queue):
                    unit, register, di, dj, low, total = queue[step]
                    weight = low_weight if low else high_weight
                    tile = weight[LANES * (di + 1) : LANES * (di + 2), LANES * (dj + 1) : LANES * (dj + 2)]
                    pltpu.matmul_push_rhs(tile, staging_register=register, mxu_index=unit)
                    rows = pl.ds(first + PITCH * di, count)
                    pltpu.matmul_acc_lhs(total, field[0][rows, :], load_staged_rhs=register)
                    if not low:
                        pltpu.matmul_acc_lhs(total, field[1][rows, :])
        value = pltpu.matmul_pop(middle) + roll(pltpu.matmul_pop(right), -1, 0)
        return value + roll(pltpu.matmul_pop(left0) + pltpu.matmul_pop(left1), 1, 0)

    totals = [pltpu.ACC(unit)((count, LANES), F32) for unit in (0, 1, 0, 1)]
    return pl.run_scoped(body, *totals)


def smooth(source, first, count):
    x = source[pl.ds(first, count), :]
    above = source[pl.ds(first - PITCH, count), :]
    below = source[pl.ds(first + PITCH, count), :]
    wide = source[pl.ds(first - 8, count + 16), :]
    before = roll(wide, 1, 0)[8 : 8 + count]
    after = roll(wide, -1, 0)[8 : 8 + count]
    lane = iota(x.shape, 1)
    column = lane % B
    upper = roll(jnp.where(lane >= LANES - B, above, x), B, 1)
    lower = roll(jnp.where(lane < B, below, x), -B, 1)
    leftward = jnp.where(column == 0, roll(before, -(B - 1), 1), roll(x, 1, 1))
    rightward = jnp.where(column == B - 1, roll(after, B - 1, 1), roll(x, -1, 1))
    return PENALTY * (4.0 * x - upper - lower - leftward - rightward)


def own(value, first):
    return jnp.concatenate(
        [value[PITCH * r + 8 - first : PITCH * r + 24 - first] for r in range(4, 8)], axis=0
    )


def pack_sides(middle, left_ref, right_ref):
    sublane = iota((8, LANES), 0)
    for pair in range(2):
        first, second = 4 + 2 * pair, 5 + 2 * pair
        left_ref[pair] = jnp.where(sublane < 4, middle[first, 0:8], roll(middle[second, 0:8], 4, 0))
        right_ref[pair] = jnp.where(sublane < 4, roll(middle[first, 8:16], 4, 0), middle[second, 8:16])


def unpack(middle, from_left, from_right, flat, masked):
    sublane = iota((8, LANES), 0)
    for r in range(ROWS):
        right = jnp.zeros((8, LANES), F32)
        left = right
        if r >= 1:
            right = from_right[(r - 1) // 2]
            if (r - 1) % 2:
                right = roll(right, 4, 0)
        if r < 12:
            left = from_left[r // 2]
            if r % 2 == 0:
                left = roll(left, 4, 0)
        start = PITCH * r
        put(flat, start, masked(jnp.where(sublane < 4, right, left), start, 8))
        if r < 12:
            put(flat, start + 8, masked(middle[r], start + 8, 16))
        else:
            put(flat, start + 8, jnp.zeros((16, LANES), F32))


def image_kernel(
    grid, b_ref, guess_ref, kernel_ref, template_ref, residual_ref,
    x_mid, v_mid, b_mid, x_left, x_right, v_left, v_right, b_left, b_right,
    x_from_left, x_from_right, v_from_left, v_from_right, b_from_left, b_from_right,
    xf, xf_low, vf, vf_low, bf, rf, rf_low, t1, t1_low, t2, t2_low, mask_ref, taps_ref, shifted_ref, k_high, k_low, kt_high, kt_low,
    r0_own, v1_own, kr0_own, kv1_own, lr0_own, lv1_own,
    first_slots, second_slots, pixels, guess_tile, b_tile, taps_in, in_sems,
    x_send, x_recv, b_send, b_recv, v_send, v_recv, first_send, first_recv, second_send, second_recv,
):
    n_rows, n_cols = grid
    loads = (
        pltpu.make_async_copy(guess_ref, guess_tile, in_sems.at[0]),
        pltpu.make_async_copy(b_ref, b_tile, in_sems.at[1]),
        pltpu.make_async_copy(kernel_ref, taps_in, in_sems.at[2]),
    )
    row, col = lax.axis_index("row"), lax.axis_index("col")

    def at(dr, dc):
        return lax.rem(row + dr + n_rows, n_rows), lax.rem(col + dc + n_cols, n_cols)

    barrier = pltpu.get_barrier_semaphore()
    partners = [at(d, 0) for d in range(1, n_rows)] + [at(0, d) for d in range(1, n_cols)]
    partners += [at(dr, dc) for dr, dc in DIRECTIONS[4:]]
    for partner in partners:
        pl.semaphore_signal(barrier, inc=1, device_id=partner, device_id_type=MESH)

    taps_ref[...] = jnp.zeros_like(taps_ref)
    for load in loads:
        load.start()

    def remote(source, target, send, recv, device):
        return pltpu.make_async_remote_copy(
            src_ref=source, dst_ref=target, send_sem=send, recv_sem=recv, device_id=device, device_id_type=MESH
        )

    def field_copies(middle, left, right, from_left, from_right, send, recv):
        copies = []
        for number, (dr, dc) in enumerate(DIRECTIONS):
            if dc == 0:
                source = middle.at[pl.ds(4, 4)]
                target = middle.at[pl.ds(4 - 4 * dr, 4)]
            else:
                source = right if dc == 1 else left
                target = (from_left if dc == 1 else from_right).at[pl.ds(2 - 2 * dr, 2)]
            copies.append(remote(source, target, send.at[number], recv.at[number], at(dr, dc)))
        return copies

    def spread(middle, first, x):
        for i in range(4):
            middle[first + i] = x[16 * i : 16 * i + 16]

    loads[0].wait()
    spread(x_mid, 4, swap_blocks(guess_tile[...]))
    pack_sides(x_mid, x_left, x_right)
    loads[1].wait()
    spread(b_mid, 2, swap_blocks(b_tile[...]))
    sublane = iota((8, LANES), 0)
    left_part = right_part = jnp.zeros((8, LANES), F32)
    for i in range(4):
        here = sublane // 2 == i
        left_part = jnp.where(here, roll(b_mid[2 + i, 0:8], 2 * i, 0), left_part)
        right_part = jnp.where(here, roll(b_mid[2 + i, 8:16], 2 * i + 2, 0), right_part)
    b_left[...] = left_part
    b_right[...] = right_part

    pl.semaphore_wait(barrier, n_rows - 1 + n_cols - 1 + 4)

    x_copies = field_copies(x_mid, x_left, x_right, x_from_left, x_from_right, x_send, x_recv)
    b_copies = []
    for number, (dr, dc) in enumerate(DIRECTIONS):
        if dc == 0:
            source = b_mid.at[pl.ds(2 if dr == -1 else 4, 2)]
            target = b_mid.at[pl.ds(6 if dr == -1 else 0, 2)]
        else:
            source = b_right if dc == 1 else b_left
            target = (b_from_left if dc == 1 else b_from_right).at[1 - dr]
        b_copies.append(remote(source, target, b_send.at[number], b_recv.at[number], at(dr, dc)))
    for copy in x_copies + b_copies:
        copy.start()

    loads[2].wait()
    taps_ref[0:31, 0:31] = taps_in[...]
    build_weights(taps_ref, shifted_ref, (k_high, k_low, kt_high, kt_low))
    flat = iota((FLAT, LANES), 0)
    slot = flat % PITCH
    block_row = row * 4 + flat // PITCH - 4 - (slot < 4).astype(jnp.int32)
    block_col = col * 16 + slot - 8 + 24 * (slot < 4).astype(jnp.int32)
    inside = (block_row >= 0) & (block_row < 4 * n_rows) & (block_col >= 0) & (block_col < 16 * n_cols)
    mask_ref[...] = inside.astype(F32)

    def masked(value, first, count):
        return jnp.where(mask_ref[pl.ds(first, count), :] > 0.5, value, 0.0)

    def apply_twice(source, second):
        for first, count, keep, kept in ((24, 152, 24, 144), (160, 112, 168, 104)):
            value = correlate(source, k_high, k_low, first, count)[keep - first : keep - first + kept]
            put((t1, t1_low), keep, masked(value, keep, kept))
        smooth_source = []
        for first, count, keep, kept in ((48, 104, 48, 96), (136, 112, 144, 104)):
            value = correlate((t1, t1_low), kt_high, kt_low, first, count)[keep - first : keep - first + kept]
            smooth_source.append(smooth(source[0], keep, kept))
            value = value + smooth_source[-1]
            put(second, keep, masked(bf[pl.ds(keep, kept), :] - value if source[0] is xf else value, keep, kept))
        for first, count, keep, kept in ((72, 56, 72, 48), (112, 112, 120, 104)):
            value = correlate(second, k_high, k_low, first, count)[keep - first : keep - first + kept]
            put((t2, t2_low), keep, masked(value, keep, kept))
        return (
            own(t1[pl.ds(96, 104), :], 96),
            own(jnp.concatenate(smooth_source, axis=0), 48),
            own(t2[pl.ds(96, 104), :], 96),
            own(smooth(second[0], 96, 104), 96),
        )

    for copy in x_copies:
        copy.wait_recv()
    unpack(x_mid, x_from_left, x_from_right, (xf, xf_low), masked)
    for copy in b_copies:
        copy.wait_recv()
    for r in range(2, 11):
        right = left = jnp.zeros((8, LANES), F32)
        if r >= 3:
            right = roll(b_from_right[(r - 1) // 4], -2 * ((r - 1) % 4), 0)
        if r < 10:
            left = roll(b_from_left[r // 4], 6 - 2 * (r % 4), 0)
        bf[PITCH * r : PITCH * r + 8] = jnp.where(sublane < 4, right, left)
        if r < 10:
            bf[PITCH * r + 8 : PITCH * r + 24] = b_mid[r - 2]

    _, _, kr0, lr0 = apply_twice((xf, xf_low), (rf, rf_low))
    v1 = own(correlate((t2, t2_low), kt_high, kt_low, 96, 104), 96) + lr0
    spread(v_mid, 4, v1)
    pack_sides(v_mid, v_left, v_right)
    v_copies = field_copies(v_mid, v_left, v_right, v_from_left, v_from_right, v_send, v_recv)
    for copy in v_copies:
        copy.start()
    r0_own[...] = own(rf[pl.ds(96, 104), :], 96)
    v1_own[...] = v1
    kr0_own[...] = kr0
    lr0_own[...] = lr0

    for copy in v_copies:
        copy.wait_recv()
    unpack(v_mid, v_from_left, v_from_right, (vf, vf_low), masked)
    kv1, lv1, kv2, lv2 = apply_twice((vf, vf_low), (rf, rf_low))
    v2 = own(rf[pl.ds(96, 104), :], 96)

    def powers(zero, one, two):
        return two, one - two, zero - 2.0 * one + two

    r0, v1 = r0_own[...], v1_own[...]
    p = powers(r0, v1, v2)
    kp = powers(kr0_own[...], kv1, kv2)
    lp = powers(lr0_own[...], lv1, lv2)

    def lanes_of(x):
        total = x[0:8]
        for i in range(1, 8):
            total = total + x[8 * i : 8 * i + 8]
        total = total[:, :128] + total[:, 128:]
        return jnp.sum(total, axis=0, keepdims=True)

    moments = [lanes_of(p[2] * p[2])]
    for i, j in ((2, 2), (1, 2), (1, 1), (0, 1), (0, 0)):
        moments.append(lanes_of(kp[i] * kp[j] + p[i] * lp[j]))
    slot8 = iota((8, 128), 0)
    packed = jnp.zeros((8, 128), F32)
    for i, moment in enumerate(moments):
        packed = jnp.where(slot8 == i, moment, packed)
    for step in (64, 32, 16):
        packed = packed + roll(packed, step, 1)
    mine = iota((8, 128), 1) // B == slot8
    packed = jnp.sum(jnp.where(mine, packed, 0.0), axis=0, keepdims=True)

    def gather(slots, me, count, target, send, recv):
        return [
            remote(slots.at[me], slots.at[me], send.at[d - 1], recv.at[d - 1], target(d)) for d in range(1, count)
        ]

    first_slots[row] = packed
    first_copies = gather(first_slots, row, n_rows, lambda d: at(d, 0), first_send, first_recv)
    for copy in first_copies:
        copy.start()
    v3 = own(correlate((t2, t2_low), kt_high, kt_low, 96, 104), 96) + lv2
    for number, value in enumerate(p + powers(v1, v2, v3)):
        pixels[number] = swap_blocks(value)
    for copy in first_copies:
        copy.wait_recv()
    total = first_slots[0]
    for i in range(1, n_rows):
        total = total + first_slots[i]
    second_slots[col] = total
    second_copies = gather(second_slots, col, n_cols, lambda d: at(0, d), second_send, second_recv)
    for copy in second_copies:
        copy.start()
    for copy in second_copies:
        copy.wait_recv()
    total = second_slots[0]
    for i in range(1, n_cols):
        total = total + second_slots[i]
    total = jnp.sum(jnp.where(mine, jnp.broadcast_to(total, (8, 128)), 0.0), axis=1, keepdims=True)
    b0, c1, c2, c3, c4, c5 = [total[i : i + 1, :] for i in range(6)]
    c = (None, c1, c2, c3, c4, c5)
    b = (b0, c1 + c2, c2 + c3, c3 + c4, c4 + c5)

    def square(q, m, base):
        return (
            q[0] * q[0] * m[base]
            + 2.0 * (q[0] * q[1]) * m[base + 1]
            + (q[1] * q[1] + 2.0 * (q[0] * q[2])) * m[base + 2]
            + 2.0 * (q[1] * q[2]) * m[base + 3]
            + q[2] * q[2] * m[base + 4]
        )

    def raised(q):
        return q[0], q[0] + q[1], q[1]

    one = (1.0, 2.0, 1.0)
    norm = square(one, b, 0)
    alpha0 = norm / square(one, c, 1)
    r1 = (1.0, 1.0 - alpha0)
    following = square(raised(r1), b, 0)
    beta0 = following / norm
    norm = following
    p1 = (r1[0] + beta0, r1[1] + beta0)
    p1_raised = raised(p1)
    alpha1 = norm / square(p1_raised, c, 1)
    r1_raised = raised(r1)
    r2 = (r1_raised[0], r1_raised[1] - alpha1 * p1[0], r1_raised[2] - alpha1 * p1[1])
    following = square(r2, b, 0)
    beta1 = following / norm
    p2 = tuple(r2[i] + beta1 * p1_raised[i] for i in range(3))
    alpha2 = following / square(p2, c, 1)
    steps = [alpha0 * one[i] + alpha1 * p1_raised[i] + alpha2 * p2[i] for i in range(3)]

    f0, f1, f2, af0, af1, af2 = [pixels[number] for number in range(6)]
    template_ref[...] = guess_tile[...] + steps[0] * f2 + steps[1] * f1 + steps[2] * f0
    residual = r2[0] * f2 + r2[1] * f1 + r2[2] * f0
    residual_ref[...] = residual - alpha2 * (p2[0] * af2 + p2[1] * af1 + p2[2] * af0)
    for copy in x_copies + b_copies + v_copies + first_copies + second_copies:
        copy.wait_send()


def on_device(grid, right_side, initial_guess, kernel):
    n_rows, n_cols = grid
    middle = pltpu.VMEM((12, 16, LANES), F32)
    b_middle = pltpu.VMEM((8, 16, LANES), F32)
    side = pltpu.VMEM((2, 8, LANES), F32)
    halo = pltpu.VMEM((6, 8, LANES), F32)
    b_side = pltpu.VMEM((8, LANES), F32)
    b_halo = pltpu.VMEM((3, 8, LANES), F32)
    flat = pltpu.VMEM((FLAT, LANES), F32)
    weight = pltpu.VMEM((3 * LANES, 3 * LANES), BF16)
    tile = pltpu.VMEM((64, LANES), F32)
    dma = pltpu.SemaphoreType.DMA
    shape = jax.ShapeDtypeStruct((64, LANES), F32)
    vmem = pl.BlockSpec(memory_space=pltpu.VMEM)

    def body(*refs):
        image_kernel(grid, *refs)

    return pl.pallas_call(
        body,
        out_shape=(shape, shape),
        in_specs=[pl.BlockSpec(memory_space=pltpu.HBM)] * 3,
        out_specs=(vmem, vmem),
        scratch_shapes=[
            middle, middle, b_middle, side, side, side, side, b_side, b_side,
            halo, halo, halo, halo, b_halo, b_halo,
            flat, flat, flat, flat, flat, flat, flat, flat, flat, flat, flat, flat,
            pltpu.VMEM((128, 128), F32), pltpu.VMEM((8, 96, 1024), BF16),
            weight, weight, weight, weight,
            tile, tile, tile, tile, tile, tile,
            pltpu.VMEM((n_rows, 1, 128), F32), pltpu.VMEM((n_cols, 1, 128), F32), pltpu.VMEM((6, 64, LANES), F32), tile, tile, pltpu.VMEM((31, 31), F32), dma((3,)),
            dma((8,)), dma((8,)), dma((8,)), dma((8,)), dma((8,)), dma((8,)),
            dma((n_rows - 1,)), dma((n_rows - 1,)), dma((n_cols - 1,)), dma((n_cols - 1,)),
        ],
        compiler_params=pltpu.CompilerParams(
            collective_id=0, has_side_effects=True, vmem_limit_bytes=16 * 1024 * 1024
        ),
    )(*(pltpu.with_memory_space_constraint(x, pltpu.HBM) for x in (right_side, initial_guess, kernel)))


def solution(mesh):
    grid = (mesh.shape["row"], mesh.shape["col"])
    tiles = P("row", "col")
    return jax.shard_map(
        lambda *arrays: on_device(grid, *arrays),
        mesh=mesh,
        in_specs=(tiles, tiles, P()),
        out_specs=(tiles, tiles),
        check_vma=False,
    )
```

```python
import jax
import jax.numpy as jnp
from jax import lax
from jax.experimental import pallas as pl
from jax.experimental.pallas import tpu as pltpu
from jax.sharding import PartitionSpec as P

PENALTY = 0.05
F32, BF16 = jnp.float32, jnp.bfloat16
B = 16
LANES = B * B
PITCH = 24
ROWS = 13
FLAT = ROWS * PITCH
DIRECTIONS = ((-1, -1), (-1, 1), (1, -1), (1, 1), (0, -1), (0, 1), (-1, 0), (1, 0))
MESH = pl.DeviceIdType.MESH


def iota(shape, dim):
    return lax.broadcasted_iota(jnp.int32, shape, dim)


def roll(x, shift, axis):
    return pltpu.roll(x, shift % x.shape[axis], axis)


def rounded(x):
    return x.astype(BF16).astype(F32)


def put(pair, first, value):
    rows = pl.ds(first, value.shape[0])
    pair[0][rows, :] = value
    pair[1][rows, :] = value - rounded(value)


def swap_blocks(x):
    top, bottom = [], []
    for i in range(4):
        upper, lower = x[16 * i : 16 * i + 8], x[16 * i + 8 : 16 * i + 16]
        top += [upper[:, :128], upper[:, 128:]]
        bottom += [lower[:, :128], lower[:, 128:]]
    y = jnp.concatenate(top + bottom, axis=0)
    row, lane = iota(y.shape, 0), iota(y.shape, 1)
    for t in range(3):
        step = 1 << t
        row_bit, lane_bit = (row >> t) & 1, (lane >> (t + 4)) & 1
        from_below = roll(roll(y, -step, 0), B * step, 1)
        from_above = roll(roll(y, step, 0), -B * step, 1)
        y = jnp.where(row_bit == lane_bit, y, jnp.where(row_bit == 0, from_below, from_above))
    return jnp.concatenate([y[:64], y[64:]], axis=1)


def pick_lanes(x, lanes):
    return jnp.take_along_axis(x, lanes, axis=1, mode="promise_in_bounds")


def build_weights(taps_ref, shifted_ref, weights):
    taps = taps_ref[...]
    lane = iota((128, 128), 1)
    empty = (lane < 1) | (lane > 31)
    ahead = jnp.where(empty, 0.0, roll(taps, 1, 1)).T[0:48]
    flipped = jnp.where(empty, 0.0, pick_lanes(taps, jnp.clip(31 - lane, 0, 127))).T[0:48]
    group = iota((48, 128), 1) // B
    for number, source in enumerate((ahead, flipped)):
        pieces = []
        for tile in range(8):
            block = 8 * tile + group
            wanted = 46 - block if number == 0 else block - 16
            valid = (wanted >= 0) & (wanted <= 30)
            pieces.append(jnp.where(valid, pick_lanes(source, jnp.clip(wanted, 0, 30)), 0.0))
        base = jnp.concatenate(pieces, axis=1)
        column = iota(base.shape, 1) % B
        for t in range(4):
            base = jnp.where((column >> t) & 1 == 1, roll(base, 1 << t, 0), base)
        for shift in range(8):
            moved = roll(base, -B * shift, 1)
            high = moved.astype(BF16)
            shifted_ref[shift, 0:48] = high
            shifted_ref[shift, 48:96] = (moved - high.astype(F32)).astype(BF16)
        for part in range(2):
            weight = weights[2 * number + part]
            for di in (-1, 0, 1):
                for r in range(B):
                    start = 31 - 16 * di - r
                    lanes = 128 * (start // 8)
                    for dj in range(3):
                        rows = 48 * part + 16 * dj
                        weight[
                            LANES * (di + 1) + B * r : LANES * (di + 1) + B * r + B,
                            LANES * dj : LANES * dj + LANES,
                        ] = shifted_ref[start % 8, rows : rows + 16, lanes : lanes + LANES]


FIRST_UNIT = [(di, 0, low) for low in (False, True) for di in (-1, 0, 1)] + [(-1, -1, False), (0, -1, False)]
SECOND_UNIT = [(di, 1, low) for low in (False, True) for di in (-1, 0, 1)]
SECOND_UNIT += [(1, -1, False), (-1, -1, True), (0, -1, True), (1, -1, True)]


def correlate(field, high_weight, low_weight, first, count):
    def body(middle, right, left0, left1):
        queues = []
        for unit, products in enumerate((FIRST_UNIT, SECOND_UNIT)):
            queue = []
            for number, (di, dj, low) in enumerate(products):
                queue.append((unit, number % 2, di, dj, low, ((left0, left1)[unit], middle, right)[dj + 1]))
            queues.append(queue)
        for step in range(max(map(len, queues))):
            for queue in queues:
                if step < len(queue):
                    unit, register, di, dj, low, total = queue[step]
                    weight = low_weight if low else high_weight
                    tile = weight[LANES * (di + 1) : LANES * (di + 2), LANES * (dj + 1) : LANES * (dj + 2)]
                    pltpu.matmul_push_rhs(tile, staging_register=register, mxu_index=unit)
                    rows = pl.ds(first + PITCH * di, count)
                    pltpu.matmul_acc_lhs(total, field[0][rows, :], load_staged_rhs=register)
                    if not low:
                        pltpu.matmul_acc_lhs(total, field[1][rows, :])
        value = pltpu.matmul_pop(middle) + roll(pltpu.matmul_pop(right), -1, 0)
        return value + roll(pltpu.matmul_pop(left0) + pltpu.matmul_pop(left1), 1, 0)

    totals = [pltpu.ACC(unit)((count, LANES), F32) for unit in (0, 1, 0, 1)]
    return pl.run_scoped(body, *totals)


def smooth(source, first, count):
    x = source[pl.ds(first, count), :]
    above = source[pl.ds(first - PITCH, count), :]
    below = source[pl.ds(first + PITCH, count), :]
    wide = source[pl.ds(first - 8, count + 16), :]
    before = roll(wide, 1, 0)[8 : 8 + count]
    after = roll(wide, -1, 0)[8 : 8 + count]
    lane = iota(x.shape, 1)
    column = lane % B
    upper = roll(jnp.where(lane >= LANES - B, above, x), B, 1)
    lower = roll(jnp.where(lane < B, below, x), -B, 1)
    leftward = jnp.where(column == 0, roll(before, -(B - 1), 1), roll(x, 1, 1))
    rightward = jnp.where(column == B - 1, roll(after, B - 1, 1), roll(x, -1, 1))
    return PENALTY * (4.0 * x - upper - lower - leftward - rightward)


def own(value, first):
    return jnp.concatenate(
        [value[PITCH * r + 8 - first : PITCH * r + 24 - first] for r in range(4, 8)], axis=0
    )


def pack_sides(middle, left_ref, right_ref):
    sublane = iota((8, LANES), 0)
    for pair in range(2):
        first, second = 4 + 2 * pair, 5 + 2 * pair
        left_ref[pair] = jnp.where(sublane < 4, middle[first, 0:8], roll(middle[second, 0:8], 4, 0))
        right_ref[pair] = jnp.where(sublane < 4, roll(middle[first, 8:16], 4, 0), middle[second, 8:16])


def unpack(middle, from_left, from_right, flat, masked):
    sublane = iota((8, LANES), 0)
    for r in range(ROWS):
        right = jnp.zeros((8, LANES), F32)
        left = right
        if r >= 1:
            right = from_right[(r - 1) // 2]
            if (r - 1) % 2:
                right = roll(right, 4, 0)
        if r < 12:
            left = from_left[r // 2]
            if r % 2 == 0:
                left = roll(left, 4, 0)
        start = PITCH * r
        put(flat, start, masked(jnp.where(sublane < 4, right, left), start, 8))
        if r < 12:
            put(flat, start + 8, masked(middle[r], start + 8, 16))
        else:
            put(flat, start + 8, jnp.zeros((16, LANES), F32))


def image_kernel(
    grid, b_ref, guess_ref, kernel_ref, template_ref, residual_ref,
    x_mid, v_mid, b_mid, x_left, x_right, v_left, v_right, b_left, b_right,
    x_from_left, x_from_right, v_from_left, v_from_right, b_from_left, b_from_right,
    xf, xf_low, vf, vf_low, bf, rf, rf_low, t1, t1_low, t2, t2_low, mask_ref, taps_ref, shifted_ref, k_high, k_low, kt_high, kt_low,
    r0_own, v1_own, kr0_own, kv1_own, lr0_own, lv1_own,
    first_slots, second_slots, pixels, far_sems, guess_tile, b_tile, taps_in, in_sems,
    x_send, x_recv, b_send, b_recv, v_send, v_recv, first_send, first_recv, second_send, second_recv,
):
    n_rows, n_cols = grid
    loads = (
        pltpu.make_async_copy(guess_ref, guess_tile, in_sems.at[0]),
        pltpu.make_async_copy(b_ref, b_tile, in_sems.at[1]),
        pltpu.make_async_copy(kernel_ref, taps_in, in_sems.at[2]),
    )
    row, col = lax.axis_index("row"), lax.axis_index("col")

    def at(dr, dc):
        return lax.rem(row + dr + n_rows, n_rows), lax.rem(col + dc + n_cols, n_cols)

    for load in loads:
        load.start()
    barrier = pltpu.get_barrier_semaphore()
    partners = [at(dr, dc) for dr, dc in DIRECTIONS[:6]] + [at(d, 0) for d in range(1, n_rows)]
    for partner in partners:
        pl.semaphore_signal(barrier, inc=1, device_id=partner, device_id_type=MESH)

    def remote(source, target, send, recv, device):
        return pltpu.make_async_remote_copy(
            src_ref=source, dst_ref=target, send_sem=send, recv_sem=recv, device_id=device, device_id_type=MESH
        )

    def field_copies(middle, left, right, from_left, from_right, send, recv):
        copies = []
        for number, (dr, dc) in enumerate(DIRECTIONS):
            if dc == 0:
                source = middle.at[pl.ds(4, 4)]
                target = middle.at[pl.ds(4 - 4 * dr, 4)]
            else:
                source = right if dc == 1 else left
                target = (from_left if dc == 1 else from_right).at[pl.ds(2 - 2 * dr, 2)]
            copies.append(remote(source, target, send.at[number], recv.at[number], at(dr, dc)))
        return copies

    def spread(middle, first, x):
        for i in range(4):
            middle[first + i] = x[16 * i : 16 * i + 16]

    loads[0].wait()
    spread(x_mid, 4, swap_blocks(guess_tile[...]))
    pack_sides(x_mid, x_left, x_right)
    pl.semaphore_wait(barrier, n_rows - 1 + 6)

    x_copies = field_copies(x_mid, x_left, x_right, x_from_left, x_from_right, x_send, x_recv)
    for copy in x_copies:
        copy.start()
    loads[1].wait()
    spread(b_mid, 2, swap_blocks(b_tile[...]))
    sublane = iota((8, LANES), 0)
    left_part = right_part = jnp.zeros((8, LANES), F32)
    for i in range(4):
        here = sublane // 2 == i
        left_part = jnp.where(here, roll(b_mid[2 + i, 0:8], 2 * i, 0), left_part)
        right_part = jnp.where(here, roll(b_mid[2 + i, 8:16], 2 * i + 2, 0), right_part)
    b_left[...] = left_part
    b_right[...] = right_part

    b_copies = []
    for number, (dr, dc) in enumerate(DIRECTIONS):
        if dc == 0:
            source = b_mid.at[pl.ds(2 if dr == -1 else 4, 2)]
            target = b_mid.at[pl.ds(6 if dr == -1 else 0, 2)]
        else:
            source = b_right if dc == 1 else b_left
            target = (b_from_left if dc == 1 else b_from_right).at[1 - dr]
        b_copies.append(remote(source, target, b_send.at[number], b_recv.at[number], at(dr, dc)))
    for copy in b_copies:
        copy.start()

    taps_ref[...] = jnp.zeros_like(taps_ref)
    loads[2].wait()
    taps_ref[0:31, 0:31] = taps_in[...]
    build_weights(taps_ref, shifted_ref, (k_high, k_low, kt_high, kt_low))
    flat = iota((FLAT, LANES), 0)
    slot = flat % PITCH
    block_row = row * 4 + flat // PITCH - 4 - (slot < 4).astype(jnp.int32)
    block_col = col * 16 + slot - 8 + 24 * (slot < 4).astype(jnp.int32)
    inside = (block_row >= 0) & (block_row < 4 * n_rows) & (block_col >= 0) & (block_col < 16 * n_cols)
    mask_ref[...] = inside.astype(F32)

    def masked(value, first, count):
        return jnp.where(mask_ref[pl.ds(first, count), :] > 0.5, value, 0.0)

    distances = []
    while 2 << len(distances) < n_cols // 2:
        distances.append(2 << len(distances))

    def greet(number):
        if number < len(distances):
            for d in (distances[number], n_cols - distances[number]):
                pl.semaphore_signal(far_sems.at[number], inc=1, device_id=at(0, d), device_id_type=MESH)

    def meet(number):
        if number < len(distances):
            pl.semaphore_wait(far_sems.at[number], 2)

    def take_b():
        for copy in b_copies:
            copy.wait_recv()
        for r in range(2, 11):
            right = left = jnp.zeros((8, LANES), F32)
            if r >= 3:
                right = roll(b_from_right[(r - 1) // 4], -2 * ((r - 1) % 4), 0)
            if r < 10:
                left = roll(b_from_left[r // 4], 6 - 2 * (r % 4), 0)
            bf[PITCH * r : PITCH * r + 8] = jnp.where(sublane < 4, right, left)
            if r < 10:
                bf[PITCH * r + 8 : PITCH * r + 24] = b_mid[r - 2]

    def apply_twice(source, second, between):
        for first, count, keep, kept in ((24, 152, 24, 144), (160, 112, 168, 104)):
            value = correlate(source, k_high, k_low, first, count)[keep - first : keep - first + kept]
            put((t1, t1_low), keep, masked(value, keep, kept))
        between()
        smooth_source = []
        for first, count, keep, kept in ((48, 104, 48, 96), (136, 112, 144, 104)):
            value = correlate((t1, t1_low), kt_high, kt_low, first, count)[keep - first : keep - first + kept]
            smooth_source.append(smooth(source[0], keep, kept))
            value = value + smooth_source[-1]
            put(second, keep, masked(bf[pl.ds(keep, kept), :] - value if source[0] is xf else value, keep, kept))
        for first, count, keep, kept in ((72, 56, 72, 48), (112, 112, 120, 104)):
            value = correlate(second, k_high, k_low, first, count)[keep - first : keep - first + kept]
            put((t2, t2_low), keep, masked(value, keep, kept))
        return (
            own(t1[pl.ds(96, 104), :], 96),
            own(jnp.concatenate(smooth_source, axis=0), 48),
            own(t2[pl.ds(96, 104), :], 96),
            own(smooth(second[0], 96, 104), 96),
        )

    for copy in x_copies:
        copy.wait_recv()
    greet(0)
    unpack(x_mid, x_from_left, x_from_right, (xf, xf_low), masked)
    _, _, kr0, lr0 = apply_twice((xf, xf_low), (rf, rf_low), take_b)
    v1 = own(correlate((t2, t2_low), kt_high, kt_low, 96, 104), 96) + lr0
    spread(v_mid, 4, v1)
    pack_sides(v_mid, v_left, v_right)
    v_copies = field_copies(v_mid, v_left, v_right, v_from_left, v_from_right, v_send, v_recv)
    for copy in v_copies:
        copy.start()
    meet(0)
    greet(1)
    r0_own[...] = own(rf[pl.ds(96, 104), :], 96)
    v1_own[...] = v1
    kr0_own[...] = kr0
    lr0_own[...] = lr0

    for copy in v_copies:
        copy.wait_recv()
    unpack(v_mid, v_from_left, v_from_right, (vf, vf_low), masked)
    kv1, lv1, kv2, lv2 = apply_twice((vf, vf_low), (rf, rf_low), lambda: None)
    v2 = own(rf[pl.ds(96, 104), :], 96)

    def powers(zero, one, two):
        return two, one - two, zero - 2.0 * one + two

    r0, v1 = r0_own[...], v1_own[...]
    p = powers(r0, v1, v2)
    kp = powers(kr0_own[...], kv1, kv2)
    lp = powers(lr0_own[...], lv1, lv2)

    def lanes_of(x):
        total = x[0:8]
        for i in range(1, 8):
            total = total + x[8 * i : 8 * i + 8]
        total = total[:, :128] + total[:, 128:]
        return jnp.sum(total, axis=0, keepdims=True)

    moments = [lanes_of(p[2] * p[2])]
    for i, j in ((2, 2), (1, 2), (1, 1), (0, 1), (0, 0)):
        moments.append(lanes_of(kp[i] * kp[j] + p[i] * lp[j]))
    slot8 = iota((8, 128), 0)
    packed = jnp.zeros((8, 128), F32)
    for i, moment in enumerate(moments):
        packed = jnp.where(slot8 == i, moment, packed)
    for step in (64, 32, 16):
        packed = packed + roll(packed, step, 1)
    mine = iota((8, 128), 1) // B == slot8
    packed = jnp.sum(jnp.where(mine, packed, 0.0), axis=0, keepdims=True)

    def gather(slots, me, count, target, send, recv):
        return [
            remote(slots.at[me], slots.at[me], send.at[d - 1], recv.at[d - 1], target(d)) for d in range(1, count)
        ]

    first_slots[row] = packed
    first_copies = gather(first_slots, row, n_rows, lambda d: at(d, 0), first_send, first_recv)
    for copy in first_copies:
        copy.start()
    v3 = own(correlate((t2, t2_low), kt_high, kt_low, 96, 104), 96) + lv2
    for number, value in enumerate(p + powers(v1, v2, v3)):
        pixels[number] = swap_blocks(value)
    for copy in first_copies:
        copy.wait_recv()
    meet(1)
    total = first_slots[0]
    for i in range(1, n_rows):
        total = total + first_slots[i]
    second_slots[col] = total
    second_copies = gather(second_slots, col, n_cols, lambda d: at(0, d), second_send, second_recv)
    for copy in second_copies:
        copy.start()
    for copy in second_copies:
        copy.wait_recv()
    total = second_slots[0]
    for i in range(1, n_cols):
        total = total + second_slots[i]
    total = jnp.sum(jnp.where(mine, jnp.broadcast_to(total, (8, 128)), 0.0), axis=1, keepdims=True)
    b0, c1, c2, c3, c4, c5 = [total[i : i + 1, :] for i in range(6)]
    c = (None, c1, c2, c3, c4, c5)
    b = (b0, c1 + c2, c2 + c3, c3 + c4, c4 + c5)

    def square(q, m, base):
        return (
            q[0] * q[0] * m[base]
            + 2.0 * (q[0] * q[1]) * m[base + 1]
            + (q[1] * q[1] + 2.0 * (q[0] * q[2])) * m[base + 2]
            + 2.0 * (q[1] * q[2]) * m[base + 3]
            + q[2] * q[2] * m[base + 4]
        )

    def raised(q):
        return q[0], q[0] + q[1], q[1]

    one = (1.0, 2.0, 1.0)
    norm = square(one, b, 0)
    alpha0 = norm / square(one, c, 1)
    r1 = (1.0, 1.0 - alpha0)
    following = square(raised(r1), b, 0)
    beta0 = following / norm
    norm = following
    p1 = (r1[0] + beta0, r1[1] + beta0)
    p1_raised = raised(p1)
    alpha1 = norm / square(p1_raised, c, 1)
    r1_raised = raised(r1)
    r2 = (r1_raised[0], r1_raised[1] - alpha1 * p1[0], r1_raised[2] - alpha1 * p1[1])
    following = square(r2, b, 0)
    beta1 = following / norm
    p2 = tuple(r2[i] + beta1 * p1_raised[i] for i in range(3))
    alpha2 = following / square(p2, c, 1)
    steps = [alpha0 * one[i] + alpha1 * p1_raised[i] + alpha2 * p2[i] for i in range(3)]

    f0, f1, f2, af0, af1, af2 = [pixels[number] for number in range(6)]
    template_ref[...] = guess_tile[...] + steps[0] * f2 + steps[1] * f1 + steps[2] * f0
    residual = r2[0] * f2 + r2[1] * f1 + r2[2] * f0
    residual_ref[...] = residual - alpha2 * (p2[0] * af2 + p2[1] * af1 + p2[2] * af0)
    for copy in x_copies + b_copies + v_copies + first_copies + second_copies:
        copy.wait_send()


def on_device(grid, right_side, initial_guess, kernel):
    n_rows, n_cols = grid
    middle = pltpu.VMEM((12, 16, LANES), F32)
    b_middle = pltpu.VMEM((8, 16, LANES), F32)
    side = pltpu.VMEM((2, 8, LANES), F32)
    halo = pltpu.VMEM((6, 8, LANES), F32)
    b_side = pltpu.VMEM((8, LANES), F32)
    b_halo = pltpu.VMEM((3, 8, LANES), F32)
    flat = pltpu.VMEM((FLAT, LANES), F32)
    weight = pltpu.VMEM((3 * LANES, 3 * LANES), BF16)
    tile = pltpu.VMEM((64, LANES), F32)
    dma = pltpu.SemaphoreType.DMA
    shape = jax.ShapeDtypeStruct((64, LANES), F32)
    vmem = pl.BlockSpec(memory_space=pltpu.VMEM)

    def body(*refs):
        image_kernel(grid, *refs)

    return pl.pallas_call(
        body,
        out_shape=(shape, shape),
        in_specs=[pl.BlockSpec(memory_space=pltpu.HBM)] * 3,
        out_specs=(vmem, vmem),
        scratch_shapes=[
            middle, middle, b_middle, side, side, side, side, b_side, b_side,
            halo, halo, halo, halo, b_halo, b_halo,
            flat, flat, flat, flat, flat, flat, flat, flat, flat, flat, flat, flat,
            pltpu.VMEM((128, 128), F32), pltpu.VMEM((8, 96, 1024), BF16),
            weight, weight, weight, weight,
            tile, tile, tile, tile, tile, tile,
            pltpu.VMEM((n_rows, 1, 128), F32), pltpu.VMEM((n_cols, 1, 128), F32), pltpu.VMEM((6, 64, LANES), F32), pltpu.SemaphoreType.REGULAR((2,)), tile, tile, pltpu.VMEM((31, 31), F32), dma((3,)),
            dma((8,)), dma((8,)), dma((8,)), dma((8,)), dma((8,)), dma((8,)),
            dma((n_rows - 1,)), dma((n_rows - 1,)), dma((n_cols - 1,)), dma((n_cols - 1,)),
        ],
        compiler_params=pltpu.CompilerParams(
            collective_id=0, has_side_effects=True, vmem_limit_bytes=16 * 1024 * 1024
        ),
    )(*(pltpu.with_memory_space_constraint(x, pltpu.HBM) for x in (right_side, initial_guess, kernel)))


def solution(mesh):
    grid = (mesh.shape["row"], mesh.shape["col"])
    tiles = P("row", "col")
    return jax.shard_map(
        lambda *arrays: on_device(grid, *arrays),
        mesh=mesh,
        in_specs=(tiles, tiles, P()),
        out_specs=(tiles, tiles),
        check_vma=False,
    )
```

```python
import jax
import jax.numpy as jnp
from jax import lax
from jax.experimental import pallas as pl
from jax.experimental.pallas import tpu as pltpu
from jax.sharding import PartitionSpec as P

PENALTY = 0.05
F32, BF16 = jnp.float32, jnp.bfloat16
B = 16
LANES = B * B
PITCH = 24
ROWS = 13
FLAT = ROWS * PITCH
DIRECTIONS = ((-1, -1), (-1, 1), (1, -1), (1, 1), (0, -1), (0, 1), (-1, 0), (1, 0))
MESH = pl.DeviceIdType.MESH


def iota(shape, dim):
    return lax.broadcasted_iota(jnp.int32, shape, dim)


def roll(x, shift, axis):
    return pltpu.roll(x, shift % x.shape[axis], axis)


def rounded(x):
    return x.astype(BF16).astype(F32)


def put(pair, first, value):
    rows = pl.ds(first, value.shape[0])
    pair[0][rows, :] = value
    pair[1][rows, :] = value - rounded(value)


def swap_blocks(x):
    top, bottom = [], []
    for i in range(4):
        upper, lower = x[16 * i : 16 * i + 8], x[16 * i + 8 : 16 * i + 16]
        top += [upper[:, :128], upper[:, 128:]]
        bottom += [lower[:, :128], lower[:, 128:]]
    y = jnp.concatenate(top + bottom, axis=0)
    row, lane = iota(y.shape, 0), iota(y.shape, 1)
    for t in range(3):
        step = 1 << t
        row_bit, lane_bit = (row >> t) & 1, (lane >> (t + 4)) & 1
        from_below = roll(roll(y, -step, 0), B * step, 1)
        from_above = roll(roll(y, step, 0), -B * step, 1)
        y = jnp.where(row_bit == lane_bit, y, jnp.where(row_bit == 0, from_below, from_above))
    return jnp.concatenate([y[:64], y[64:]], axis=1)


def pick_lanes(x, lanes):
    return jnp.take_along_axis(x, lanes, axis=1, mode="promise_in_bounds")


def build_weights(taps_ref, shifted_ref, weights):
    taps = taps_ref[...]
    lane = iota((128, 128), 1)
    empty = (lane < 1) | (lane > 31)
    ahead = jnp.where(empty, 0.0, roll(taps, 1, 1)).T[0:48]
    flipped = jnp.where(empty, 0.0, pick_lanes(taps, jnp.clip(31 - lane, 0, 127))).T[0:48]
    group = iota((48, 128), 1) // B
    for number, source in enumerate((ahead, flipped)):
        pieces = []
        for tile in range(8):
            block = 8 * tile + group
            wanted = 46 - block if number == 0 else block - 16
            valid = (wanted >= 0) & (wanted <= 30)
            pieces.append(jnp.where(valid, pick_lanes(source, jnp.clip(wanted, 0, 30)), 0.0))
        base = jnp.concatenate(pieces, axis=1)
        column = iota(base.shape, 1) % B
        for t in range(4):
            base = jnp.where((column >> t) & 1 == 1, roll(base, 1 << t, 0), base)
        for shift in range(8):
            moved = roll(base, -B * shift, 1)
            high = moved.astype(BF16)
            shifted_ref[shift, 0:48] = high
            shifted_ref[shift, 48:96] = (moved - high.astype(F32)).astype(BF16)
        for part in range(2):
            weight = weights[2 * number + part]
            for di in (-1, 0, 1):
                for r in range(B):
                    start = 31 - 16 * di - r
                    lanes = 128 * (start // 8)
                    for dj in range(3):
                        rows = 48 * part + 16 * dj
                        weight[
                            LANES * (di + 1) + B * r : LANES * (di + 1) + B * r + B,
                            LANES * dj : LANES * dj + LANES,
                        ] = shifted_ref[start % 8, rows : rows + 16, lanes : lanes + LANES]


FIRST_UNIT = [(di, 0, low) for low in (False, True) for di in (-1, 0, 1)] + [(-1, -1, False), (0, -1, False)]
SECOND_UNIT = [(di, 1, low) for low in (False, True) for di in (-1, 0, 1)]
SECOND_UNIT += [(1, -1, False), (-1, -1, True), (0, -1, True), (1, -1, True)]


def correlate(field, high_weight, low_weight, first, count):
    def body(middle, right, left0, left1):
        queues = []
        for unit, products in enumerate((FIRST_UNIT, SECOND_UNIT)):
            queue = []
            for number, (di, dj, low) in enumerate(products):
                queue.append((unit, number % 2, di, dj, low, ((left0, left1)[unit], middle, right)[dj + 1]))
            queues.append(queue)
        for step in range(max(map(len, queues))):
            for queue in queues:
                if step < len(queue):
                    unit, register, di, dj, low, total = queue[step]
                    weight = low_weight if low else high_weight
                    tile = weight[LANES * (di + 1) : LANES * (di + 2), LANES * (dj + 1) : LANES * (dj + 2)]
                    pltpu.matmul_push_rhs(tile, staging_register=register, mxu_index=unit)
                    rows = pl.ds(first + PITCH * di, count)
                    pltpu.matmul_acc_lhs(total, field[0][rows, :], load_staged_rhs=register)
                    if not low:
                        pltpu.matmul_acc_lhs(total, field[1][rows, :])
        value = pltpu.matmul_pop(middle) + roll(pltpu.matmul_pop(right), -1, 0)
        return value + roll(pltpu.matmul_pop(left0) + pltpu.matmul_pop(left1), 1, 0)

    totals = [pltpu.ACC(unit)((count, LANES), F32) for unit in (0, 1, 0, 1)]
    return pl.run_scoped(body, *totals)


def smooth(source, first, count):
    x = source[pl.ds(first, count), :]
    above = source[pl.ds(first - PITCH, count), :]
    below = source[pl.ds(first + PITCH, count), :]
    wide = source[pl.ds(first - 8, count + 16), :]
    before = roll(wide, 1, 0)[8 : 8 + count]
    after = roll(wide, -1, 0)[8 : 8 + count]
    lane = iota(x.shape, 1)
    column = lane % B
    upper = roll(jnp.where(lane >= LANES - B, above, x), B, 1)
    lower = roll(jnp.where(lane < B, below, x), -B, 1)
    leftward = jnp.where(column == 0, roll(before, -(B - 1), 1), roll(x, 1, 1))
    rightward = jnp.where(column == B - 1, roll(after, B - 1, 1), roll(x, -1, 1))
    return PENALTY * (4.0 * x - upper - lower - leftward - rightward)


def own(value, first):
    return jnp.concatenate(
        [value[PITCH * r + 8 - first : PITCH * r + 24 - first] for r in range(4, 8)], axis=0
    )


def pack_sides(middle, left_ref, right_ref):
    sublane = iota((8, LANES), 0)
    for pair in range(2):
        first, second = 4 + 2 * pair, 5 + 2 * pair
        left_ref[pair] = jnp.where(sublane < 4, middle[first, 0:8], roll(middle[second, 0:8], 4, 0))
        right_ref[pair] = jnp.where(sublane < 4, roll(middle[first, 8:16], 4, 0), middle[second, 8:16])


def unpack(middle, from_left, from_right, flat, masked):
    sublane = iota((8, LANES), 0)
    for r in range(ROWS):
        right = jnp.zeros((8, LANES), F32)
        left = right
        if r >= 1:
            right = from_right[(r - 1) // 2]
            if (r - 1) % 2:
                right = roll(right, 4, 0)
        if r < 12:
            left = from_left[r // 2]
            if r % 2 == 0:
                left = roll(left, 4, 0)
        start = PITCH * r
        put(flat, start, masked(jnp.where(sublane < 4, right, left), start, 8))
        if r < 12:
            put(flat, start + 8, masked(middle[r], start + 8, 16))
        else:
            put(flat, start + 8, jnp.zeros((16, LANES), F32))


def image_kernel(
    grid, b_ref, guess_ref, kernel_ref, template_ref, residual_ref,
    x_mid, v_mid, b_mid, x_left, x_right, v_left, v_right, b_left, b_right,
    x_from_left, x_from_right, v_from_left, v_from_right, b_from_left, b_from_right,
    xf, xf_low, vf, vf_low, bf, rf, rf_low, t1, t1_low, t2, t2_low, mask_ref, taps_ref, shifted_ref, k_high, k_low, kt_high, kt_low,
    r0_own, v1_own, kr0_own, kv1_own, lr0_own, lv1_own,
    slots, pixels, far_sems, guess_tile, b_tile, taps_in, in_sems,
    x_send, x_recv, b_send, b_recv, v_send, v_recv, sum_send, sum_recv,
):
    n_rows, n_cols = grid
    loads = (
        pltpu.make_async_copy(guess_ref, guess_tile, in_sems.at[0]),
        pltpu.make_async_copy(b_ref, b_tile, in_sems.at[1]),
        pltpu.make_async_copy(kernel_ref, taps_in, in_sems.at[2]),
    )
    row, col = lax.axis_index("row"), lax.axis_index("col")

    def at(dr, dc):
        return lax.rem(row + dr + n_rows, n_rows), lax.rem(col + dc + n_cols, n_cols)

    for load in loads:
        load.start()
    barrier = pltpu.get_barrier_semaphore()
    partners = [at(dr, dc) for dr, dc in DIRECTIONS[:6]] + [at(d, 0) for d in range(1, n_rows)]
    for partner in partners:
        pl.semaphore_signal(barrier, inc=1, device_id=partner, device_id_type=MESH)

    def remote(source, target, send, recv, device):
        return pltpu.make_async_remote_copy(
            src_ref=source, dst_ref=target, send_sem=send, recv_sem=recv, device_id=device, device_id_type=MESH
        )

    def field_copies(middle, left, right, from_left, from_right, send, recv):
        copies = []
        for number, (dr, dc) in enumerate(DIRECTIONS):
            if dc == 0:
                source = middle.at[pl.ds(4, 4)]
                target = middle.at[pl.ds(4 - 4 * dr, 4)]
            else:
                source = right if dc == 1 else left
                target = (from_left if dc == 1 else from_right).at[pl.ds(2 - 2 * dr, 2)]
            copies.append(remote(source, target, send.at[number], recv.at[number], at(dr, dc)))
        return copies

    def spread(middle, first, x):
        for i in range(4):
            middle[first + i] = x[16 * i : 16 * i + 16]

    loads[0].wait()
    spread(x_mid, 4, swap_blocks(guess_tile[...]))
    pack_sides(x_mid, x_left, x_right)
    pl.semaphore_wait(barrier, n_rows - 1 + 6)

    x_copies = field_copies(x_mid, x_left, x_right, x_from_left, x_from_right, x_send, x_recv)
    for copy in x_copies:
        copy.start()
    loads[1].wait()
    spread(b_mid, 2, swap_blocks(b_tile[...]))
    sublane = iota((8, LANES), 0)
    left_part = right_part = jnp.zeros((8, LANES), F32)
    for i in range(4):
        here = sublane // 2 == i
        left_part = jnp.where(here, roll(b_mid[2 + i, 0:8], 2 * i, 0), left_part)
        right_part = jnp.where(here, roll(b_mid[2 + i, 8:16], 2 * i + 2, 0), right_part)
    b_left[...] = left_part
    b_right[...] = right_part

    b_copies = []
    for number, (dr, dc) in enumerate(DIRECTIONS):
        if dc == 0:
            source = b_mid.at[pl.ds(2 if dr == -1 else 4, 2)]
            target = b_mid.at[pl.ds(6 if dr == -1 else 0, 2)]
        else:
            source = b_right if dc == 1 else b_left
            target = (b_from_left if dc == 1 else b_from_right).at[1 - dr]
        b_copies.append(remote(source, target, b_send.at[number], b_recv.at[number], at(dr, dc)))
    for copy in b_copies:
        copy.start()

    taps_ref[...] = jnp.zeros_like(taps_ref)
    loads[2].wait()
    taps_ref[0:31, 0:31] = taps_in[...]
    build_weights(taps_ref, shifted_ref, (k_high, k_low, kt_high, kt_low))
    flat = iota((FLAT, LANES), 0)
    slot = flat % PITCH
    block_row = row * 4 + flat // PITCH - 4 - (slot < 4).astype(jnp.int32)
    block_col = col * 16 + slot - 8 + 24 * (slot < 4).astype(jnp.int32)
    inside = (block_row >= 0) & (block_row < 4 * n_rows) & (block_col >= 0) & (block_col < 16 * n_cols)
    mask_ref[...] = inside.astype(F32)

    def masked(value, first, count):
        return jnp.where(mask_ref[pl.ds(first, count), :] > 0.5, value, 0.0)

    distances = []
    while 2 << len(distances) <= n_cols // 2:
        distances.append(2 << len(distances))

    def greet(number):
        if number < len(distances):
            for d in sorted({distances[number], n_cols - distances[number]}):
                pl.semaphore_signal(far_sems.at[number], inc=1, device_id=at(0, d), device_id_type=MESH)

    def meet(number):
        if number < len(distances):
            pl.semaphore_wait(far_sems.at[number], 1 if 2 * distances[number] == n_cols else 2)

    def take_b():
        for copy in b_copies:
            copy.wait_recv()
        for r in range(2, 11):
            right = left = jnp.zeros((8, LANES), F32)
            if r >= 3:
                right = roll(b_from_right[(r - 1) // 4], -2 * ((r - 1) % 4), 0)
            if r < 10:
                left = roll(b_from_left[r // 4], 6 - 2 * (r % 4), 0)
            bf[PITCH * r : PITCH * r + 8] = jnp.where(sublane < 4, right, left)
            if r < 10:
                bf[PITCH * r + 8 : PITCH * r + 24] = b_mid[r - 2]

    def apply_twice(source, second, between):
        for first, count, keep, kept in ((24, 152, 24, 144), (160, 112, 168, 104)):
            value = correlate(source, k_high, k_low, first, count)[keep - first : keep - first + kept]
            put((t1, t1_low), keep, masked(value, keep, kept))
        between()
        smooth_source = []
        for first, count, keep, kept in ((48, 104, 48, 96), (136, 112, 144, 104)):
            value = correlate((t1, t1_low), kt_high, kt_low, first, count)[keep - first : keep - first + kept]
            smooth_source.append(smooth(source[0], keep, kept))
            value = value + smooth_source[-1]
            put(second, keep, masked(bf[pl.ds(keep, kept), :] - value if source[0] is xf else value, keep, kept))
        for first, count, keep, kept in ((72, 56, 72, 48), (112, 112, 120, 104)):
            value = correlate(second, k_high, k_low, first, count)[keep - first : keep - first + kept]
            put((t2, t2_low), keep, masked(value, keep, kept))
        return (
            own(t1[pl.ds(96, 104), :], 96),
            own(jnp.concatenate(smooth_source, axis=0), 48),
            own(t2[pl.ds(96, 104), :], 96),
            own(smooth(second[0], 96, 104), 96),
        )

    for copy in x_copies:
        copy.wait_recv()
    greet(0)
    unpack(x_mid, x_from_left, x_from_right, (xf, xf_low), masked)
    _, _, kr0, lr0 = apply_twice((xf, xf_low), (rf, rf_low), take_b)
    v1 = own(correlate((t2, t2_low), kt_high, kt_low, 96, 104), 96) + lr0
    spread(v_mid, 4, v1)
    pack_sides(v_mid, v_left, v_right)
    v_copies = field_copies(v_mid, v_left, v_right, v_from_left, v_from_right, v_send, v_recv)
    for copy in v_copies:
        copy.start()
    meet(0)
    greet(1)
    r0_own[...] = own(rf[pl.ds(96, 104), :], 96)
    v1_own[...] = v1
    kr0_own[...] = kr0
    lr0_own[...] = lr0

    for copy in v_copies:
        copy.wait_recv()
    meet(1)
    greet(2)
    unpack(v_mid, v_from_left, v_from_right, (vf, vf_low), masked)
    kv1, lv1, kv2, lv2 = apply_twice((vf, vf_low), (rf, rf_low), lambda: None)
    v2 = own(rf[pl.ds(96, 104), :], 96)

    def powers(zero, one, two):
        return two, one - two, zero - 2.0 * one + two

    r0, v1 = r0_own[...], v1_own[...]
    p = powers(r0, v1, v2)
    kp = powers(kr0_own[...], kv1, kv2)
    lp = powers(lr0_own[...], lv1, lv2)

    def lanes_of(x):
        total = x[0:8]
        for i in range(1, 8):
            total = total + x[8 * i : 8 * i + 8]
        total = total[:, :128] + total[:, 128:]
        return jnp.sum(total, axis=0, keepdims=True)

    moments = [lanes_of(p[2] * p[2])]
    for i, j in ((2, 2), (1, 2), (1, 1), (0, 1), (0, 0)):
        moments.append(lanes_of(kp[i] * kp[j] + p[i] * lp[j]))
    slot8 = iota((8, 128), 0)
    packed = jnp.zeros((8, 128), F32)
    for i, moment in enumerate(moments):
        packed = jnp.where(slot8 == i, moment, packed)
    mine = iota((8, 128), 1) == slot8
    packed = jnp.sum(packed, axis=1, keepdims=True)
    packed = jnp.sum(jnp.where(mine, packed, 0.0), axis=0, keepdims=True)

    meet(2)
    me = row * n_cols + col
    slots[me] = packed

    def hops(offset):
        z, y, x = offset[0] // 2, offset[1] // 4, offset[1] % 4
        return -(min(z, 4 - z) + min(y, 4 - y) + min(x, 4 - x))

    rows_at = [at(d, 0)[0] for d in range(n_rows)]
    cols_at = [at(0, d)[1] for d in range(n_cols)]
    offsets = [(dr, dc) for dr in range(n_rows) for dc in range(n_cols)][1:]
    for dr, dc in sorted(offsets, key=hops):
        remote(slots.at[me], slots.at[me], sum_send, sum_recv, (rows_at[dr], cols_at[dc])).start()
    others = pl.ds(0, n_rows * n_cols - 1)
    sums = remote(slots.at[others], slots.at[others], sum_send, sum_recv, at(1, 0))
    v3 = own(correlate((t2, t2_low), kt_high, kt_low, 96, 104), 96) + lv2
    for number, value in enumerate(p + powers(v1, v2, v3)):
        pixels[number] = swap_blocks(value)
    sums.wait_recv()
    total = jnp.sum(slots[...], axis=0)
    total = jnp.sum(jnp.where(mine, jnp.broadcast_to(total, (8, 128)), 0.0), axis=1, keepdims=True)
    b0, c1, c2, c3, c4, c5 = [total[i : i + 1, :] for i in range(6)]
    c = (None, c1, c2, c3, c4, c5)
    b = (b0, c1 + c2, c2 + c3, c3 + c4, c4 + c5)

    def square(q, m, base):
        return (
            q[0] * q[0] * m[base]
            + 2.0 * (q[0] * q[1]) * m[base + 1]
            + (q[1] * q[1] + 2.0 * (q[0] * q[2])) * m[base + 2]
            + 2.0 * (q[1] * q[2]) * m[base + 3]
            + q[2] * q[2] * m[base + 4]
        )

    def raised(q):
        return q[0], q[0] + q[1], q[1]

    one = (1.0, 2.0, 1.0)
    norm = square(one, b, 0)
    alpha0 = norm / square(one, c, 1)
    r1 = (1.0, 1.0 - alpha0)
    following = square(raised(r1), b, 0)
    beta0 = following / norm
    norm = following
    p1 = (r1[0] + beta0, r1[1] + beta0)
    p1_raised = raised(p1)
    alpha1 = norm / square(p1_raised, c, 1)
    r1_raised = raised(r1)
    r2 = (r1_raised[0], r1_raised[1] - alpha1 * p1[0], r1_raised[2] - alpha1 * p1[1])
    following = square(r2, b, 0)
    beta1 = following / norm
    p2 = tuple(r2[i] + beta1 * p1_raised[i] for i in range(3))
    alpha2 = following / square(p2, c, 1)
    steps = [alpha0 * one[i] + alpha1 * p1_raised[i] + alpha2 * p2[i] for i in range(3)]

    f0, f1, f2, af0, af1, af2 = [pixels[number] for number in range(6)]
    template_ref[...] = guess_tile[...] + steps[0] * f2 + steps[1] * f1 + steps[2] * f0
    residual = r2[0] * f2 + r2[1] * f1 + r2[2] * f0
    residual_ref[...] = residual - alpha2 * (p2[0] * af2 + p2[1] * af1 + p2[2] * af0)
    for copy in x_copies + b_copies + v_copies:
        copy.wait_send()
    sums.wait_send()


def on_device(grid, right_side, initial_guess, kernel):
    n_rows, n_cols = grid
    middle = pltpu.VMEM((12, 16, LANES), F32)
    b_middle = pltpu.VMEM((8, 16, LANES), F32)
    side = pltpu.VMEM((2, 8, LANES), F32)
    halo = pltpu.VMEM((6, 8, LANES), F32)
    b_side = pltpu.VMEM((8, LANES), F32)
    b_halo = pltpu.VMEM((3, 8, LANES), F32)
    flat = pltpu.VMEM((FLAT, LANES), F32)
    weight = pltpu.VMEM((3 * LANES, 3 * LANES), BF16)
    tile = pltpu.VMEM((64, LANES), F32)
    dma = pltpu.SemaphoreType.DMA
    shape = jax.ShapeDtypeStruct((64, LANES), F32)
    vmem = pl.BlockSpec(memory_space=pltpu.VMEM)

    def body(*refs):
        image_kernel(grid, *refs)

    return pl.pallas_call(
        body,
        out_shape=(shape, shape),
        in_specs=[pl.BlockSpec(memory_space=pltpu.HBM)] * 3,
        out_specs=(vmem, vmem),
        scratch_shapes=[
            middle, middle, b_middle, side, side, side, side, b_side, b_side,
            halo, halo, halo, halo, b_halo, b_halo,
            flat, flat, flat, flat, flat, flat, flat, flat, flat, flat, flat, flat,
            pltpu.VMEM((128, 128), F32), pltpu.VMEM((8, 96, 1024), BF16),
            weight, weight, weight, weight,
            tile, tile, tile, tile, tile, tile,
            pltpu.VMEM((n_rows * n_cols, 1, 128), F32), pltpu.VMEM((6, 64, LANES), F32), pltpu.SemaphoreType.REGULAR((3,)), tile, tile, pltpu.VMEM((31, 31), F32), dma((3,)),
            dma((8,)), dma((8,)), dma((8,)), dma((8,)), dma((8,)), dma((8,)),
            dma, dma,
        ],
        compiler_params=pltpu.CompilerParams(
            collective_id=0, has_side_effects=True, vmem_limit_bytes=16 * 1024 * 1024
        ),
    )(*(pltpu.with_memory_space_constraint(x, pltpu.HBM) for x in (right_side, initial_guess, kernel)))


def solution(mesh):
    grid = (mesh.shape["row"], mesh.shape["col"])
    tiles = P("row", "col")
    return jax.shard_map(
        lambda *arrays: on_device(grid, *arrays),
        mesh=mesh,
        in_specs=(tiles, tiles, P()),
        out_specs=(tiles, tiles),
        check_vma=False,
    )
```

```python
import jax
import jax.numpy as jnp
from jax import lax
from jax.experimental import pallas as pl
from jax.experimental.pallas import tpu as pltpu
from jax.sharding import PartitionSpec as P

PENALTY = 0.05
F32, BF16 = jnp.float32, jnp.bfloat16
B = 16
LANES = B * B
PITCH = 24
ROWS = 13
FLAT = ROWS * PITCH
DIRECTIONS = ((-1, -1), (-1, 1), (1, -1), (1, 1), (0, -1), (0, 1), (-1, 0), (1, 0))
MESH = pl.DeviceIdType.MESH


def iota(shape, dim):
    return lax.broadcasted_iota(jnp.int32, shape, dim)


def roll(x, shift, axis):
    return pltpu.roll(x, shift % x.shape[axis], axis)


def rounded(x):
    return x.astype(BF16).astype(F32)


def put(pair, first, value):
    rows = pl.ds(first, value.shape[0])
    pair[0][rows, :] = value
    pair[1][rows, :] = value - rounded(value)


def swap_blocks(x):
    top, bottom = [], []
    for i in range(4):
        upper, lower = x[16 * i : 16 * i + 8], x[16 * i + 8 : 16 * i + 16]
        top += [upper[:, :128], upper[:, 128:]]
        bottom += [lower[:, :128], lower[:, 128:]]
    y = jnp.concatenate(top + bottom, axis=0)
    row, lane = iota(y.shape, 0), iota(y.shape, 1)
    for t in range(3):
        step = 1 << t
        row_bit, lane_bit = (row >> t) & 1, (lane >> (t + 4)) & 1
        from_below = roll(roll(y, -step, 0), B * step, 1)
        from_above = roll(roll(y, step, 0), -B * step, 1)
        y = jnp.where(row_bit == lane_bit, y, jnp.where(row_bit == 0, from_below, from_above))
    return jnp.concatenate([y[:64], y[64:]], axis=1)


def pick_lanes(x, lanes):
    return jnp.take_along_axis(x, lanes, axis=1, mode="promise_in_bounds")


def build_weights(taps_ref, shifted_ref, weights):
    taps = taps_ref[...]
    lane = iota((128, 128), 1)
    empty = (lane < 1) | (lane > 31)
    ahead = jnp.where(empty, 0.0, roll(taps, 1, 1)).T[0:48]
    flipped = jnp.where(empty, 0.0, pick_lanes(taps, jnp.clip(31 - lane, 0, 127))).T[0:48]
    group = iota((48, 128), 1) // B
    for number, source in enumerate((ahead, flipped)):
        pieces = []
        for tile in range(8):
            block = 8 * tile + group
            wanted = 46 - block if number == 0 else block - 16
            valid = (wanted >= 0) & (wanted <= 30)
            pieces.append(jnp.where(valid, pick_lanes(source, jnp.clip(wanted, 0, 30)), 0.0))
        base = jnp.concatenate(pieces, axis=1)
        column = iota(base.shape, 1) % B
        for t in range(4):
            base = jnp.where((column >> t) & 1 == 1, roll(base, 1 << t, 0), base)
        for shift in range(8):
            moved = roll(base, -B * shift, 1)
            high = moved.astype(BF16)
            shifted_ref[shift, 0:48] = high
            shifted_ref[shift, 48:96] = (moved - high.astype(F32)).astype(BF16)
        for part in range(2):
            weight = weights[2 * number + part]
            for di in (-1, 0, 1):
                for r in range(B):
                    start = 31 - 16 * di - r
                    lanes = 128 * (start // 8)
                    for dj in range(3):
                        rows = 48 * part + 16 * dj
                        weight[
                            LANES * (di + 1) + B * r : LANES * (di + 1) + B * r + B,
                            LANES * dj : LANES * dj + LANES,
                        ] = shifted_ref[start % 8, rows : rows + 16, lanes : lanes + LANES]


FIRST_UNIT = [(di, 0, low) for low in (False, True) for di in (-1, 0, 1)] + [(-1, -1, False), (0, -1, False)]
SECOND_UNIT = [(di, 1, low) for low in (False, True) for di in (-1, 0, 1)]
SECOND_UNIT += [(1, -1, False), (-1, -1, True), (0, -1, True), (1, -1, True)]


def multiply(field, high_weight, low_weight, runs, finish):
    count = sum(run[1] for run in runs)

    def rows(part, di):
        return jnp.concatenate([part[pl.ds(first + PITCH * di, length), :] for first, length in runs], axis=0)

    def body(middle, right, left0, left1):
        queues = []
        for unit, products in enumerate((FIRST_UNIT, SECOND_UNIT)):
            queue = []
            for number, (di, dj, low) in enumerate(products):
                queue.append((unit, number % 2, di, dj, low, ((left0, left1)[unit], middle, right)[dj + 1]))
            queues.append(queue)
        for step in range(max(map(len, queues))):
            for queue in queues:
                if step < len(queue):
                    unit, register, di, dj, low, total = queue[step]
                    weight = low_weight if low else high_weight
                    tile = weight[LANES * (di + 1) : LANES * (di + 2), LANES * (dj + 1) : LANES * (dj + 2)]
                    pltpu.matmul_push_rhs(tile, staging_register=register, mxu_index=unit)
                    pltpu.matmul_acc_lhs(total, rows(field[0], di), load_staged_rhs=register)
                    if not low:
                        pltpu.matmul_acc_lhs(total, rows(field[1], di))
        return finish(
            pltpu.matmul_pop(middle), pltpu.matmul_pop(right), pltpu.matmul_pop(left0) + pltpu.matmul_pop(left1)
        )

    totals = [pltpu.ACC(unit)((count, LANES), F32) for unit in (0, 1, 0, 1)]
    return pl.run_scoped(body, *totals)


def combine(middle, right, left):
    return middle + roll(right, -1, 0) + roll(left, 1, 0)


def correlate(field, high_weight, low_weight, first, count):
    return multiply(field, high_weight, low_weight, [(first, count)], combine)


def smooth(source, first, count):
    x = source[pl.ds(first, count), :]
    above = source[pl.ds(first - PITCH, count), :]
    below = source[pl.ds(first + PITCH, count), :]
    wide = source[pl.ds(first - 8, count + 16), :]
    before = roll(wide, 1, 0)[8 : 8 + count]
    after = roll(wide, -1, 0)[8 : 8 + count]
    lane = iota(x.shape, 1)
    column = lane % B
    upper = roll(jnp.where(lane >= LANES - B, above, x), B, 1)
    lower = roll(jnp.where(lane < B, below, x), -B, 1)
    leftward = jnp.where(column == 0, roll(before, -(B - 1), 1), roll(x, 1, 1))
    rightward = jnp.where(column == B - 1, roll(after, B - 1, 1), roll(x, -1, 1))
    return PENALTY * (4.0 * x - upper - lower - leftward - rightward)


def own(value, first):
    return jnp.concatenate(
        [value[PITCH * r + 8 - first : PITCH * r + 24 - first] for r in range(4, 8)], axis=0
    )


def pack_sides(middle, left_ref, right_ref):
    sublane = iota((8, LANES), 0)
    for pair in range(2):
        first, second = 4 + 2 * pair, 5 + 2 * pair
        left_ref[pair] = jnp.where(sublane < 4, middle[first, 0:8], roll(middle[second, 0:8], 4, 0))
        right_ref[pair] = jnp.where(sublane < 4, roll(middle[first, 8:16], 4, 0), middle[second, 8:16])


def unpack_middle(middle, flat, masked):
    for r in range(12):
        start = PITCH * r + 8
        put(flat, start, masked(middle[r], start, 16))


def unpack_sides(from_left, from_right, flat, masked):
    sublane = iota((8, LANES), 0)
    for r in range(ROWS):
        right = left = jnp.zeros((8, LANES), F32)
        if r >= 1:
            right = from_right[(r - 1) // 2]
            if (r - 1) % 2:
                right = roll(right, 4, 0)
        if r < 12:
            left = from_left[r // 2]
            if r % 2 == 0:
                left = roll(left, 4, 0)
        put(flat, PITCH * r, masked(jnp.where(sublane < 4, right, left), PITCH * r, 8))


def image_kernel(
    grid, b_ref, guess_ref, kernel_ref, template_ref, residual_ref,
    x_mid, v_mid, b_mid, x_left, x_right, v_left, v_right, b_left, b_right,
    x_from_left, x_from_right, v_from_left, v_from_right, b_from_left, b_from_right,
    xf, xf_low, vf, vf_low, bf, rf, rf_low, t1, t1_low, t2, t2_low, y_middle, y_right, y_left, mask_ref, taps_ref, shifted_ref, k_high, k_low, kt_high, kt_low,
    r0_own, v1_own, kr0_own, kv1_own, lr0_own, lv1_own,
    slots, pixels, far_sems, guess_tile, b_tile, taps_in, in_sems,
    x_send, x_recv, b_send, b_recv, v_send, v_recv, sum_send, sum_recv,
):
    n_rows, n_cols = grid
    loads = (
        pltpu.make_async_copy(guess_ref, guess_tile, in_sems.at[0]),
        pltpu.make_async_copy(b_ref, b_tile, in_sems.at[1]),
        pltpu.make_async_copy(kernel_ref, taps_in, in_sems.at[2]),
    )
    row, col = lax.axis_index("row"), lax.axis_index("col")

    def at(dr, dc):
        return lax.rem(row + dr + n_rows, n_rows), lax.rem(col + dc + n_cols, n_cols)

    for load in loads:
        load.start()
    barrier = pltpu.get_barrier_semaphore()
    partners = [at(dr, dc) for dr, dc in DIRECTIONS[:6]] + [at(d, 0) for d in range(1, n_rows)]
    for partner in partners:
        pl.semaphore_signal(barrier, inc=1, device_id=partner, device_id_type=MESH)

    def remote(source, target, send, recv, device):
        return pltpu.make_async_remote_copy(
            src_ref=source, dst_ref=target, send_sem=send, recv_sem=recv, device_id=device, device_id_type=MESH
        )

    def field_copies(middle, left, right, from_left, from_right, send, recv):
        copies = []
        for number, (dr, dc) in enumerate(DIRECTIONS):
            if dc == 0:
                source = middle.at[pl.ds(4, 4)]
                target = middle.at[pl.ds(4 - 4 * dr, 4)]
            else:
                source = right if dc == 1 else left
                target = (from_left if dc == 1 else from_right).at[pl.ds(2 - 2 * dr, 2)]
            copies.append(remote(source, target, send.at[number], recv.at[number], at(dr, dc)))
        return copies

    def spread(middle, first, x):
        for i in range(4):
            middle[first + i] = x[16 * i : 16 * i + 16]

    loads[0].wait()
    spread(x_mid, 4, swap_blocks(guess_tile[...]))
    pack_sides(x_mid, x_left, x_right)
    pl.semaphore_wait(barrier, n_rows - 1 + 6)

    x_copies = field_copies(x_mid, x_left, x_right, x_from_left, x_from_right, x_send, x_recv)
    for copy in x_copies:
        copy.start()
    loads[1].wait()
    spread(b_mid, 2, swap_blocks(b_tile[...]))
    sublane = iota((8, LANES), 0)
    left_part = right_part = jnp.zeros((8, LANES), F32)
    for i in range(4):
        here = sublane // 2 == i
        left_part = jnp.where(here, roll(b_mid[2 + i, 0:8], 2 * i, 0), left_part)
        right_part = jnp.where(here, roll(b_mid[2 + i, 8:16], 2 * i + 2, 0), right_part)
    b_left[...] = left_part
    b_right[...] = right_part

    b_copies = []
    for number, (dr, dc) in enumerate(DIRECTIONS):
        if dc == 0:
            source = b_mid.at[pl.ds(2 if dr == -1 else 4, 2)]
            target = b_mid.at[pl.ds(6 if dr == -1 else 0, 2)]
        else:
            source = b_right if dc == 1 else b_left
            target = (b_from_left if dc == 1 else b_from_right).at[1 - dr]
        b_copies.append(remote(source, target, b_send.at[number], b_recv.at[number], at(dr, dc)))
    for copy in b_copies:
        copy.start()

    taps_ref[...] = jnp.zeros_like(taps_ref)
    loads[2].wait()
    taps_ref[0:31, 0:31] = taps_in[...]
    build_weights(taps_ref, shifted_ref, (k_high, k_low, kt_high, kt_low))
    flat = iota((FLAT, LANES), 0)
    slot = flat % PITCH
    block_row = row * 4 + flat // PITCH - 4 - (slot < 4).astype(jnp.int32)
    block_col = col * 16 + slot - 8 + 24 * (slot < 4).astype(jnp.int32)
    inside = (block_row >= 0) & (block_row < 4 * n_rows) & (block_col >= 0) & (block_col < 16 * n_cols)
    mask_ref[...] = inside.astype(F32)

    def masked(value, first, count):
        return jnp.where(mask_ref[pl.ds(first, count), :] > 0.5, value, 0.0)

    distances = []
    while 2 << len(distances) <= n_cols // 2:
        distances.append(2 << len(distances))

    def greet(number):
        if number < len(distances):
            for d in sorted({distances[number], n_cols - distances[number]}):
                pl.semaphore_signal(far_sems.at[number], inc=1, device_id=at(0, d), device_id_type=MESH)

    def meet(number):
        if number < len(distances):
            pl.semaphore_wait(far_sems.at[number], 1 if 2 * distances[number] == n_cols else 2)

    def take_b():
        for copy in b_copies:
            copy.wait_recv()
        for r in range(2, 11):
            right = left = jnp.zeros((8, LANES), F32)
            if r >= 3:
                right = roll(b_from_right[(r - 1) // 4], -2 * ((r - 1) % 4), 0)
            if r < 10:
                left = roll(b_from_left[r // 4], 6 - 2 * (r % 4), 0)
            bf[PITCH * r : PITCH * r + 8] = jnp.where(sublane < 4, right, left)
            if r < 10:
                bf[PITCH * r + 8 : PITCH * r + 24] = b_mid[r - 2]

    parts_refs = (y_middle, y_right, y_left)

    def receive(copies, middle, from_left, from_right, field, greeting):
        def keep(runs):
            def finish(*parts):
                for part, value in zip(parts_refs, parts):
                    start = 0
                    for first, length in runs:
                        part[pl.ds(first, length), :] = value[start : start + length]
                        start += length

            return finish

        for copy in copies[6:]:
            copy.wait_recv()
        unpack_middle(middle, field, masked)
        runs = [(PITCH * r + 8, 16) for r in range(1, 11)]
        multiply(field, k_high, k_low, runs, keep(runs))
        for copy in copies[:6]:
            copy.wait_recv()
        greeting()
        unpack_sides(from_left, from_right, field, masked)
        runs = [(PITCH * r, 8) for r in range(1, 12)]
        multiply(field, k_high, k_low, runs, keep(runs))
        value = combine(*[part[pl.ds(24, 248), :] for part in parts_refs])
        put((t1, t1_low), 24, masked(value, 24, 248))

    def apply_twice(source, second, between):
        between()
        smooth_source = []
        for first, count, keep, kept in ((48, 104, 48, 96), (136, 112, 144, 104)):
            value = correlate((t1, t1_low), kt_high, kt_low, first, count)[keep - first : keep - first + kept]
            smooth_source.append(smooth(source[0], keep, kept))
            value = value + smooth_source[-1]
            put(second, keep, masked(bf[pl.ds(keep, kept), :] - value if source[0] is xf else value, keep, kept))
        for first, count, keep, kept in ((72, 56, 72, 48), (112, 112, 120, 104)):
            value = correlate(second, k_high, k_low, first, count)[keep - first : keep - first + kept]
            put((t2, t2_low), keep, masked(value, keep, kept))
        return (
            own(t1[pl.ds(96, 104), :], 96),
            own(jnp.concatenate(smooth_source, axis=0), 48),
            own(t2[pl.ds(96, 104), :], 96),
            own(smooth(second[0], 96, 104), 96),
        )

    receive(x_copies, x_mid, x_from_left, x_from_right, (xf, xf_low), lambda: greet(0))
    _, _, kr0, lr0 = apply_twice((xf, xf_low), (rf, rf_low), take_b)
    v1 = own(correlate((t2, t2_low), kt_high, kt_low, 96, 104), 96) + lr0
    spread(v_mid, 4, v1)
    pack_sides(v_mid, v_left, v_right)
    v_copies = field_copies(v_mid, v_left, v_right, v_from_left, v_from_right, v_send, v_recv)
    for copy in v_copies:
        copy.start()
    meet(0)
    greet(1)
    r0_own[...] = own(rf[pl.ds(96, 104), :], 96)
    v1_own[...] = v1
    kr0_own[...] = kr0
    lr0_own[...] = lr0

    def meet_and_greet():
        meet(1)
        greet(2)

    receive(v_copies, v_mid, v_from_left, v_from_right, (vf, vf_low), meet_and_greet)
    kv1, lv1, kv2, lv2 = apply_twice((vf, vf_low), (rf, rf_low), lambda: None)
    v2 = own(rf[pl.ds(96, 104), :], 96)

    def powers(zero, one, two):
        return two, one - two, zero - 2.0 * one + two

    r0, v1 = r0_own[...], v1_own[...]
    p = powers(r0, v1, v2)
    kp = powers(kr0_own[...], kv1, kv2)
    lp = powers(lr0_own[...], lv1, lv2)

    def lanes_of(x):
        total = x[0:8]
        for i in range(1, 8):
            total = total + x[8 * i : 8 * i + 8]
        total = total[:, :128] + total[:, 128:]
        return jnp.sum(total, axis=0, keepdims=True)

    moments = [lanes_of(p[2] * p[2])]
    for i, j in ((2, 2), (1, 2), (1, 1), (0, 1), (0, 0)):
        moments.append(lanes_of(kp[i] * kp[j] + p[i] * lp[j]))
    slot8 = iota((8, 128), 0)
    packed = jnp.zeros((8, 128), F32)
    for i, moment in enumerate(moments):
        packed = jnp.where(slot8 == i, moment, packed)
    mine = iota((8, 128), 1) == slot8
    packed = jnp.sum(packed, axis=1, keepdims=True)
    packed = jnp.sum(jnp.where(mine, packed, 0.0), axis=0, keepdims=True)

    meet(2)
    me = row * n_cols + col
    slots[me] = packed

    def hops(offset):
        z, y, x = offset[0] // 2, offset[1] // 4, offset[1] % 4
        return -(min(z, 4 - z) + min(y, 4 - y) + min(x, 4 - x))

    rows_at = [at(d, 0)[0] for d in range(n_rows)]
    cols_at = [at(0, d)[1] for d in range(n_cols)]
    offsets = [(dr, dc) for dr in range(n_rows) for dc in range(n_cols)][1:]
    for dr, dc in sorted(offsets, key=hops):
        remote(slots.at[me], slots.at[me], sum_send, sum_recv, (rows_at[dr], cols_at[dc])).start()
    others = pl.ds(0, n_rows * n_cols - 1)
    sums = remote(slots.at[others], slots.at[others], sum_send, sum_recv, at(1, 0))
    v3 = own(correlate((t2, t2_low), kt_high, kt_low, 96, 104), 96) + lv2
    for number, value in enumerate(p + powers(v1, v2, v3)):
        pixels[number] = swap_blocks(value)
    sums.wait_recv()
    total = jnp.sum(slots[...], axis=0)
    total = jnp.sum(jnp.where(mine, jnp.broadcast_to(total, (8, 128)), 0.0), axis=1, keepdims=True)
    b0, c1, c2, c3, c4, c5 = [total[i : i + 1, :] for i in range(6)]
    c = (None, c1, c2, c3, c4, c5)
    b = (b0, c1 + c2, c2 + c3, c3 + c4, c4 + c5)

    def square(q, m, base):
        return (
            q[0] * q[0] * m[base]
            + 2.0 * (q[0] * q[1]) * m[base + 1]
            + (q[1] * q[1] + 2.0 * (q[0] * q[2])) * m[base + 2]
            + 2.0 * (q[1] * q[2]) * m[base + 3]
            + q[2] * q[2] * m[base + 4]
        )

    def raised(q):
        return q[0], q[0] + q[1], q[1]

    one = (1.0, 2.0, 1.0)
    norm = square(one, b, 0)
    alpha0 = norm / square(one, c, 1)
    r1 = (1.0, 1.0 - alpha0)
    following = square(raised(r1), b, 0)
    beta0 = following / norm
    norm = following
    p1 = (r1[0] + beta0, r1[1] + beta0)
    p1_raised = raised(p1)
    alpha1 = norm / square(p1_raised, c, 1)
    r1_raised = raised(r1)
    r2 = (r1_raised[0], r1_raised[1] - alpha1 * p1[0], r1_raised[2] - alpha1 * p1[1])
    following = square(r2, b, 0)
    beta1 = following / norm
    p2 = tuple(r2[i] + beta1 * p1_raised[i] for i in range(3))
    alpha2 = following / square(p2, c, 1)
    steps = [alpha0 * one[i] + alpha1 * p1_raised[i] + alpha2 * p2[i] for i in range(3)]

    f0, f1, f2, af0, af1, af2 = [pixels[number] for number in range(6)]
    template_ref[...] = guess_tile[...] + steps[0] * f2 + steps[1] * f1 + steps[2] * f0
    residual = r2[0] * f2 + r2[1] * f1 + r2[2] * f0
    residual_ref[...] = residual - alpha2 * (p2[0] * af2 + p2[1] * af1 + p2[2] * af0)
    for copy in x_copies + b_copies + v_copies:
        copy.wait_send()
    sums.wait_send()


def on_device(grid, right_side, initial_guess, kernel):
    n_rows, n_cols = grid
    middle = pltpu.VMEM((12, 16, LANES), F32)
    b_middle = pltpu.VMEM((8, 16, LANES), F32)
    side = pltpu.VMEM((2, 8, LANES), F32)
    halo = pltpu.VMEM((6, 8, LANES), F32)
    b_side = pltpu.VMEM((8, LANES), F32)
    b_halo = pltpu.VMEM((3, 8, LANES), F32)
    flat = pltpu.VMEM((FLAT, LANES), F32)
    weight = pltpu.VMEM((3 * LANES, 3 * LANES), BF16)
    tile = pltpu.VMEM((64, LANES), F32)
    dma = pltpu.SemaphoreType.DMA
    shape = jax.ShapeDtypeStruct((64, LANES), F32)
    vmem = pl.BlockSpec(memory_space=pltpu.VMEM)

    def body(*refs):
        image_kernel(grid, *refs)

    results = pl.pallas_call(
        body,
        out_shape=(shape, shape),
        in_specs=[pl.BlockSpec(memory_space=pltpu.HBM)] * 3,
        out_specs=(vmem, vmem),
        scratch_shapes=[
            middle, middle, b_middle, side, side, side, side, b_side, b_side,
            halo, halo, halo, halo, b_halo, b_halo,
            flat, flat, flat, flat, flat, flat, flat, flat, flat, flat, flat, flat, flat, flat, flat,
            pltpu.VMEM((128, 128), F32), pltpu.VMEM((8, 96, 1024), BF16),
            weight, weight, weight, weight,
            tile, tile, tile, tile, tile, tile,
            pltpu.VMEM((n_rows * n_cols, 1, 128), F32), pltpu.VMEM((6, 64, LANES), F32), pltpu.SemaphoreType.REGULAR((3,)), tile, tile, pltpu.VMEM((31, 31), F32), dma((3,)),
            dma((8,)), dma((8,)), dma((8,)), dma((8,)), dma((8,)), dma((8,)),
            dma, dma,
        ],
        compiler_params=pltpu.CompilerParams(
            collective_id=0, has_side_effects=True, vmem_limit_bytes=16 * 1024 * 1024
        ),
    )(*(pltpu.with_memory_space_constraint(x, pltpu.HBM) for x in (right_side, initial_guess, kernel)))

    def store(template_ref, residual_ref, template_out, residual_out, sems):
        copies = (
            pltpu.make_async_copy(template_ref, template_out, sems.at[0]),
            pltpu.make_async_copy(residual_ref, residual_out, sems.at[1]),
        )
        for copy in copies:
            copy.start()
        for copy in copies:
            copy.wait()

    return pl.pallas_call(
        store,
        out_shape=(shape, shape),
        in_specs=[vmem] * 2,
        out_specs=(pl.BlockSpec(memory_space=pltpu.HBM),) * 2,
        scratch_shapes=[dma((2,))],
        compiler_params=pltpu.CompilerParams(vmem_limit_bytes=1024 * 1024),
    )(*results)


def solution(mesh):
    grid = (mesh.shape["row"], mesh.shape["col"])
    tiles = P("row", "col")
    return jax.shard_map(
        lambda *arrays: on_device(grid, *arrays),
        mesh=mesh,
        in_specs=(tiles, tiles, P()),
        out_specs=(tiles, tiles),
        check_vma=False,
    )
```

```python
import jax
import jax.numpy as jnp
from jax import lax
from jax.experimental import pallas as pl
from jax.experimental.pallas import tpu as pltpu
from jax.sharding import PartitionSpec as P

PENALTY = 0.05
F32, BF16 = jnp.float32, jnp.bfloat16
B = 16
LANES = B * B
PITCH = 24
ROWS = 13
FLAT = ROWS * PITCH
DIRECTIONS = ((-1, -1), (-1, 1), (1, -1), (1, 1), (0, -1), (0, 1), (-1, 0), (1, 0))
MESH = pl.DeviceIdType.MESH


def iota(shape, dim):
    return lax.broadcasted_iota(jnp.int32, shape, dim)


def roll(x, shift, axis):
    return pltpu.roll(x, shift % x.shape[axis], axis)


def rounded(x):
    return x.astype(BF16).astype(F32)


def put(pair, first, value):
    rows = pl.ds(first, value.shape[0])
    pair[0][rows, :] = value
    pair[1][rows, :] = value - rounded(value)


def swap_blocks(x):
    top, bottom = [], []
    for i in range(4):
        upper, lower = x[16 * i : 16 * i + 8], x[16 * i + 8 : 16 * i + 16]
        top += [upper[:, :128], upper[:, 128:]]
        bottom += [lower[:, :128], lower[:, 128:]]
    y = jnp.concatenate(top + bottom, axis=0)
    row, lane = iota(y.shape, 0), iota(y.shape, 1)
    for t in range(3):
        step = 1 << t
        row_bit, lane_bit = (row >> t) & 1, (lane >> (t + 4)) & 1
        from_below = roll(roll(y, -step, 0), B * step, 1)
        from_above = roll(roll(y, step, 0), -B * step, 1)
        y = jnp.where(row_bit == lane_bit, y, jnp.where(row_bit == 0, from_below, from_above))
    return jnp.concatenate([y[:64], y[64:]], axis=1)


def pick_lanes(x, lanes):
    return jnp.take_along_axis(x, lanes, axis=1, mode="promise_in_bounds")


def build_weights(taps_ref, shifted_ref, weights):
    taps = taps_ref[...]
    lane = iota((128, 128), 1)
    empty = (lane < 1) | (lane > 31)
    ahead = jnp.where(empty, 0.0, roll(taps, 1, 1)).T[0:48]
    flipped = jnp.where(empty, 0.0, pick_lanes(taps, jnp.clip(31 - lane, 0, 127))).T[0:48]
    group = iota((48, 128), 1) // B
    for number, source in enumerate((ahead, flipped)):
        pieces = []
        for tile in range(8):
            block = 8 * tile + group
            wanted = 46 - block if number == 0 else block - 16
            valid = (wanted >= 0) & (wanted <= 30)
            pieces.append(jnp.where(valid, pick_lanes(source, jnp.clip(wanted, 0, 30)), 0.0))
        base = jnp.concatenate(pieces, axis=1)
        column = iota(base.shape, 1) % B
        for t in range(4):
            base = jnp.where((column >> t) & 1 == 1, roll(base, 1 << t, 0), base)
        for shift in range(8):
            moved = roll(base, -B * shift, 1)
            high = moved.astype(BF16)
            shifted_ref[shift, 0:48] = high
            shifted_ref[shift, 48:96] = (moved - high.astype(F32)).astype(BF16)
        for part in range(2):
            weight = weights[2 * number + part]
            for di in (-1, 0, 1):
                for r in range(B):
                    start = 31 - 16 * di - r
                    lanes = 128 * (start // 8)
                    for dj in range(3):
                        rows = 48 * part + 16 * dj
                        weight[
                            LANES * (di + 1) + B * r : LANES * (di + 1) + B * r + B,
                            LANES * dj : LANES * dj + LANES,
                        ] = shifted_ref[start % 8, rows : rows + 16, lanes : lanes + LANES]


FIRST_UNIT = [(di, 0, low) for low in (False, True) for di in (-1, 0, 1)] + [(-1, -1, False), (0, -1, False)]
SECOND_UNIT = [(di, 1, low) for low in (False, True) for di in (-1, 0, 1)]
SECOND_UNIT += [(1, -1, False), (-1, -1, True), (0, -1, True), (1, -1, True)]


def multiply(field, high_weight, low_weight, runs, finish):
    count = sum(run[1] for run in runs)

    def rows(part, di):
        return jnp.concatenate([part[pl.ds(first + PITCH * di, length), :] for first, length in runs], axis=0)

    def body(middle, right, left0, left1):
        queues = []
        for unit, products in enumerate((FIRST_UNIT, SECOND_UNIT)):
            queue = []
            for number, (di, dj, low) in enumerate(products):
                queue.append((unit, number % 2, di, dj, low, ((left0, left1)[unit], middle, right)[dj + 1]))
            queues.append(queue)
        for step in range(max(map(len, queues))):
            for queue in queues:
                if step < len(queue):
                    unit, register, di, dj, low, total = queue[step]
                    weight = low_weight if low else high_weight
                    tile = weight[LANES * (di + 1) : LANES * (di + 2), LANES * (dj + 1) : LANES * (dj + 2)]
                    pltpu.matmul_push_rhs(tile, staging_register=register, mxu_index=unit)
                    pltpu.matmul_acc_lhs(total, rows(field[0], di), load_staged_rhs=register)
                    if not low:
                        pltpu.matmul_acc_lhs(total, rows(field[1], di))
        return finish(
            pltpu.matmul_pop(middle), pltpu.matmul_pop(right), pltpu.matmul_pop(left0) + pltpu.matmul_pop(left1)
        )

    totals = [pltpu.ACC(unit)((count, LANES), F32) for unit in (0, 1, 0, 1)]
    return pl.run_scoped(body, *totals)


def combine(middle, right, left):
    return middle + roll(right, -1, 0) + roll(left, 1, 0)


def correlate(field, high_weight, low_weight, first, count):
    return multiply(field, high_weight, low_weight, [(first, count)], combine)


def smooth(source, first, count):
    x = source[pl.ds(first, count), :]
    above = source[pl.ds(first - PITCH, count), :]
    below = source[pl.ds(first + PITCH, count), :]
    wide = source[pl.ds(first - 8, count + 16), :]
    before = roll(wide, 1, 0)[8 : 8 + count]
    after = roll(wide, -1, 0)[8 : 8 + count]
    lane = iota(x.shape, 1)
    column = lane % B
    upper = roll(jnp.where(lane >= LANES - B, above, x), B, 1)
    lower = roll(jnp.where(lane < B, below, x), -B, 1)
    leftward = jnp.where(column == 0, roll(before, -(B - 1), 1), roll(x, 1, 1))
    rightward = jnp.where(column == B - 1, roll(after, B - 1, 1), roll(x, -1, 1))
    return PENALTY * (4.0 * x - upper - lower - leftward - rightward)


def own(value, first):
    return jnp.concatenate(
        [value[PITCH * r + 8 - first : PITCH * r + 24 - first] for r in range(4, 8)], axis=0
    )


def pack_sides(middle, left_ref, right_ref):
    sublane = iota((8, LANES), 0)
    for pair in range(2):
        first, second = 4 + 2 * pair, 5 + 2 * pair
        left_ref[pair] = jnp.where(sublane < 4, middle[first, 0:8], roll(middle[second, 0:8], 4, 0))
        right_ref[pair] = jnp.where(sublane < 4, roll(middle[first, 8:16], 4, 0), middle[second, 8:16])


def unpack_middle(middle, flat, masked):
    for r in range(12):
        start = PITCH * r + 8
        put(flat, start, masked(middle[r], start, 16))


def unpack_sides(from_left, from_right, flat, masked):
    sublane = iota((8, LANES), 0)
    for r in range(ROWS):
        right = left = jnp.zeros((8, LANES), F32)
        if r >= 1:
            right = from_right[(r - 1) // 2]
            if (r - 1) % 2:
                right = roll(right, 4, 0)
        if r < 12:
            left = from_left[r // 2]
            if r % 2 == 0:
                left = roll(left, 4, 0)
        put(flat, PITCH * r, masked(jnp.where(sublane < 4, right, left), PITCH * r, 8))


def image_kernel(
    grid, b_ref, guess_ref, kernel_ref, template_ref, residual_ref,
    x_mid, v_mid, b_mid, x_left, x_right, v_left, v_right, b_left, b_right,
    x_from_left, x_from_right, v_from_left, v_from_right, b_from_left, b_from_right,
    xf, xf_low, vf, vf_low, bf, rf, rf_low, t1, t1_low, t2, t2_low, y_middle, y_right, y_left, mask_ref, taps_ref, shifted_ref, k_high, k_low, kt_high, kt_low,
    r0_own, v1_own, kr0_own, kv1_own, lr0_own, lv1_own,
    slots, pixels, far_sems, guess_tile, b_tile, taps_in, in_sems,
    x_send, x_recv, b_send, b_recv, v_send, v_recv, sum_send, sum_recv,
):
    n_rows, n_cols = grid
    loads = (
        pltpu.make_async_copy(guess_ref, guess_tile, in_sems.at[0]),
        pltpu.make_async_copy(b_ref, b_tile, in_sems.at[1]),
        pltpu.make_async_copy(kernel_ref, taps_in, in_sems.at[2]),
    )
    row, col = lax.axis_index("row"), lax.axis_index("col")

    def at(dr, dc):
        return lax.rem(row + dr + n_rows, n_rows), lax.rem(col + dc + n_cols, n_cols)

    for load in loads:
        load.start()
    barrier = pltpu.get_barrier_semaphore()
    partners = [at(dr, dc) for dr, dc in DIRECTIONS[:6]] + [at(d, 0) for d in range(1, n_rows)]
    for partner in partners:
        pl.semaphore_signal(barrier, inc=1, device_id=partner, device_id_type=MESH)

    def remote(source, target, send, recv, device):
        return pltpu.make_async_remote_copy(
            src_ref=source, dst_ref=target, send_sem=send, recv_sem=recv, device_id=device, device_id_type=MESH
        )

    def field_copies(middle, left, right, from_left, from_right, send, recv):
        copies = []
        for number, (dr, dc) in enumerate(DIRECTIONS):
            if dc == 0:
                source = middle.at[pl.ds(4, 4)]
                target = middle.at[pl.ds(4 - 4 * dr, 4)]
            else:
                source = right if dc == 1 else left
                target = (from_left if dc == 1 else from_right).at[pl.ds(2 - 2 * dr, 2)]
            copies.append(remote(source, target, send.at[number], recv.at[number], at(dr, dc)))
        return copies

    def spread(middle, first, x):
        for i in range(4):
            middle[first + i] = x[16 * i : 16 * i + 16]

    loads[0].wait()
    spread(x_mid, 4, swap_blocks(guess_tile[...]))
    pack_sides(x_mid, x_left, x_right)
    pl.semaphore_wait(barrier, n_rows - 1 + 6)

    x_copies = field_copies(x_mid, x_left, x_right, x_from_left, x_from_right, x_send, x_recv)
    for copy in x_copies:
        copy.start()
    loads[1].wait()
    spread(b_mid, 2, swap_blocks(b_tile[...]))
    sublane = iota((8, LANES), 0)
    left_part = right_part = jnp.zeros((8, LANES), F32)
    for i in range(4):
        here = sublane // 2 == i
        left_part = jnp.where(here, roll(b_mid[2 + i, 0:8], 2 * i, 0), left_part)
        right_part = jnp.where(here, roll(b_mid[2 + i, 8:16], 2 * i + 2, 0), right_part)
    b_left[...] = left_part
    b_right[...] = right_part

    b_copies = []
    for number, (dr, dc) in enumerate(DIRECTIONS):
        if dc == 0:
            source = b_mid.at[pl.ds(2 if dr == -1 else 4, 2)]
            target = b_mid.at[pl.ds(6 if dr == -1 else 0, 2)]
        else:
            source = b_right if dc == 1 else b_left
            target = (b_from_left if dc == 1 else b_from_right).at[1 - dr]
        b_copies.append(remote(source, target, b_send.at[number], b_recv.at[number], at(dr, dc)))
    for copy in b_copies:
        copy.start()

    taps_ref[...] = jnp.zeros_like(taps_ref)
    loads[2].wait()
    taps_ref[0:31, 0:31] = taps_in[...]
    build_weights(taps_ref, shifted_ref, (k_high, k_low, kt_high, kt_low))
    flat = iota((FLAT, LANES), 0)
    slot = flat % PITCH
    block_row = row * 4 + flat // PITCH - 4 - (slot < 4).astype(jnp.int32)
    block_col = col * 16 + slot - 8 + 24 * (slot < 4).astype(jnp.int32)
    inside = (block_row >= 0) & (block_row < 4 * n_rows) & (block_col >= 0) & (block_col < 16 * n_cols)
    mask_ref[...] = inside.astype(F32)

    def masked(value, first, count):
        return jnp.where(mask_ref[pl.ds(first, count), :] > 0.5, value, 0.0)

    distances = []
    while 2 << len(distances) <= n_cols // 2:
        distances.append(2 << len(distances))

    def greet(number):
        if number < len(distances):
            for d in sorted({distances[number], n_cols - distances[number]}):
                pl.semaphore_signal(far_sems.at[number], inc=1, device_id=at(0, d), device_id_type=MESH)

    def meet(number):
        if number < len(distances):
            pl.semaphore_wait(far_sems.at[number], 1 if 2 * distances[number] == n_cols else 2)

    def take_b():
        for copy in b_copies:
            copy.wait_recv()
        for r in range(2, 11):
            right = left = jnp.zeros((8, LANES), F32)
            if r >= 3:
                right = roll(b_from_right[(r - 1) // 4], -2 * ((r - 1) % 4), 0)
            if r < 10:
                left = roll(b_from_left[r // 4], 6 - 2 * (r % 4), 0)
            bf[PITCH * r : PITCH * r + 8] = jnp.where(sublane < 4, right, left)
            if r < 10:
                bf[PITCH * r + 8 : PITCH * r + 24] = b_mid[r - 2]

    parts_refs = (y_middle, y_right, y_left)

    def receive(copies, middle, from_left, from_right, field, greeting, top, bottom):
        def keep(runs):
            def finish(*parts):
                for part, value in zip(parts_refs, parts):
                    start = 0
                    for first, length in runs:
                        part[pl.ds(first, length), :] = value[start : start + length]
                        start += length

            return finish

        for copy in copies[6:]:
            copy.wait_recv()
        unpack_middle(middle, field, masked)
        runs = [(PITCH * r + 8, 16) for r in range(top, bottom)]
        multiply(field, k_high, k_low, runs, keep(runs))
        for copy in copies[:6]:
            copy.wait_recv()
        greeting()
        unpack_sides(from_left, from_right, field, masked)
        runs = [(PITCH * r, 8) for r in range(top, bottom + 1)]
        multiply(field, k_high, k_low, runs, keep(runs))
        first, count = PITCH * top, PITCH * (bottom - top) + 8
        value = combine(*[part[pl.ds(first, count), :] for part in parts_refs])
        put((t1, t1_low), first, masked(value, first, count))

    blur, blur_back = (k_high, k_low), (kt_high, kt_low)
    blurred, second, blurred_second = (t1, t1_low), (rf, rf_low), (t2, t2_low)

    def stage(source, weights, target, runs, extra=None):
        value = multiply(source, *weights, [run[:2] for run in runs], combine)
        start = 0
        for first, count, keep, kept in runs:
            piece = value[start + keep - first : start + keep - first + kept]
            start += count
            if extra is not None:
                piece = extra(piece, keep, kept)
            put(target, keep, masked(piece, keep, kept))

    receive(x_copies, x_mid, x_from_left, x_from_right, (xf, xf_low), lambda: greet(0), 1, 11)
    take_b()

    def remainder(piece, keep, kept):
        return bf[pl.ds(keep, kept), :] - (piece + smooth(xf, keep, kept))

    stage(blurred, blur_back, second, [(48, 136, 48, 128)], remainder)
    stage(blurred, blur_back, second, [(168, 80, 176, 72)], remainder)
    stage(second, blur, blurred_second, [(72, 80, 72, 72)])
    stage(second, blur, blurred_second, [(136, 88, 144, 80)])
    kr0 = own(t2[pl.ds(96, 104), :], 96)
    lr0 = own(smooth(rf, 96, 104), 96)
    v1 = own(correlate((t2, t2_low), kt_high, kt_low, 96, 104), 96) + lr0
    spread(v_mid, 4, v1)
    pack_sides(v_mid, v_left, v_right)
    v_copies = field_copies(v_mid, v_left, v_right, v_from_left, v_from_right, v_send, v_recv)
    for copy in v_copies:
        copy.start()
    meet(0)
    greet(1)
    r0_own[...] = own(rf[pl.ds(96, 104), :], 96)
    v1_own[...] = v1
    kr0_own[...] = kr0
    lr0_own[...] = lr0

    def meet_and_greet():
        meet(1)
        greet(2)

    receive(v_copies, v_mid, v_from_left, v_from_right, (vf, vf_low), meet_and_greet, 2, 10)
    smooth_pieces = []

    def image(piece, keep, kept):
        smooth_pieces.append(smooth(vf, keep, kept))
        return piece + smooth_pieces[-1]

    stage(blurred, blur_back, second, [(64, 88, 72, 72)], image)
    stage(blurred, blur_back, second, [(136, 96, 144, 80)], image)
    stage(second, blur, blurred_second, [(96, 104, 104, 88)])
    kv1, kv2 = own(t1[pl.ds(96, 104), :], 96), own(t2[pl.ds(96, 104), :], 96)
    lv1, lv2 = own(jnp.concatenate(smooth_pieces, axis=0), 72), own(smooth(rf, 96, 104), 96)
    v2 = own(rf[pl.ds(96, 104), :], 96)

    def powers(zero, one, two):
        return two, one - two, zero - 2.0 * one + two

    r0, v1 = r0_own[...], v1_own[...]
    p = powers(r0, v1, v2)
    kp = powers(kr0_own[...], kv1, kv2)
    lp = powers(lr0_own[...], lv1, lv2)

    def lanes_of(x):
        total = x[0:8]
        for i in range(1, 8):
            total = total + x[8 * i : 8 * i + 8]
        total = total[:, :128] + total[:, 128:]
        return jnp.sum(total, axis=0, keepdims=True)

    moments = [lanes_of(p[2] * p[2])]
    for i, j in ((2, 2), (1, 2), (1, 1), (0, 1), (0, 0)):
        moments.append(lanes_of(kp[i] * kp[j] + p[i] * lp[j]))
    slot8 = iota((8, 128), 0)
    packed = jnp.zeros((8, 128), F32)
    for i, moment in enumerate(moments):
        packed = jnp.where(slot8 == i, moment, packed)
    mine = iota((8, 128), 1) == slot8
    packed = jnp.sum(packed, axis=1, keepdims=True)
    packed = jnp.sum(jnp.where(mine, packed, 0.0), axis=0, keepdims=True)

    meet(2)
    me = row * n_cols + col
    slots[me] = packed

    def hops(offset):
        z, y, x = offset[0] // 2, offset[1] // 4, offset[1] % 4
        return -(min(z, 4 - z) + min(y, 4 - y) + min(x, 4 - x))

    rows_at = [at(d, 0)[0] for d in range(n_rows)]
    cols_at = [at(0, d)[1] for d in range(n_cols)]
    offsets = [(dr, dc) for dr in range(n_rows) for dc in range(n_cols)][1:]
    for dr, dc in sorted(offsets, key=hops):
        remote(slots.at[me], slots.at[me], sum_send, sum_recv, (rows_at[dr], cols_at[dc])).start()
    others = pl.ds(0, n_rows * n_cols - 1)
    sums = remote(slots.at[others], slots.at[others], sum_send, sum_recv, at(1, 0))
    for copy in x_copies + b_copies + v_copies:
        copy.wait_send()
    stage((vf, vf_low), blur, blurred, [(24, 40, 24, 32), (232, 40, 240, 32)])
    stage(blurred, blur_back, second, [(48, 40, 48, 32), (208, 40, 216, 32)], image)
    stage(second, blur, blurred_second, [(72, 40, 72, 32), (184, 40, 192, 32)])
    v3 = own(correlate((t2, t2_low), kt_high, kt_low, 96, 104), 96) + lv2
    for number, value in enumerate(p + powers(v1, v2, v3)):
        pixels[number] = swap_blocks(value)
    sums.wait_recv()
    total = jnp.sum(slots[...], axis=0)
    total = jnp.sum(jnp.where(mine, jnp.broadcast_to(total, (8, 128)), 0.0), axis=1, keepdims=True)
    b0, c1, c2, c3, c4, c5 = [total[i : i + 1, :] for i in range(6)]
    c = (None, c1, c2, c3, c4, c5)
    b = (b0, c1 + c2, c2 + c3, c3 + c4, c4 + c5)

    def square(q, m, base):
        return (
            q[0] * q[0] * m[base]
            + 2.0 * (q[0] * q[1]) * m[base + 1]
            + (q[1] * q[1] + 2.0 * (q[0] * q[2])) * m[base + 2]
            + 2.0 * (q[1] * q[2]) * m[base + 3]
            + q[2] * q[2] * m[base + 4]
        )

    def raised(q):
        return q[0], q[0] + q[1], q[1]

    one = (1.0, 2.0, 1.0)
    norm = square(one, b, 0)
    alpha0 = norm / square(one, c, 1)
    r1 = (1.0, 1.0 - alpha0)
    following = square(raised(r1), b, 0)
    beta0 = following / norm
    norm = following
    p1 = (r1[0] + beta0, r1[1] + beta0)
    p1_raised = raised(p1)
    alpha1 = norm / square(p1_raised, c, 1)
    r1_raised = raised(r1)
    r2 = (r1_raised[0], r1_raised[1] - alpha1 * p1[0], r1_raised[2] - alpha1 * p1[1])
    following = square(r2, b, 0)
    beta1 = following / norm
    p2 = tuple(r2[i] + beta1 * p1_raised[i] for i in range(3))
    alpha2 = following / square(p2, c, 1)
    steps = [alpha0 * one[i] + alpha1 * p1_raised[i] + alpha2 * p2[i] for i in range(3)]

    f0, f1, f2, af0, af1, af2 = [pixels[number] for number in range(6)]
    template_ref[...] = guess_tile[...] + steps[0] * f2 + steps[1] * f1 + steps[2] * f0
    residual = r2[0] * f2 + r2[1] * f1 + r2[2] * f0
    residual_ref[...] = residual - alpha2 * (p2[0] * af2 + p2[1] * af1 + p2[2] * af0)
    sums.wait_send()


def on_device(grid, right_side, initial_guess, kernel):
    n_rows, n_cols = grid
    middle = pltpu.VMEM((12, 16, LANES), F32)
    b_middle = pltpu.VMEM((8, 16, LANES), F32)
    side = pltpu.VMEM((2, 8, LANES), F32)
    halo = pltpu.VMEM((6, 8, LANES), F32)
    b_side = pltpu.VMEM((8, LANES), F32)
    b_halo = pltpu.VMEM((3, 8, LANES), F32)
    flat = pltpu.VMEM((FLAT, LANES), F32)
    weight = pltpu.VMEM((3 * LANES, 3 * LANES), BF16)
    tile = pltpu.VMEM((64, LANES), F32)
    dma = pltpu.SemaphoreType.DMA
    shape = jax.ShapeDtypeStruct((64, LANES), F32)
    vmem = pl.BlockSpec(memory_space=pltpu.VMEM)

    def body(*refs):
        image_kernel(grid, *refs)

    results = pl.pallas_call(
        body,
        out_shape=(shape, shape),
        in_specs=[pl.BlockSpec(memory_space=pltpu.HBM)] * 3,
        out_specs=(vmem, vmem),
        scratch_shapes=[
            middle, middle, b_middle, side, side, side, side, b_side, b_side,
            halo, halo, halo, halo, b_halo, b_halo,
            flat, flat, flat, flat, flat, flat, flat, flat, flat, flat, flat, flat, flat, flat, flat,
            pltpu.VMEM((128, 128), F32), pltpu.VMEM((8, 96, 1024), BF16),
            weight, weight, weight, weight,
            tile, tile, tile, tile, tile, tile,
            pltpu.VMEM((n_rows * n_cols, 1, 128), F32), pltpu.VMEM((6, 64, LANES), F32), pltpu.SemaphoreType.REGULAR((3,)), tile, tile, pltpu.VMEM((31, 31), F32), dma((3,)),
            dma((8,)), dma((8,)), dma((8,)), dma((8,)), dma((8,)), dma((8,)),
            dma, dma,
        ],
        compiler_params=pltpu.CompilerParams(
            collective_id=0, has_side_effects=True, vmem_limit_bytes=16 * 1024 * 1024
        ),
    )(*(pltpu.with_memory_space_constraint(x, pltpu.HBM) for x in (right_side, initial_guess, kernel)))

    def store(template_ref, residual_ref, template_out, residual_out, sems):
        copies = (
            pltpu.make_async_copy(template_ref, template_out, sems.at[0]),
            pltpu.make_async_copy(residual_ref, residual_out, sems.at[1]),
        )
        for copy in copies:
            copy.start()
        for copy in copies:
            copy.wait()

    return pl.pallas_call(
        store,
        out_shape=(shape, shape),
        in_specs=[vmem] * 2,
        out_specs=(pl.BlockSpec(memory_space=pltpu.HBM),) * 2,
        scratch_shapes=[dma((2,))],
        compiler_params=pltpu.CompilerParams(vmem_limit_bytes=1024 * 1024),
    )(*results)


def solution(mesh):
    grid = (mesh.shape["row"], mesh.shape["col"])
    tiles = P("row", "col")
    return jax.shard_map(
        lambda *arrays: on_device(grid, *arrays),
        mesh=mesh,
        in_specs=(tiles, tiles, P()),
        out_specs=(tiles, tiles),
        check_vma=False,
    )
```

```python
import jax
import jax.numpy as jnp
from jax import lax
from jax.experimental import pallas as pl
from jax.experimental.pallas import tpu as pltpu
from jax.sharding import PartitionSpec as P

PENALTY = 0.05
F32, BF16 = jnp.float32, jnp.bfloat16
B = 16
LANES = B * B
PITCH = 24
ROWS = 13
FLAT = ROWS * PITCH
DIRECTIONS = ((-1, -1), (-1, 1), (1, -1), (1, 1), (0, -1), (0, 1), (-1, 0), (1, 0))
MESH = pl.DeviceIdType.MESH


def iota(shape, dim):
    return lax.broadcasted_iota(jnp.int32, shape, dim)


def roll(x, shift, axis):
    return pltpu.roll(x, shift % x.shape[axis], axis)


def rounded(x):
    return x.astype(BF16).astype(F32)


def put(pair, first, value):
    rows = pl.ds(first, value.shape[0])
    pair[0][rows, :] = value
    pair[1][rows, :] = value - rounded(value)


def swap_blocks(x):
    top, bottom = [], []
    for i in range(4):
        upper, lower = x[16 * i : 16 * i + 8], x[16 * i + 8 : 16 * i + 16]
        top += [upper[:, :128], upper[:, 128:]]
        bottom += [lower[:, :128], lower[:, 128:]]
    y = jnp.concatenate(top + bottom, axis=0)
    row, lane = iota(y.shape, 0), iota(y.shape, 1)
    for t in range(3):
        step = 1 << t
        row_bit, lane_bit = (row >> t) & 1, (lane >> (t + 4)) & 1
        from_below = roll(roll(y, -step, 0), B * step, 1)
        from_above = roll(roll(y, step, 0), -B * step, 1)
        y = jnp.where(row_bit == lane_bit, y, jnp.where(row_bit == 0, from_below, from_above))
    return jnp.concatenate([y[:64], y[64:]], axis=1)


def pick_lanes(x, lanes):
    return jnp.take_along_axis(x, lanes, axis=1, mode="promise_in_bounds")


def build_weights(taps_ref, shifted_ref, weights):
    taps = taps_ref[...]
    lane = iota((128, 128), 1)
    empty = (lane < 1) | (lane > 31)
    ahead = jnp.where(empty, 0.0, roll(taps, 1, 1)).T[0:48]
    flipped = jnp.where(empty, 0.0, pick_lanes(taps, jnp.clip(31 - lane, 0, 127))).T[0:48]
    group = iota((48, 128), 1) // B
    for number, source in enumerate((ahead, flipped)):
        pieces = []
        for tile in range(8):
            block = 8 * tile + group
            wanted = 46 - block if number == 0 else block - 16
            valid = (wanted >= 0) & (wanted <= 30)
            pieces.append(jnp.where(valid, pick_lanes(source, jnp.clip(wanted, 0, 30)), 0.0))
        base = jnp.concatenate(pieces, axis=1)
        column = iota(base.shape, 1) % B
        for t in range(4):
            base = jnp.where((column >> t) & 1 == 1, roll(base, 1 << t, 0), base)
        for shift in range(8):
            moved = roll(base, -B * shift, 1)
            high = moved.astype(BF16)
            shifted_ref[shift, 0:48] = high
            shifted_ref[shift, 48:96] = (moved - high.astype(F32)).astype(BF16)
        for part in range(2):
            weight = weights[2 * number + part]
            for di in (-1, 0, 1):
                for r in range(B):
                    start = 31 - 16 * di - r
                    lanes = 128 * (start // 8)
                    for dj in range(3):
                        rows = 48 * part + 16 * dj
                        weight[
                            LANES * (di + 1) + B * r : LANES * (di + 1) + B * r + B,
                            LANES * dj : LANES * dj + LANES,
                        ] = shifted_ref[start % 8, rows : rows + 16, lanes : lanes + LANES]


FIRST_UNIT = [(di, 0, low) for low in (False, True) for di in (-1, 0, 1)] + [(-1, -1, False), (0, -1, False)]
SECOND_UNIT = [(di, 1, low) for low in (False, True) for di in (-1, 0, 1)]
SECOND_UNIT += [(1, -1, False), (-1, -1, True), (0, -1, True), (1, -1, True)]


def multiply(field, high_weight, low_weight, runs, finish):
    count = sum(run[1] for run in runs)

    def rows(part, di):
        return jnp.concatenate([part[pl.ds(first + PITCH * di, length), :] for first, length in runs], axis=0)

    def body(middle, right, left0, left1):
        queues = []
        for unit, products in enumerate((FIRST_UNIT, SECOND_UNIT)):
            queue = []
            for number, (di, dj, low) in enumerate(products):
                queue.append((unit, number % 2, di, dj, low, ((left0, left1)[unit], middle, right)[dj + 1]))
            queues.append(queue)
        for step in range(max(map(len, queues))):
            for queue in queues:
                if step < len(queue):
                    unit, register, di, dj, low, total = queue[step]
                    weight = low_weight if low else high_weight
                    tile = weight[LANES * (di + 1) : LANES * (di + 2), LANES * (dj + 1) : LANES * (dj + 2)]
                    pltpu.matmul_push_rhs(tile, staging_register=register, mxu_index=unit)
                    pltpu.matmul_acc_lhs(total, rows(field[0], di), load_staged_rhs=register)
                    if not low:
                        pltpu.matmul_acc_lhs(total, rows(field[1], di))
        return finish(
            pltpu.matmul_pop(middle), pltpu.matmul_pop(right), pltpu.matmul_pop(left0) + pltpu.matmul_pop(left1)
        )

    totals = [pltpu.ACC(unit)((count, LANES), F32) for unit in (0, 1, 0, 1)]
    return pl.run_scoped(body, *totals)


def combine(middle, right, left):
    return middle + roll(right, -1, 0) + roll(left, 1, 0)


def correlate(field, high_weight, low_weight, first, count):
    return multiply(field, high_weight, low_weight, [(first, count)], combine)


def smooth(source, first, count):
    x = source[pl.ds(first, count), :]
    above = source[pl.ds(first - PITCH, count), :]
    below = source[pl.ds(first + PITCH, count), :]
    wide = source[pl.ds(first - 8, count + 16), :]
    before = roll(wide, 1, 0)[8 : 8 + count]
    after = roll(wide, -1, 0)[8 : 8 + count]
    lane = iota(x.shape, 1)
    column = lane % B
    upper = roll(jnp.where(lane >= LANES - B, above, x), B, 1)
    lower = roll(jnp.where(lane < B, below, x), -B, 1)
    leftward = jnp.where(column == 0, roll(before, -(B - 1), 1), roll(x, 1, 1))
    rightward = jnp.where(column == B - 1, roll(after, B - 1, 1), roll(x, -1, 1))
    return PENALTY * (4.0 * x - upper - lower - leftward - rightward)


def own(value, first):
    return jnp.concatenate(
        [value[PITCH * r + 8 - first : PITCH * r + 24 - first] for r in range(4, 8)], axis=0
    )


def pack_sides(middle, left_ref, right_ref):
    sublane = iota((8, LANES), 0)
    for pair in range(2):
        first, second = 4 + 2 * pair, 5 + 2 * pair
        left_ref[pair] = jnp.where(sublane < 4, middle[first, 0:8], roll(middle[second, 0:8], 4, 0))
        right_ref[pair] = jnp.where(sublane < 4, roll(middle[first, 8:16], 4, 0), middle[second, 8:16])


def unpack_middle(middle, flat, masked):
    for r in range(12):
        start = PITCH * r + 8
        put(flat, start, masked(middle[r], start, 16))


def unpack_sides(from_left, from_right, flat, masked):
    sublane = iota((8, LANES), 0)
    for r in range(ROWS):
        right = left = jnp.zeros((8, LANES), F32)
        if r >= 1:
            right = from_right[(r - 1) // 2]
            if (r - 1) % 2:
                right = roll(right, 4, 0)
        if r < 12:
            left = from_left[r // 2]
            if r % 2 == 0:
                left = roll(left, 4, 0)
        put(flat, PITCH * r, masked(jnp.where(sublane < 4, right, left), PITCH * r, 8))


def image_kernel(
    grid, b_ref, guess_ref, kernel_ref, template_ref, residual_ref,
    x_mid, v_mid, b_mid, x_left, x_right, v_left, v_right, b_left, b_right,
    x_from_left, x_from_right, v_from_left, v_from_right, b_from_left, b_from_right,
    xf, xf_low, vf, vf_low, bf, rf, rf_low, t1, t1_low, t2, t2_low, y_middle, y_right, y_left, mask_ref, taps_ref, shifted_ref, k_high, k_low, kt_high, kt_low,
    r0_own, v1_own, kr0_own, kv1_own, lr0_own, lv1_own,
    slots, pixels, far_sems, guess_tile, b_tile, taps_in, in_sems,
    x_send, x_recv, b_send, b_recv, v_send, v_recv, sum_send, sum_recv,
):
    n_rows, n_cols = grid
    loads = (
        pltpu.make_async_copy(guess_ref, guess_tile, in_sems.at[0]),
        pltpu.make_async_copy(b_ref, b_tile, in_sems.at[1]),
        pltpu.make_async_copy(kernel_ref, taps_in, in_sems.at[2]),
    )
    row, col = lax.axis_index("row"), lax.axis_index("col")

    def at(dr, dc):
        return lax.rem(row + dr + n_rows, n_rows), lax.rem(col + dc + n_cols, n_cols)

    for load in loads:
        load.start()
    barrier = pltpu.get_barrier_semaphore()
    def signal(semaphore, device):
        pl.semaphore_signal(semaphore, inc=1, device_id=device, device_id_type=MESH)

    def exists(dr, dc):
        inside = None
        for place, step, count in ((row, dr, n_rows), (col, dc, n_cols)):
            if step:
                test = place + step < count if step > 0 else place + step >= 0
                inside = test if inside is None else inside & test
        return inside

    for dr, dc in DIRECTIONS[:6]:
        pl.when(exists(dr, dc))(lambda dr=dr, dc=dc: signal(barrier, at(dr, dc)))
    for d in range(1, n_rows):
        signal(barrier, at(d, 0))
    greetings = n_rows - 1 + sum(exists(dr, dc).astype(jnp.int32) for dr, dc in DIRECTIONS[:6])

    def remote(source, target, send, recv, device):
        return pltpu.make_async_remote_copy(
            src_ref=source, dst_ref=target, send_sem=send, recv_sem=recv, device_id=device, device_id_type=MESH
        )

    def start(copies):
        for (dr, dc), copy in zip(DIRECTIONS, copies):
            pl.when(exists(dr, dc))(copy.start)

    def sent(copies):
        for (dr, dc), copy in zip(DIRECTIONS, copies):
            pl.when(exists(dr, dc))(copy.wait_send)

    def received(copies, numbers=range(8)):
        for number in numbers:
            dr, dc = DIRECTIONS[number]
            pl.when(exists(-dr, -dc))(copies[number].wait_recv)

    def field_copies(middle, left, right, from_left, from_right, send, recv):
        copies = []
        for number, (dr, dc) in enumerate(DIRECTIONS):
            if dc == 0:
                source = middle.at[pl.ds(4, 4)]
                target = middle.at[pl.ds(4 - 4 * dr, 4)]
            else:
                source = right if dc == 1 else left
                target = (from_left if dc == 1 else from_right).at[pl.ds(2 - 2 * dr, 2)]
            copies.append(remote(source, target, send.at[number], recv.at[number], at(dr, dc)))
        return copies

    def spread(middle, first, x):
        for i in range(4):
            middle[first + i] = x[16 * i : 16 * i + 16]

    loads[0].wait()
    spread(x_mid, 4, swap_blocks(guess_tile[...]))
    pack_sides(x_mid, x_left, x_right)
    pl.semaphore_wait(barrier, greetings)

    x_copies = field_copies(x_mid, x_left, x_right, x_from_left, x_from_right, x_send, x_recv)
    start(x_copies)
    loads[1].wait()
    spread(b_mid, 2, swap_blocks(b_tile[...]))
    sublane = iota((8, LANES), 0)
    left_part = right_part = jnp.zeros((8, LANES), F32)
    for i in range(4):
        here = sublane // 2 == i
        left_part = jnp.where(here, roll(b_mid[2 + i, 0:8], 2 * i, 0), left_part)
        right_part = jnp.where(here, roll(b_mid[2 + i, 8:16], 2 * i + 2, 0), right_part)
    b_left[...] = left_part
    b_right[...] = right_part

    b_copies = []
    for number, (dr, dc) in enumerate(DIRECTIONS):
        if dc == 0:
            source = b_mid.at[pl.ds(2 if dr == -1 else 4, 2)]
            target = b_mid.at[pl.ds(6 if dr == -1 else 0, 2)]
        else:
            source = b_right if dc == 1 else b_left
            target = (b_from_left if dc == 1 else b_from_right).at[1 - dr]
        b_copies.append(remote(source, target, b_send.at[number], b_recv.at[number], at(dr, dc)))
    start(b_copies)

    taps_ref[...] = jnp.zeros_like(taps_ref)
    loads[2].wait()
    taps_ref[0:31, 0:31] = taps_in[...]
    build_weights(taps_ref, shifted_ref, (k_high, k_low, kt_high, kt_low))
    flat = iota((FLAT, LANES), 0)
    slot = flat % PITCH
    block_row = row * 4 + flat // PITCH - 4 - (slot < 4).astype(jnp.int32)
    block_col = col * 16 + slot - 8 + 24 * (slot < 4).astype(jnp.int32)
    inside = (block_row >= 0) & (block_row < 4 * n_rows) & (block_col >= 0) & (block_col < 16 * n_cols)
    mask_ref[...] = inside.astype(F32)

    def masked(value, first, count):
        return jnp.where(mask_ref[pl.ds(first, count), :] > 0.5, value, 0.0)

    distances = []
    while (2 << len(distances)) - 1 < n_cols - 1:
        distances.append(2 << len(distances))

    def greet(number):
        if number < len(distances):
            for d in (distances[number], -distances[number]):
                pl.when(exists(0, d))(lambda d=d: signal(far_sems.at[number], at(0, d)))

    def meet(number):
        if number < len(distances):
            d = distances[number]
            count = exists(0, d).astype(jnp.int32) + exists(0, -d).astype(jnp.int32)
            pl.semaphore_wait(far_sems.at[number], count)

    def take_b():
        received(b_copies)
        for r in range(2, 11):
            right = left = jnp.zeros((8, LANES), F32)
            if r >= 3:
                right = roll(b_from_right[(r - 1) // 4], -2 * ((r - 1) % 4), 0)
            if r < 10:
                left = roll(b_from_left[r // 4], 6 - 2 * (r % 4), 0)
            bf[PITCH * r : PITCH * r + 8] = jnp.where(sublane < 4, right, left)
            if r < 10:
                bf[PITCH * r + 8 : PITCH * r + 24] = b_mid[r - 2]

    parts_refs = (y_middle, y_right, y_left)

    def receive(copies, middle, from_left, from_right, field, greeting, top, bottom):
        def keep(runs):
            def finish(*parts):
                for part, value in zip(parts_refs, parts):
                    start = 0
                    for first, length in runs:
                        part[pl.ds(first, length), :] = value[start : start + length]
                        start += length

            return finish

        received(copies, range(6, 8))
        unpack_middle(middle, field, masked)
        runs = [(PITCH * r + 8, 16) for r in range(top, bottom)]
        multiply(field, k_high, k_low, runs, keep(runs))
        received(copies, range(6))
        greeting()
        unpack_sides(from_left, from_right, field, masked)
        runs = [(PITCH * r, 8) for r in range(top, bottom + 1)]
        multiply(field, k_high, k_low, runs, keep(runs))
        first, count = PITCH * top, PITCH * (bottom - top) + 8
        value = combine(*[part[pl.ds(first, count), :] for part in parts_refs])
        put((t1, t1_low), first, masked(value, first, count))

    blur, blur_back = (k_high, k_low), (kt_high, kt_low)
    blurred, second, blurred_second = (t1, t1_low), (rf, rf_low), (t2, t2_low)

    def stage(source, weights, target, runs, extra=None):
        value = multiply(source, *weights, [run[:2] for run in runs], combine)
        start = 0
        for first, count, keep, kept in runs:
            piece = value[start + keep - first : start + keep - first + kept]
            start += count
            if extra is not None:
                piece = extra(piece, keep, kept)
            put(target, keep, masked(piece, keep, kept))

    receive(x_copies, x_mid, x_from_left, x_from_right, (xf, xf_low), lambda: greet(0), 1, 11)
    take_b()

    def remainder(piece, keep, kept):
        return bf[pl.ds(keep, kept), :] - (piece + smooth(xf, keep, kept))

    stage(blurred, blur_back, second, [(48, 136, 48, 128)], remainder)
    stage(blurred, blur_back, second, [(168, 80, 176, 72)], remainder)
    stage(second, blur, blurred_second, [(72, 80, 72, 72)])
    stage(second, blur, blurred_second, [(136, 88, 144, 80)])
    kr0 = own(t2[pl.ds(96, 104), :], 96)
    lr0 = own(smooth(rf, 96, 104), 96)
    v1 = own(correlate((t2, t2_low), kt_high, kt_low, 96, 104), 96) + lr0
    spread(v_mid, 4, v1)
    pack_sides(v_mid, v_left, v_right)
    v_copies = field_copies(v_mid, v_left, v_right, v_from_left, v_from_right, v_send, v_recv)
    start(v_copies)
    meet(0)
    greet(1)
    r0_own[...] = own(rf[pl.ds(96, 104), :], 96)
    v1_own[...] = v1
    kr0_own[...] = kr0
    lr0_own[...] = lr0

    def meet_and_greet():
        meet(1)
        greet(2)

    receive(v_copies, v_mid, v_from_left, v_from_right, (vf, vf_low), meet_and_greet, 2, 10)
    smooth_pieces = []

    def image(piece, keep, kept):
        smooth_pieces.append(smooth(vf, keep, kept))
        return piece + smooth_pieces[-1]

    stage(blurred, blur_back, second, [(64, 88, 72, 72)], image)
    stage(blurred, blur_back, second, [(136, 96, 144, 80)], image)
    stage(second, blur, blurred_second, [(96, 104, 104, 88)])
    kv1, kv2 = own(t1[pl.ds(96, 104), :], 96), own(t2[pl.ds(96, 104), :], 96)
    lv1, lv2 = own(jnp.concatenate(smooth_pieces, axis=0), 72), own(smooth(rf, 96, 104), 96)
    v2 = own(rf[pl.ds(96, 104), :], 96)

    def powers(zero, one, two):
        return two, one - two, zero - 2.0 * one + two

    r0, v1 = r0_own[...], v1_own[...]
    p = powers(r0, v1, v2)
    kp = powers(kr0_own[...], kv1, kv2)
    lp = powers(lr0_own[...], lv1, lv2)

    def lanes_of(x):
        total = x[0:8]
        for i in range(1, 8):
            total = total + x[8 * i : 8 * i + 8]
        total = total[:, :128] + total[:, 128:]
        return jnp.sum(total, axis=0, keepdims=True)

    moments = [lanes_of(p[2] * p[2])]
    for i, j in ((2, 2), (1, 2), (1, 1), (0, 1), (0, 0)):
        moments.append(lanes_of(kp[i] * kp[j] + p[i] * lp[j]))
    slot8 = iota((8, 128), 0)
    packed = jnp.zeros((8, 128), F32)
    for i, moment in enumerate(moments):
        packed = jnp.where(slot8 == i, moment, packed)
    mine = iota((8, 128), 1) == slot8
    packed = jnp.sum(packed, axis=1, keepdims=True)
    packed = jnp.sum(jnp.where(mine, packed, 0.0), axis=0, keepdims=True)

    meet(2)
    me = row * n_cols + col
    slots[me] = packed

    def hops(offset):
        z, y, x = offset[0] // 2, offset[1] // 4, offset[1] % 4
        return -(min(z, 4 - z) + min(y, 4 - y) + min(x, 4 - x))

    rows_at = [at(d, 0)[0] for d in range(n_rows)]
    cols_at = [at(0, d)[1] for d in range(n_cols)]
    offsets = [(dr, dc) for dr in range(n_rows) for dc in range(n_cols)][1:]
    for dr, dc in sorted(offsets, key=hops):
        remote(slots.at[me], slots.at[me], sum_send, sum_recv, (rows_at[dr], cols_at[dc])).start()
    others = pl.ds(0, n_rows * n_cols - 1)
    sums = remote(slots.at[others], slots.at[others], sum_send, sum_recv, at(1, 0))
    for copies in (x_copies, b_copies, v_copies):
        sent(copies)
    stage((vf, vf_low), blur, blurred, [(24, 40, 24, 32), (232, 40, 240, 32)])
    stage(blurred, blur_back, second, [(48, 40, 48, 32), (208, 40, 216, 32)], image)
    stage(second, blur, blurred_second, [(72, 40, 72, 32), (184, 40, 192, 32)])
    v3 = own(correlate((t2, t2_low), kt_high, kt_low, 96, 104), 96) + lv2
    for number, value in enumerate(p + powers(v1, v2, v3)):
        pixels[number] = swap_blocks(value)
    sums.wait_recv()
    groups = [jnp.sum(slots[pl.ds(start, n_cols)], axis=0) for start in range(0, n_rows * n_cols, n_cols)]
    while len(groups) > 1:
        groups = [sum(groups[i : i + 2][1:], groups[i]) for i in range(0, len(groups), 2)]
    total = groups[0]
    total = jnp.sum(jnp.where(mine, jnp.broadcast_to(total, (8, 128)), 0.0), axis=1, keepdims=True)
    b0, c1, c2, c3, c4, c5 = [total[i : i + 1, :] for i in range(6)]
    c = (None, c1, c2, c3, c4, c5)
    b = (b0, c1 + c2, c2 + c3, c3 + c4, c4 + c5)

    def square(q, m, base):
        return (
            q[0] * q[0] * m[base]
            + 2.0 * (q[0] * q[1]) * m[base + 1]
            + (q[1] * q[1] + 2.0 * (q[0] * q[2])) * m[base + 2]
            + 2.0 * (q[1] * q[2]) * m[base + 3]
            + q[2] * q[2] * m[base + 4]
        )

    def raised(q):
        return q[0], q[0] + q[1], q[1]

    one = (1.0, 2.0, 1.0)
    norm = square(one, b, 0)
    alpha0 = norm / square(one, c, 1)
    r1 = (1.0, 1.0 - alpha0)
    following = square(raised(r1), b, 0)
    beta0 = following / norm
    norm = following
    p1 = (r1[0] + beta0, r1[1] + beta0)
    p1_raised = raised(p1)
    alpha1 = norm / square(p1_raised, c, 1)
    r1_raised = raised(r1)
    r2 = (r1_raised[0], r1_raised[1] - alpha1 * p1[0], r1_raised[2] - alpha1 * p1[1])
    following = square(r2, b, 0)
    beta1 = following / norm
    p2 = tuple(r2[i] + beta1 * p1_raised[i] for i in range(3))
    alpha2 = following / square(p2, c, 1)
    steps = [alpha0 * one[i] + alpha1 * p1_raised[i] + alpha2 * p2[i] for i in range(3)]

    f0, f1, f2, af0, af1, af2 = [pixels[number] for number in range(6)]
    template_ref[...] = guess_tile[...] + steps[0] * f2 + steps[1] * f1 + steps[2] * f0
    residual = r2[0] * f2 + r2[1] * f1 + r2[2] * f0
    residual_ref[...] = residual - alpha2 * (p2[0] * af2 + p2[1] * af1 + p2[2] * af0)
    sums.wait_send()


def on_device(grid, right_side, initial_guess, kernel):
    n_rows, n_cols = grid
    middle = pltpu.VMEM((12, 16, LANES), F32)
    b_middle = pltpu.VMEM((8, 16, LANES), F32)
    side = pltpu.VMEM((2, 8, LANES), F32)
    halo = pltpu.VMEM((6, 8, LANES), F32)
    b_side = pltpu.VMEM((8, LANES), F32)
    b_halo = pltpu.VMEM((3, 8, LANES), F32)
    flat = pltpu.VMEM((FLAT, LANES), F32)
    weight = pltpu.VMEM((3 * LANES, 3 * LANES), BF16)
    tile = pltpu.VMEM((64, LANES), F32)
    dma = pltpu.SemaphoreType.DMA
    shape = jax.ShapeDtypeStruct((64, LANES), F32)
    vmem = pl.BlockSpec(memory_space=pltpu.VMEM)

    def body(*refs):
        image_kernel(grid, *refs)

    results = pl.pallas_call(
        body,
        out_shape=(shape, shape),
        in_specs=[pl.BlockSpec(memory_space=pltpu.HBM)] * 3,
        out_specs=(vmem, vmem),
        scratch_shapes=[
            middle, middle, b_middle, side, side, side, side, b_side, b_side,
            halo, halo, halo, halo, b_halo, b_halo,
            flat, flat, flat, flat, flat, flat, flat, flat, flat, flat, flat, flat, flat, flat, flat,
            pltpu.VMEM((128, 128), F32), pltpu.VMEM((8, 96, 1024), BF16),
            weight, weight, weight, weight,
            tile, tile, tile, tile, tile, tile,
            pltpu.VMEM((n_rows * n_cols, 1, 128), F32), pltpu.VMEM((6, 64, LANES), F32), pltpu.SemaphoreType.REGULAR((3,)), tile, tile, pltpu.VMEM((31, 31), F32), dma((3,)),
            dma((8,)), dma((8,)), dma((8,)), dma((8,)), dma((8,)), dma((8,)),
            dma, dma,
        ],
        compiler_params=pltpu.CompilerParams(
            collective_id=0, has_side_effects=True, vmem_limit_bytes=16 * 1024 * 1024
        ),
    )(*(pltpu.with_memory_space_constraint(x, pltpu.HBM) for x in (right_side, initial_guess, kernel)))

    def store(template_ref, residual_ref, template_out, residual_out, sems):
        copies = (
            pltpu.make_async_copy(template_ref, template_out, sems.at[0]),
            pltpu.make_async_copy(residual_ref, residual_out, sems.at[1]),
        )
        for copy in copies:
            copy.start()
        for copy in copies:
            copy.wait()

    return pl.pallas_call(
        store,
        out_shape=(shape, shape),
        in_specs=[vmem] * 2,
        out_specs=(pl.BlockSpec(memory_space=pltpu.HBM),) * 2,
        scratch_shapes=[dma((2,))],
        compiler_params=pltpu.CompilerParams(vmem_limit_bytes=1024 * 1024),
    )(*results)


def solution(mesh):
    grid = (mesh.shape["row"], mesh.shape["col"])
    tiles = P("row", "col")
    return jax.shard_map(
        lambda *arrays: on_device(grid, *arrays),
        mesh=mesh,
        in_specs=(tiles, tiles, P()),
        out_specs=(tiles, tiles),
        check_vma=False,
    )
```

```python
import jax
import jax.numpy as jnp
from jax import lax
from jax.experimental import pallas as pl
from jax.experimental.pallas import tpu as pltpu
from jax.sharding import PartitionSpec as P

PENALTY = 0.05
F32, BF16 = jnp.float32, jnp.bfloat16
B = 16
LANES = B * B
PITCH = 24
ROWS = 13
FLAT = ROWS * PITCH
DIRECTIONS = ((-1, -1), (-1, 1), (1, -1), (1, 1), (0, -1), (0, 1), (-1, 0), (1, 0))
MESH = pl.DeviceIdType.MESH


def iota(shape, dim):
    return lax.broadcasted_iota(jnp.int32, shape, dim)


def roll(x, shift, axis):
    return pltpu.roll(x, shift % x.shape[axis], axis)


def rounded(x):
    return x.astype(BF16).astype(F32)


def put(pair, first, value):
    rows = pl.ds(first, value.shape[0])
    pair[0][rows, :] = value
    pair[1][rows, :] = value - rounded(value)


def swap_blocks(x):
    top, bottom = [], []
    for i in range(4):
        upper, lower = x[16 * i : 16 * i + 8], x[16 * i + 8 : 16 * i + 16]
        top += [upper[:, :128], upper[:, 128:]]
        bottom += [lower[:, :128], lower[:, 128:]]
    y = jnp.concatenate(top + bottom, axis=0)
    row, lane = iota(y.shape, 0), iota(y.shape, 1)
    for t in range(3):
        step = 1 << t
        row_bit, lane_bit = (row >> t) & 1, (lane >> (t + 4)) & 1
        from_below = roll(roll(y, -step, 0), B * step, 1)
        from_above = roll(roll(y, step, 0), -B * step, 1)
        y = jnp.where(row_bit == lane_bit, y, jnp.where(row_bit == 0, from_below, from_above))
    return jnp.concatenate([y[:64], y[64:]], axis=1)


def pick_lanes(x, lanes):
    return jnp.take_along_axis(x, lanes, axis=1, mode="promise_in_bounds")


def build_weights(taps_ref, shifted_ref, weights):
    taps = taps_ref[...]
    lane = iota((128, 128), 1)
    empty = (lane < 1) | (lane > 31)
    ahead = jnp.where(empty, 0.0, roll(taps, 1, 1)).T[0:48]
    flipped = jnp.where(empty, 0.0, pick_lanes(taps, jnp.clip(31 - lane, 0, 127))).T[0:48]
    group = iota((48, 128), 1) // B
    for number, source in enumerate((ahead, flipped)):
        pieces = []
        for tile in range(8):
            block = 8 * tile + group
            wanted = 46 - block if number == 0 else block - 16
            valid = (wanted >= 0) & (wanted <= 30)
            pieces.append(jnp.where(valid, pick_lanes(source, jnp.clip(wanted, 0, 30)), 0.0))
        base = jnp.concatenate(pieces, axis=1)
        column = iota(base.shape, 1) % B
        for t in range(4):
            base = jnp.where((column >> t) & 1 == 1, roll(base, 1 << t, 0), base)
        for shift in range(8):
            moved = roll(base, -B * shift, 1)
            high = moved.astype(BF16)
            shifted_ref[shift, 0:48] = high
            shifted_ref[shift, 48:96] = (moved - high.astype(F32)).astype(BF16)
        for part in range(2):
            weight = weights[2 * number + part]
            for di in (-1, 0, 1):
                for r in range(B):
                    start = 31 - 16 * di - r
                    lanes = 128 * (start // 8)
                    for dj in range(3):
                        rows = 48 * part + 16 * dj
                        weight[
                            LANES * (di + 1) + B * r : LANES * (di + 1) + B * r + B,
                            LANES * dj : LANES * dj + LANES,
                        ] = shifted_ref[start % 8, rows : rows + 16, lanes : lanes + LANES]


FIRST_UNIT = [(di, 0, low) for low in (False, True) for di in (-1, 0, 1)]
FIRST_UNIT += [(-1, -1, False), (-1, -1, True), (0, -1, True)]
SECOND_UNIT = [(di, 1, low) for low in (False, True) for di in (-1, 0, 1)]
SECOND_UNIT += [(0, -1, False), (1, -1, False), (1, -1, True)]


def multiply(field, high_weight, low_weight, runs, finish):
    count = sum(run[1] for run in runs)

    def rows(part, di):
        return jnp.concatenate([part[pl.ds(first + PITCH * di, length), :] for first, length in runs], axis=0)

    def body(middle, right, left0, left1):
        queues = []
        for unit, products in enumerate((FIRST_UNIT, SECOND_UNIT)):
            queue = []
            for number, (di, dj, low) in enumerate(products):
                queue.append((unit, number % 2, di, dj, low, ((left0, left1)[unit], middle, right)[dj + 1]))
            queues.append(queue)
        for step in range(max(map(len, queues))):
            for queue in queues:
                if step < len(queue):
                    unit, register, di, dj, low, total = queue[step]
                    weight = low_weight if low else high_weight
                    tile = weight[LANES * (di + 1) : LANES * (di + 2), LANES * (dj + 1) : LANES * (dj + 2)]
                    pltpu.matmul_push_rhs(tile, staging_register=register, mxu_index=unit)
                    pltpu.matmul_acc_lhs(total, rows(field[0], di), load_staged_rhs=register)
                    if not low:
                        pltpu.matmul_acc_lhs(total, rows(field[1], di))
        return finish(
            pltpu.matmul_pop(middle), pltpu.matmul_pop(right), pltpu.matmul_pop(left0) + pltpu.matmul_pop(left1)
        )

    totals = [pltpu.ACC(unit)((count, LANES), F32) for unit in (0, 1, 0, 1)]
    return pl.run_scoped(body, *totals)


def combine(middle, right, left):
    return middle + roll(right, -1, 0) + roll(left, 1, 0)


def correlate(field, high_weight, low_weight, first, count):
    return multiply(field, high_weight, low_weight, [(first, count)], combine)


def smooth(source, first, count):
    x = source[pl.ds(first, count), :]
    above = source[pl.ds(first - PITCH, count), :]
    below = source[pl.ds(first + PITCH, count), :]
    wide = source[pl.ds(first - 8, count + 16), :]
    before = roll(wide, 1, 0)[8 : 8 + count]
    after = roll(wide, -1, 0)[8 : 8 + count]
    lane = iota(x.shape, 1)
    column = lane % B
    upper = roll(jnp.where(lane >= LANES - B, above, x), B, 1)
    lower = roll(jnp.where(lane < B, below, x), -B, 1)
    leftward = jnp.where(column == 0, roll(before, -(B - 1), 1), roll(x, 1, 1))
    rightward = jnp.where(column == B - 1, roll(after, B - 1, 1), roll(x, -1, 1))
    return PENALTY * (4.0 * x - upper - lower - leftward - rightward)


def own(value, first):
    return jnp.concatenate(
        [value[PITCH * r + 8 - first : PITCH * r + 24 - first] for r in range(4, 8)], axis=0
    )


def pack_sides(middle, left_ref, right_ref):
    sublane = iota((8, LANES), 0)
    for pair in range(2):
        first, second = 4 + 2 * pair, 5 + 2 * pair
        left_ref[pair] = jnp.where(sublane < 4, middle[first, 0:8], roll(middle[second, 0:8], 4, 0))
        right_ref[pair] = jnp.where(sublane < 4, roll(middle[first, 8:16], 4, 0), middle[second, 8:16])


def unpack_middle(middle, flat, masked):
    for r in range(12):
        start = PITCH * r + 8
        put(flat, start, masked(middle[r], start, 16))


def unpack_sides(from_left, from_right, flat, masked):
    sublane = iota((8, LANES), 0)
    for r in range(ROWS):
        right = left = jnp.zeros((8, LANES), F32)
        if r >= 1:
            right = from_right[(r - 1) // 2]
            if (r - 1) % 2:
                right = roll(right, 4, 0)
        if r < 12:
            left = from_left[r // 2]
            if r % 2 == 0:
                left = roll(left, 4, 0)
        put(flat, PITCH * r, masked(jnp.where(sublane < 4, right, left), PITCH * r, 8))


def image_kernel(
    grid, b_ref, guess_ref, kernel_ref, template_ref, residual_ref,
    x_mid, v_mid, b_mid, x_left, x_right, v_left, v_right, b_left, b_right,
    x_from_left, x_from_right, v_from_left, v_from_right, b_from_left, b_from_right,
    xf, xf_low, vf, vf_low, bf, rf, rf_low, t1, t1_low, t2, t2_low, y_middle, y_right, y_left, mask_ref, taps_ref, shifted_ref, k_high, k_low, kt_high, kt_low,
    r0_own, v1_own, kr0_own, kv1_own, lr0_own, lv1_own,
    slots, pixels, far_sems, guess_tile, b_tile, taps_in, in_sems,
    x_send, x_recv, b_send, b_recv, v_send, v_recv, sum_send, sum_recv,
):
    n_rows, n_cols = grid
    loads = (
        pltpu.make_async_copy(guess_ref, guess_tile, in_sems.at[0]),
        pltpu.make_async_copy(b_ref, b_tile, in_sems.at[1]),
        pltpu.make_async_copy(kernel_ref, taps_in, in_sems.at[2]),
    )
    row, col = lax.axis_index("row"), lax.axis_index("col")

    def at(dr, dc):
        return lax.rem(row + dr + n_rows, n_rows), lax.rem(col + dc + n_cols, n_cols)

    for load in loads:
        load.start()
    barrier = pltpu.get_barrier_semaphore()
    def signal(semaphore, device):
        pl.semaphore_signal(semaphore, inc=1, device_id=device, device_id_type=MESH)

    def exists(dr, dc):
        inside = None
        for place, step, count in ((row, dr, n_rows), (col, dc, n_cols)):
            if step:
                test = place + step < count if step > 0 else place + step >= 0
                inside = test if inside is None else inside & test
        return inside

    for dr, dc in DIRECTIONS[:6]:
        pl.when(exists(dr, dc))(lambda dr=dr, dc=dc: signal(barrier, at(dr, dc)))
    for d in range(1, n_rows):
        signal(barrier, at(d, 0))
    greetings = n_rows - 1 + sum(exists(dr, dc).astype(jnp.int32) for dr, dc in DIRECTIONS[:6])

    def remote(source, target, send, recv, device):
        return pltpu.make_async_remote_copy(
            src_ref=source, dst_ref=target, send_sem=send, recv_sem=recv, device_id=device, device_id_type=MESH
        )

    def start(copies):
        for (dr, dc), copy in zip(DIRECTIONS, copies):
            pl.when(exists(dr, dc))(copy.start)

    def sent(copies):
        for (dr, dc), copy in zip(DIRECTIONS, copies):
            pl.when(exists(dr, dc))(copy.wait_send)

    def received(copies, numbers=range(8)):
        for number in numbers:
            dr, dc = DIRECTIONS[number]
            pl.when(exists(-dr, -dc))(copies[number].wait_recv)

    def field_copies(middle, left, right, from_left, from_right, send, recv):
        copies = []
        for number, (dr, dc) in enumerate(DIRECTIONS):
            if dc == 0:
                source = middle.at[pl.ds(4, 4)]
                target = middle.at[pl.ds(4 - 4 * dr, 4)]
            else:
                source = right if dc == 1 else left
                target = (from_left if dc == 1 else from_right).at[pl.ds(2 - 2 * dr, 2)]
            copies.append(remote(source, target, send.at[number], recv.at[number], at(dr, dc)))
        return copies

    def spread(middle, first, x):
        for i in range(4):
            middle[first + i] = x[16 * i : 16 * i + 16]

    loads[0].wait()
    spread(x_mid, 4, swap_blocks(guess_tile[...]))
    pack_sides(x_mid, x_left, x_right)
    pl.semaphore_wait(barrier, greetings)

    x_copies = field_copies(x_mid, x_left, x_right, x_from_left, x_from_right, x_send, x_recv)
    start(x_copies)
    loads[1].wait()
    spread(b_mid, 2, swap_blocks(b_tile[...]))
    sublane = iota((8, LANES), 0)
    left_part = right_part = jnp.zeros((8, LANES), F32)
    for i in range(4):
        here = sublane // 2 == i
        left_part = jnp.where(here, roll(b_mid[2 + i, 0:8], 2 * i, 0), left_part)
        right_part = jnp.where(here, roll(b_mid[2 + i, 8:16], 2 * i + 2, 0), right_part)
    b_left[...] = left_part
    b_right[...] = right_part

    b_copies = []
    for number, (dr, dc) in enumerate(DIRECTIONS):
        if dc == 0:
            source = b_mid.at[pl.ds(2 if dr == -1 else 4, 2)]
            target = b_mid.at[pl.ds(6 if dr == -1 else 0, 2)]
        else:
            source = b_right if dc == 1 else b_left
            target = (b_from_left if dc == 1 else b_from_right).at[1 - dr]
        b_copies.append(remote(source, target, b_send.at[number], b_recv.at[number], at(dr, dc)))
    start(b_copies)

    taps_ref[...] = jnp.zeros_like(taps_ref)
    loads[2].wait()
    taps_ref[0:31, 0:31] = taps_in[...]
    build_weights(taps_ref, shifted_ref, (k_high, k_low, kt_high, kt_low))
    flat = iota((FLAT, LANES), 0)
    slot = flat % PITCH
    block_row = row * 4 + flat // PITCH - 4 - (slot < 4).astype(jnp.int32)
    block_col = col * 16 + slot - 8 + 24 * (slot < 4).astype(jnp.int32)
    inside = (block_row >= 0) & (block_row < 4 * n_rows) & (block_col >= 0) & (block_col < 16 * n_cols)
    mask_ref[...] = inside.astype(F32)

    def masked(value, first, count):
        return jnp.where(mask_ref[pl.ds(first, count), :] > 0.5, value, 0.0)

    distances = []
    while (2 << len(distances)) - 1 < n_cols - 1:
        distances.append(2 << len(distances))

    def greet(number):
        if number < len(distances):
            for d in (distances[number], -distances[number]):
                pl.when(exists(0, d))(lambda d=d: signal(far_sems.at[number], at(0, d)))

    def meet(number):
        if number < len(distances):
            d = distances[number]
            count = exists(0, d).astype(jnp.int32) + exists(0, -d).astype(jnp.int32)
            pl.semaphore_wait(far_sems.at[number], count)

    def take_b():
        received(b_copies)
        for r in range(2, 11):
            right = left = jnp.zeros((8, LANES), F32)
            if r >= 3:
                right = roll(b_from_right[(r - 1) // 4], -2 * ((r - 1) % 4), 0)
            if r < 10:
                left = roll(b_from_left[r // 4], 6 - 2 * (r % 4), 0)
            bf[PITCH * r : PITCH * r + 8] = jnp.where(sublane < 4, right, left)
            if r < 10:
                bf[PITCH * r + 8 : PITCH * r + 24] = b_mid[r - 2]

    parts_refs = (y_middle, y_right, y_left)

    def receive(copies, middle, from_left, from_right, field, greeting, top, bottom):
        def keep(runs):
            def finish(*parts):
                for part, value in zip(parts_refs, parts):
                    start = 0
                    for first, length in runs:
                        part[pl.ds(first, length), :] = value[start : start + length]
                        start += length

            return finish

        received(copies, range(6, 8))
        unpack_middle(middle, field, masked)
        runs = [(PITCH * r + 8, 16) for r in range(top, bottom)]
        multiply(field, k_high, k_low, runs, keep(runs))
        received(copies, range(6))
        greeting()
        unpack_sides(from_left, from_right, field, masked)
        runs = [(PITCH * r, 8) for r in range(top, bottom + 1)]
        multiply(field, k_high, k_low, runs, keep(runs))
        first, count = PITCH * top, PITCH * (bottom - top) + 8
        value = combine(*[part[pl.ds(first, count), :] for part in parts_refs])
        put((t1, t1_low), first, masked(value, first, count))

    blur, blur_back = (k_high, k_low), (kt_high, kt_low)
    blurred, second, blurred_second = (t1, t1_low), (rf, rf_low), (t2, t2_low)

    def stage(source, weights, target, runs, term=None, sign=1.0):
        terms = [None if term is None else term(keep, kept) for first, count, keep, kept in runs]
        value = multiply(source, *weights, [run[:2] for run in runs], combine)
        start = 0
        for (first, count, keep, kept), added in zip(runs, terms):
            piece = value[start + keep - first : start + keep - first + kept]
            start += count
            if added is not None:
                piece = added + sign * piece
            put(target, keep, masked(piece, keep, kept))

    receive(x_copies, x_mid, x_from_left, x_from_right, (xf, xf_low), lambda: greet(0), 1, 11)
    take_b()

    def remainder(keep, kept):
        return bf[pl.ds(keep, kept), :] - smooth(xf, keep, kept)

    stage(blurred, blur_back, second, [(48, 200, 48, 200)], remainder, -1.0)
    stage(second, blur, blurred_second, [(72, 152, 72, 152)])
    kr0 = own(t2[pl.ds(96, 104), :], 96)
    lr0 = own(smooth(rf, 96, 104), 96)
    v1 = own(correlate((t2, t2_low), kt_high, kt_low, 96, 104), 96) + lr0
    spread(v_mid, 4, v1)
    pack_sides(v_mid, v_left, v_right)
    v_copies = field_copies(v_mid, v_left, v_right, v_from_left, v_from_right, v_send, v_recv)
    start(v_copies)
    meet(0)
    greet(1)
    r0_own[...] = own(rf[pl.ds(96, 104), :], 96)
    v1_own[...] = v1
    kr0_own[...] = kr0
    lr0_own[...] = lr0

    def meet_and_greet():
        meet(1)
        greet(2)

    receive(v_copies, v_mid, v_from_left, v_from_right, (vf, vf_low), meet_and_greet, 2, 10)
    smooth_pieces = []

    def image(keep, kept):
        smooth_pieces.append(smooth(vf, keep, kept))
        return smooth_pieces[-1]

    stage(blurred, blur_back, second, [(72, 152, 72, 152)], image)
    stage(second, blur, blurred_second, [(96, 104, 104, 88)])
    kv1, kv2 = own(t1[pl.ds(96, 104), :], 96), own(t2[pl.ds(96, 104), :], 96)
    lv1, lv2 = own(jnp.concatenate(smooth_pieces, axis=0), 72), own(smooth(rf, 96, 104), 96)
    v2 = own(rf[pl.ds(96, 104), :], 96)

    def powers(zero, one, two):
        return two, one - two, zero - 2.0 * one + two

    r0, v1 = r0_own[...], v1_own[...]
    p = powers(r0, v1, v2)
    kp = powers(kr0_own[...], kv1, kv2)
    lp = powers(lr0_own[...], lv1, lv2)

    def lanes_of(x):
        total = x[0:8]
        for i in range(1, 8):
            total = total + x[8 * i : 8 * i + 8]
        total = total[:, :128] + total[:, 128:]
        return jnp.sum(total, axis=0, keepdims=True)

    moments = [lanes_of(p[2] * p[2])]
    for i, j in ((2, 2), (1, 2), (1, 1), (0, 1), (0, 0)):
        moments.append(lanes_of(kp[i] * kp[j] + p[i] * lp[j]))
    slot8 = iota((8, 128), 0)
    packed = jnp.zeros((8, 128), F32)
    for i, moment in enumerate(moments):
        packed = jnp.where(slot8 == i, moment, packed)
    mine = iota((8, 128), 1) == slot8
    packed = jnp.sum(packed, axis=1, keepdims=True)
    packed = jnp.sum(jnp.where(mine, packed, 0.0), axis=0, keepdims=True)

    meet(2)
    me = row * n_cols + col
    slots[me] = packed

    def hops(offset):
        z, y, x = offset[0] // 2, offset[1] // 4, offset[1] % 4
        return -(min(z, 4 - z) + min(y, 4 - y) + min(x, 4 - x))

    rows_at = [at(d, 0)[0] for d in range(n_rows)]
    cols_at = [at(0, d)[1] for d in range(n_cols)]
    offsets = [(dr, dc) for dr in range(n_rows) for dc in range(n_cols)][1:]
    for dr, dc in sorted(offsets, key=hops):
        remote(slots.at[me], slots.at[me], sum_send, sum_recv, (rows_at[dr], cols_at[dc])).start()
    others = pl.ds(0, n_rows * n_cols - 1)
    sums = remote(slots.at[others], slots.at[others], sum_send, sum_recv, at(1, 0))
    for copies in (x_copies, b_copies, v_copies):
        sent(copies)
    stage((vf, vf_low), blur, blurred, [(24, 40, 24, 32), (232, 40, 240, 32)])
    stage(blurred, blur_back, second, [(48, 40, 48, 32), (208, 40, 216, 32)], image)
    stage(second, blur, blurred_second, [(72, 40, 72, 32), (184, 40, 192, 32)])
    v3 = own(correlate((t2, t2_low), kt_high, kt_low, 96, 104), 96) + lv2
    for number, value in enumerate(p + powers(v1, v2, v3)):
        pixels[number] = swap_blocks(value)
    sums.wait_recv()
    groups = [jnp.sum(slots[pl.ds(start, n_cols)], axis=0) for start in range(0, n_rows * n_cols, n_cols)]
    while len(groups) > 1:
        groups = [sum(groups[i : i + 2][1:], groups[i]) for i in range(0, len(groups), 2)]
    total = groups[0]
    total = jnp.sum(jnp.where(mine, jnp.broadcast_to(total, (8, 128)), 0.0), axis=1, keepdims=True)
    b0, c1, c2, c3, c4, c5 = [total[i : i + 1, :] for i in range(6)]
    c = (None, c1, c2, c3, c4, c5)
    b = (b0, c1 + c2, c2 + c3, c3 + c4, c4 + c5)

    def square(q, m, base):
        return (
            q[0] * q[0] * m[base]
            + 2.0 * (q[0] * q[1]) * m[base + 1]
            + (q[1] * q[1] + 2.0 * (q[0] * q[2])) * m[base + 2]
            + 2.0 * (q[1] * q[2]) * m[base + 3]
            + q[2] * q[2] * m[base + 4]
        )

    def raised(q):
        return q[0], q[0] + q[1], q[1]

    one = (1.0, 2.0, 1.0)
    norm = square(one, b, 0)
    alpha0 = norm / square(one, c, 1)
    r1 = (1.0, 1.0 - alpha0)
    following = square(raised(r1), b, 0)
    beta0 = following / norm
    norm = following
    p1 = (r1[0] + beta0, r1[1] + beta0)
    p1_raised = raised(p1)
    alpha1 = norm / square(p1_raised, c, 1)
    r1_raised = raised(r1)
    r2 = (r1_raised[0], r1_raised[1] - alpha1 * p1[0], r1_raised[2] - alpha1 * p1[1])
    following = square(r2, b, 0)
    beta1 = following / norm
    p2 = tuple(r2[i] + beta1 * p1_raised[i] for i in range(3))
    alpha2 = following / square(p2, c, 1)
    steps = [alpha0 * one[i] + alpha1 * p1_raised[i] + alpha2 * p2[i] for i in range(3)]

    f0, f1, f2, af0, af1, af2 = [pixels[number] for number in range(6)]
    template_ref[...] = guess_tile[...] + steps[0] * f2 + steps[1] * f1 + steps[2] * f0
    residual = r2[0] * f2 + r2[1] * f1 + r2[2] * f0
    residual_ref[...] = residual - alpha2 * (p2[0] * af2 + p2[1] * af1 + p2[2] * af0)
    sums.wait_send()


def on_device(grid, right_side, initial_guess, kernel):
    n_rows, n_cols = grid
    middle = pltpu.VMEM((12, 16, LANES), F32)
    b_middle = pltpu.VMEM((8, 16, LANES), F32)
    side = pltpu.VMEM((2, 8, LANES), F32)
    halo = pltpu.VMEM((6, 8, LANES), F32)
    b_side = pltpu.VMEM((8, LANES), F32)
    b_halo = pltpu.VMEM((3, 8, LANES), F32)
    flat = pltpu.VMEM((FLAT, LANES), F32)
    weight = pltpu.VMEM((3 * LANES, 3 * LANES), BF16)
    tile = pltpu.VMEM((64, LANES), F32)
    dma = pltpu.SemaphoreType.DMA
    shape = jax.ShapeDtypeStruct((64, LANES), F32)
    vmem = pl.BlockSpec(memory_space=pltpu.VMEM)

    def body(*refs):
        image_kernel(grid, *refs)

    results = pl.pallas_call(
        body,
        out_shape=(shape, shape),
        in_specs=[pl.BlockSpec(memory_space=pltpu.HBM)] * 3,
        out_specs=(vmem, vmem),
        scratch_shapes=[
            middle, middle, b_middle, side, side, side, side, b_side, b_side,
            halo, halo, halo, halo, b_halo, b_halo,
            flat, flat, flat, flat, flat, flat, flat, flat, flat, flat, flat, flat, flat, flat, flat,
            pltpu.VMEM((128, 128), F32), pltpu.VMEM((8, 96, 1024), BF16),
            weight, weight, weight, weight,
            tile, tile, tile, tile, tile, tile,
            pltpu.VMEM((n_rows * n_cols, 1, 128), F32), pltpu.VMEM((6, 64, LANES), F32), pltpu.SemaphoreType.REGULAR((3,)), tile, tile, pltpu.VMEM((31, 31), F32), dma((3,)),
            dma((8,)), dma((8,)), dma((8,)), dma((8,)), dma((8,)), dma((8,)),
            dma, dma,
        ],
        compiler_params=pltpu.CompilerParams(
            collective_id=0, has_side_effects=True, vmem_limit_bytes=16 * 1024 * 1024
        ),
    )(*(pltpu.with_memory_space_constraint(x, pltpu.HBM) for x in (right_side, initial_guess, kernel)))

    def store(template_ref, residual_ref, template_out, residual_out, sems):
        copies = (
            pltpu.make_async_copy(template_ref, template_out, sems.at[0]),
            pltpu.make_async_copy(residual_ref, residual_out, sems.at[1]),
        )
        for copy in copies:
            copy.start()
        for copy in copies:
            copy.wait()

    return pl.pallas_call(
        store,
        out_shape=(shape, shape),
        in_specs=[vmem] * 2,
        out_specs=(pl.BlockSpec(memory_space=pltpu.HBM),) * 2,
        scratch_shapes=[dma((2,))],
        compiler_params=pltpu.CompilerParams(vmem_limit_bytes=1024 * 1024),
    )(*results)


def solution(mesh):
    grid = (mesh.shape["row"], mesh.shape["col"])
    tiles = P("row", "col")
    return jax.shard_map(
        lambda *arrays: on_device(grid, *arrays),
        mesh=mesh,
        in_specs=(tiles, tiles, P()),
        out_specs=(tiles, tiles),
        check_vma=False,
    )
```

```python
import jax
import jax.numpy as jnp
from jax import lax
from jax.experimental import pallas as pl
from jax.experimental.pallas import tpu as pltpu
from jax.sharding import PartitionSpec as P

PENALTY = 0.05
F32, BF16 = jnp.float32, jnp.bfloat16
B = 16
LANES = B * B
PITCH = 24
ROWS = 13
FLAT = ROWS * PITCH
DIRECTIONS = ((-1, -1), (-1, 1), (1, -1), (1, 1), (0, -1), (0, 1), (-1, 0), (1, 0))
MESH = pl.DeviceIdType.MESH


def iota(shape, dim):
    return lax.broadcasted_iota(jnp.int32, shape, dim)


def roll(x, shift, axis):
    return pltpu.roll(x, shift % x.shape[axis], axis)


def rounded(x):
    return x.astype(BF16).astype(F32)


def put(pair, first, value):
    rows = pl.ds(first, value.shape[0])
    pair[0][rows, :] = value
    rest = value - rounded(value)
    pair[1][rows, :] = rest
    pair[2][rows, :] = rest - rounded(rest)


def swap_blocks(x):
    top, bottom = [], []
    for i in range(4):
        upper, lower = x[16 * i : 16 * i + 8], x[16 * i + 8 : 16 * i + 16]
        top += [upper[:, :128], upper[:, 128:]]
        bottom += [lower[:, :128], lower[:, 128:]]
    y = jnp.concatenate(top + bottom, axis=0)
    row, lane = iota(y.shape, 0), iota(y.shape, 1)
    for t in range(3):
        step = 1 << t
        row_bit, lane_bit = (row >> t) & 1, (lane >> (t + 4)) & 1
        from_below = roll(roll(y, -step, 0), B * step, 1)
        from_above = roll(roll(y, step, 0), -B * step, 1)
        y = jnp.where(row_bit == lane_bit, y, jnp.where(row_bit == 0, from_below, from_above))
    return jnp.concatenate([y[:64], y[64:]], axis=1)


def pick_lanes(x, lanes):
    return jnp.take_along_axis(x, lanes, axis=1, mode="promise_in_bounds")


def build_weights(taps_ref, shifted_ref, weights):
    taps = taps_ref[...]
    lane = iota((128, 128), 1)
    empty = (lane < 1) | (lane > 31)
    ahead = jnp.where(empty, 0.0, roll(taps, 1, 1)).T[0:48]
    flipped = jnp.where(empty, 0.0, pick_lanes(taps, jnp.clip(31 - lane, 0, 127))).T[0:48]
    group = iota((48, 128), 1) // B
    for number, source in enumerate((ahead, flipped)):
        pieces = []
        for tile in range(8):
            block = 8 * tile + group
            wanted = 46 - block if number == 0 else block - 16
            valid = (wanted >= 0) & (wanted <= 30)
            pieces.append(jnp.where(valid, pick_lanes(source, jnp.clip(wanted, 0, 30)), 0.0))
        base = jnp.concatenate(pieces, axis=1)
        column = iota(base.shape, 1) % B
        for t in range(4):
            base = jnp.where((column >> t) & 1 == 1, roll(base, 1 << t, 0), base)
        for shift in range(8):
            moved = roll(base, -B * shift, 1)
            high = moved.astype(BF16)
            shifted_ref[shift, 0:48] = high
            rest = moved - high.astype(F32)
            shifted_ref[shift, 48:96] = rest.astype(BF16)
            shifted_ref[shift, 96:144] = (rest - rounded(rest)).astype(BF16)
        for part in range(3):
            weight = weights[number][part]
            for di in (-1, 0, 1):
                for r in range(B):
                    start = 31 - 16 * di - r
                    lanes = 128 * (start // 8)
                    for dj in range(3):
                        rows = 48 * part + 16 * dj
                        weight[
                            LANES * (di + 1) + B * r : LANES * (di + 1) + B * r + B,
                            LANES * dj : LANES * dj + LANES,
                        ] = shifted_ref[start % 8, rows : rows + 16, lanes : lanes + LANES]


FIRST_UNIT = [(di, 0, part) for part in range(3) for di in (-1, 0, 1)]
FIRST_UNIT += [(-1, -1, 0), (0, -1, 0), (-1, -1, 2), (0, -1, 2), (1, -1, 2)]
SECOND_UNIT = [(di, 1, part) for part in range(3) for di in (-1, 0, 1)]
SECOND_UNIT += [(1, -1, 0), (-1, -1, 1), (0, -1, 1), (1, -1, 1)]


def multiply(field, weights, runs, finish):
    count = sum(run[1] for run in runs)

    def rows(part, di):
        return jnp.concatenate([part[pl.ds(first + PITCH * di, length), :] for first, length in runs], axis=0)

    def body(middle, right, left0, left1):
        queues = []
        for unit, products in enumerate((FIRST_UNIT, SECOND_UNIT)):
            queue = []
            for number, (di, dj, part) in enumerate(products):
                queue.append((unit, number % 2, di, dj, part, ((left0, left1)[unit], middle, right)[dj + 1]))
            queues.append(queue)
        for step in range(max(map(len, queues))):
            for queue in queues:
                if step < len(queue):
                    unit, register, di, dj, part, total = queue[step]
                    weight = weights[part]
                    tile = weight[LANES * (di + 1) : LANES * (di + 2), LANES * (dj + 1) : LANES * (dj + 2)]
                    pltpu.matmul_push_rhs(tile, staging_register=register, mxu_index=unit)
                    pltpu.matmul_acc_lhs(total, rows(field[0], di), load_staged_rhs=register)
                    for other in range(1, 3 - part):
                        pltpu.matmul_acc_lhs(total, rows(field[other], di))
        return finish(
            pltpu.matmul_pop(middle), pltpu.matmul_pop(right), pltpu.matmul_pop(left0) + pltpu.matmul_pop(left1)
        )

    totals = [pltpu.ACC(unit)((count, LANES), F32) for unit in (0, 1, 0, 1)]
    return pl.run_scoped(body, *totals)


def combine(middle, right, left):
    return middle + roll(right, -1, 0) + roll(left, 1, 0)


def correlate(field, weights, first, count):
    return multiply(field, weights, [(first, count)], combine)


def smooth(source, first, count):
    x = source[pl.ds(first, count), :]
    above = source[pl.ds(first - PITCH, count), :]
    below = source[pl.ds(first + PITCH, count), :]
    wide = source[pl.ds(first - 8, count + 16), :]
    before = roll(wide, 1, 0)[8 : 8 + count]
    after = roll(wide, -1, 0)[8 : 8 + count]
    lane = iota(x.shape, 1)
    column = lane % B
    upper = roll(jnp.where(lane >= LANES - B, above, x), B, 1)
    lower = roll(jnp.where(lane < B, below, x), -B, 1)
    leftward = jnp.where(column == 0, roll(before, -(B - 1), 1), roll(x, 1, 1))
    rightward = jnp.where(column == B - 1, roll(after, B - 1, 1), roll(x, -1, 1))
    return PENALTY * (4.0 * x - upper - lower - leftward - rightward)


def own(value, first):
    return jnp.concatenate(
        [value[PITCH * r + 8 - first : PITCH * r + 24 - first] for r in range(4, 8)], axis=0
    )


def pack_sides(middle, left_ref, right_ref):
    sublane = iota((8, LANES), 0)
    for pair in range(2):
        first, second = 4 + 2 * pair, 5 + 2 * pair
        left_ref[pair] = jnp.where(sublane < 4, middle[first, 0:8], roll(middle[second, 0:8], 4, 0))
        right_ref[pair] = jnp.where(sublane < 4, roll(middle[first, 8:16], 4, 0), middle[second, 8:16])


def unpack_middle(middle, flat, masked):
    for r in range(12):
        start = PITCH * r + 8
        put(flat, start, masked(middle[r], start, 16))


def unpack_sides(from_left, from_right, flat, masked):
    sublane = iota((8, LANES), 0)
    for r in range(ROWS):
        right = left = jnp.zeros((8, LANES), F32)
        if r >= 1:
            right = from_right[(r - 1) // 2]
            if (r - 1) % 2:
                right = roll(right, 4, 0)
        if r < 12:
            left = from_left[r // 2]
            if r % 2 == 0:
                left = roll(left, 4, 0)
        put(flat, PITCH * r, masked(jnp.where(sublane < 4, right, left), PITCH * r, 8))


def image_kernel(
    grid, b_ref, guess_ref, kernel_ref, template_ref, residual_ref,
    x_mid, v_mid, b_mid, x_left, x_right, v_left, v_right, b_left, b_right,
    x_from_left, x_from_right, v_from_left, v_from_right, b_from_left, b_from_right,
    xf, xf_low, xf_last, vf, vf_low, vf_last, bf, rf, rf_low, rf_last, t1, t1_low, t1_last, t2, t2_low, t2_last, y_middle, y_right, y_left, mask_ref, taps_ref, shifted_ref, k_high, k_low, k_last, kt_high, kt_low, kt_last,
    r0_own, v1_own, kr0_own, kv1_own, lr0_own, lv1_own,
    slots, pixels, far_sems, guess_tile, b_tile, taps_in, in_sems,
    x_send, x_recv, b_send, b_recv, v_send, v_recv, sum_send, sum_recv,
):
    n_rows, n_cols = grid
    loads = (
        pltpu.make_async_copy(guess_ref, guess_tile, in_sems.at[0]),
        pltpu.make_async_copy(b_ref, b_tile, in_sems.at[1]),
        pltpu.make_async_copy(kernel_ref, taps_in, in_sems.at[2]),
    )
    row, col = lax.axis_index("row"), lax.axis_index("col")

    def at(dr, dc):
        return lax.rem(row + dr + n_rows, n_rows), lax.rem(col + dc + n_cols, n_cols)

    for load in loads:
        load.start()
    barrier = pltpu.get_barrier_semaphore()
    def signal(semaphore, device):
        pl.semaphore_signal(semaphore, inc=1, device_id=device, device_id_type=MESH)

    def exists(dr, dc):
        inside = None
        for place, step, count in ((row, dr, n_rows), (col, dc, n_cols)):
            if step:
                test = place + step < count if step > 0 else place + step >= 0
                inside = test if inside is None else inside & test
        return inside

    for dr, dc in DIRECTIONS[:6]:
        pl.when(exists(dr, dc))(lambda dr=dr, dc=dc: signal(barrier, at(dr, dc)))
    for d in range(1, n_rows):
        signal(barrier, at(d, 0))
    greetings = n_rows - 1 + sum(exists(dr, dc).astype(jnp.int32) for dr, dc in DIRECTIONS[:6])

    def remote(source, target, send, recv, device):
        return pltpu.make_async_remote_copy(
            src_ref=source, dst_ref=target, send_sem=send, recv_sem=recv, device_id=device, device_id_type=MESH
        )

    def start(copies):
        for (dr, dc), copy in zip(DIRECTIONS, copies):
            pl.when(exists(dr, dc))(copy.start)

    def sent(copies):
        for (dr, dc), copy in zip(DIRECTIONS, copies):
            pl.when(exists(dr, dc))(copy.wait_send)

    def received(copies, numbers=range(8)):
        for number in numbers:
            dr, dc = DIRECTIONS[number]
            pl.when(exists(-dr, -dc))(copies[number].wait_recv)

    def field_copies(middle, left, right, from_left, from_right, send, recv):
        copies = []
        for number, (dr, dc) in enumerate(DIRECTIONS):
            if dc == 0:
                source = middle.at[pl.ds(4, 4)]
                target = middle.at[pl.ds(4 - 4 * dr, 4)]
            else:
                source = right if dc == 1 else left
                target = (from_left if dc == 1 else from_right).at[pl.ds(2 - 2 * dr, 2)]
            copies.append(remote(source, target, send.at[number], recv.at[number], at(dr, dc)))
        return copies

    def spread(middle, first, x):
        for i in range(4):
            middle[first + i] = x[16 * i : 16 * i + 16]

    loads[0].wait()
    spread(x_mid, 4, swap_blocks(guess_tile[...]))
    pack_sides(x_mid, x_left, x_right)
    pl.semaphore_wait(barrier, greetings)

    x_copies = field_copies(x_mid, x_left, x_right, x_from_left, x_from_right, x_send, x_recv)
    start(x_copies)
    loads[1].wait()
    spread(b_mid, 2, swap_blocks(b_tile[...]))
    sublane = iota((8, LANES), 0)
    left_part = right_part = jnp.zeros((8, LANES), F32)
    for i in range(4):
        here = sublane // 2 == i
        left_part = jnp.where(here, roll(b_mid[2 + i, 0:8], 2 * i, 0), left_part)
        right_part = jnp.where(here, roll(b_mid[2 + i, 8:16], 2 * i + 2, 0), right_part)
    b_left[...] = left_part
    b_right[...] = right_part

    b_copies = []
    for number, (dr, dc) in enumerate(DIRECTIONS):
        if dc == 0:
            source = b_mid.at[pl.ds(2 if dr == -1 else 4, 2)]
            target = b_mid.at[pl.ds(6 if dr == -1 else 0, 2)]
        else:
            source = b_right if dc == 1 else b_left
            target = (b_from_left if dc == 1 else b_from_right).at[1 - dr]
        b_copies.append(remote(source, target, b_send.at[number], b_recv.at[number], at(dr, dc)))
    start(b_copies)

    taps_ref[...] = jnp.zeros_like(taps_ref)
    blur, blur_back = (k_high, k_low, k_last), (kt_high, kt_low, kt_last)
    blurred, second, blurred_second = (t1, t1_low, t1_last), (rf, rf_low, rf_last), (t2, t2_low, t2_last)
    loads[2].wait()
    taps_ref[0:31, 0:31] = taps_in[...]
    build_weights(taps_ref, shifted_ref, (blur, blur_back))
    flat = iota((FLAT, LANES), 0)
    slot = flat % PITCH
    block_row = row * 4 + flat // PITCH - 4 - (slot < 4).astype(jnp.int32)
    block_col = col * 16 + slot - 8 + 24 * (slot < 4).astype(jnp.int32)
    inside = (block_row >= 0) & (block_row < 4 * n_rows) & (block_col >= 0) & (block_col < 16 * n_cols)
    mask_ref[...] = inside.astype(F32)

    def masked(value, first, count):
        return jnp.where(mask_ref[pl.ds(first, count), :] > 0.5, value, 0.0)

    distances = []
    while (2 << len(distances)) - 1 < n_cols - 1:
        distances.append(2 << len(distances))

    def greet(number):
        if number < len(distances):
            for d in (distances[number], -distances[number]):
                pl.when(exists(0, d))(lambda d=d: signal(far_sems.at[number], at(0, d)))

    def meet(number):
        if number < len(distances):
            d = distances[number]
            count = exists(0, d).astype(jnp.int32) + exists(0, -d).astype(jnp.int32)
            pl.semaphore_wait(far_sems.at[number], count)

    def take_b():
        received(b_copies)
        for r in range(2, 11):
            right = left = jnp.zeros((8, LANES), F32)
            if r >= 3:
                right = roll(b_from_right[(r - 1) // 4], -2 * ((r - 1) % 4), 0)
            if r < 10:
                left = roll(b_from_left[r // 4], 6 - 2 * (r % 4), 0)
            bf[PITCH * r : PITCH * r + 8] = jnp.where(sublane < 4, right, left)
            if r < 10:
                bf[PITCH * r + 8 : PITCH * r + 24] = b_mid[r - 2]

    parts_refs = (y_middle, y_right, y_left)

    def receive(copies, middle, from_left, from_right, field, greeting, top, bottom):
        def keep(runs):
            def finish(*parts):
                for part, value in zip(parts_refs, parts):
                    start = 0
                    for first, length in runs:
                        part[pl.ds(first, length), :] = value[start : start + length]
                        start += length

            return finish

        received(copies, range(6, 8))
        unpack_middle(middle, field, masked)
        runs = [(PITCH * r + 8, 16) for r in range(top, bottom)]
        multiply(field, blur, runs, keep(runs))
        received(copies, range(6))
        greeting()
        unpack_sides(from_left, from_right, field, masked)
        runs = [(PITCH * r, 8) for r in range(top, bottom + 1)]
        multiply(field, blur, runs, keep(runs))
        first, count = PITCH * top, PITCH * (bottom - top) + 8
        value = combine(*[part[pl.ds(first, count), :] for part in parts_refs])
        put(blurred, first, masked(value, first, count))


    def stage(source, weights, target, runs, term=None, sign=1.0):
        terms = [None if term is None else term(keep, kept) for first, count, keep, kept in runs]
        value = multiply(source, weights, [run[:2] for run in runs], combine)
        start = 0
        for (first, count, keep, kept), added in zip(runs, terms):
            piece = value[start + keep - first : start + keep - first + kept]
            start += count
            if added is not None:
                piece = added + sign * piece
            put(target, keep, masked(piece, keep, kept))

    receive(x_copies, x_mid, x_from_left, x_from_right, (xf, xf_low, xf_last), lambda: greet(0), 1, 11)
    take_b()

    def remainder(keep, kept):
        return bf[pl.ds(keep, kept), :] - smooth(xf, keep, kept)

    stage(blurred, blur_back, second, [(48, 200, 48, 200)], remainder, -1.0)
    stage(second, blur, blurred_second, [(72, 152, 72, 152)])
    kr0 = own(t2[pl.ds(96, 104), :], 96)
    lr0 = own(smooth(rf, 96, 104), 96)
    v1 = own(correlate(blurred_second, blur_back, 96, 104), 96) + lr0
    spread(v_mid, 4, v1)
    pack_sides(v_mid, v_left, v_right)
    v_copies = field_copies(v_mid, v_left, v_right, v_from_left, v_from_right, v_send, v_recv)
    start(v_copies)
    meet(0)
    greet(1)
    r0_own[...] = own(rf[pl.ds(96, 104), :], 96)
    v1_own[...] = v1
    kr0_own[...] = kr0
    lr0_own[...] = lr0

    def meet_and_greet():
        meet(1)
        greet(2)

    receive(v_copies, v_mid, v_from_left, v_from_right, (vf, vf_low, vf_last), meet_and_greet, 2, 10)
    smooth_pieces = []

    def image(keep, kept):
        smooth_pieces.append(smooth(vf, keep, kept))
        return smooth_pieces[-1]

    stage(blurred, blur_back, second, [(72, 152, 72, 152)], image)
    stage(second, blur, blurred_second, [(96, 104, 104, 88)])
    kv1, kv2 = own(t1[pl.ds(96, 104), :], 96), own(t2[pl.ds(96, 104), :], 96)
    lv1, lv2 = own(jnp.concatenate(smooth_pieces, axis=0), 72), own(smooth(rf, 96, 104), 96)
    v2 = own(rf[pl.ds(96, 104), :], 96)

    def powers(zero, one, two):
        return two, one - two, zero - 2.0 * one + two

    r0, v1 = r0_own[...], v1_own[...]
    p = powers(r0, v1, v2)
    kp = powers(kr0_own[...], kv1, kv2)
    lp = powers(lr0_own[...], lv1, lv2)

    def lanes_of(x):
        total = x[0:8]
        for i in range(1, 8):
            total = total + x[8 * i : 8 * i + 8]
        total = total[:, :128] + total[:, 128:]
        return jnp.sum(total, axis=0, keepdims=True)

    moments = [lanes_of(p[2] * p[2])]
    for i, j in ((2, 2), (1, 2), (1, 1), (0, 1), (0, 0)):
        moments.append(lanes_of(kp[i] * kp[j] + p[i] * lp[j]))
    slot8 = iota((8, 128), 0)
    packed = jnp.zeros((8, 128), F32)
    for i, moment in enumerate(moments):
        packed = jnp.where(slot8 == i, moment, packed)
    mine = iota((8, 128), 1) == slot8
    packed = jnp.sum(packed, axis=1, keepdims=True)
    packed = jnp.sum(jnp.where(mine, packed, 0.0), axis=0, keepdims=True)

    meet(2)
    me = row * n_cols + col
    slots[me] = packed

    def hops(offset):
        z, y, x = offset[0] // 2, offset[1] // 4, offset[1] % 4
        return -(min(z, 4 - z) + min(y, 4 - y) + min(x, 4 - x))

    rows_at = [at(d, 0)[0] for d in range(n_rows)]
    cols_at = [at(0, d)[1] for d in range(n_cols)]
    offsets = [(dr, dc) for dr in range(n_rows) for dc in range(n_cols)][1:]
    for dr, dc in sorted(offsets, key=hops):
        remote(slots.at[me], slots.at[me], sum_send, sum_recv, (rows_at[dr], cols_at[dc])).start()
    others = pl.ds(0, n_rows * n_cols - 1)
    sums = remote(slots.at[others], slots.at[others], sum_send, sum_recv, at(1, 0))
    for copies in (x_copies, b_copies, v_copies):
        sent(copies)
    stage((vf, vf_low, vf_last), blur, blurred, [(24, 40, 24, 32), (232, 40, 240, 32)])
    stage(blurred, blur_back, second, [(48, 40, 48, 32), (208, 40, 216, 32)], image)
    stage(second, blur, blurred_second, [(72, 40, 72, 32), (184, 40, 192, 32)])
    v3 = own(correlate(blurred_second, blur_back, 96, 104), 96) + lv2
    for number, value in enumerate(p + powers(v1, v2, v3)):
        pixels[number] = swap_blocks(value)
    sums.wait_recv()
    groups = [jnp.sum(slots[pl.ds(start, n_cols)], axis=0) for start in range(0, n_rows * n_cols, n_cols)]
    while len(groups) > 1:
        groups = [sum(groups[i : i + 2][1:], groups[i]) for i in range(0, len(groups), 2)]
    total = groups[0]
    total = jnp.sum(jnp.where(mine, jnp.broadcast_to(total, (8, 128)), 0.0), axis=1, keepdims=True)
    b0, c1, c2, c3, c4, c5 = [total[i : i + 1, :] for i in range(6)]
    c = (None, c1, c2, c3, c4, c5)
    b = (b0, c1 + c2, c2 + c3, c3 + c4, c4 + c5)

    def square(q, m, base):
        return (
            q[0] * q[0] * m[base]
            + 2.0 * (q[0] * q[1]) * m[base + 1]
            + (q[1] * q[1] + 2.0 * (q[0] * q[2])) * m[base + 2]
            + 2.0 * (q[1] * q[2]) * m[base + 3]
            + q[2] * q[2] * m[base + 4]
        )

    def raised(q):
        return q[0], q[0] + q[1], q[1]

    one = (1.0, 2.0, 1.0)
    norm = square(one, b, 0)
    alpha0 = norm / square(one, c, 1)
    r1 = (1.0, 1.0 - alpha0)
    following = square(raised(r1), b, 0)
    beta0 = following / norm
    norm = following
    p1 = (r1[0] + beta0, r1[1] + beta0)
    p1_raised = raised(p1)
    alpha1 = norm / square(p1_raised, c, 1)
    r1_raised = raised(r1)
    r2 = (r1_raised[0], r1_raised[1] - alpha1 * p1[0], r1_raised[2] - alpha1 * p1[1])
    following = square(r2, b, 0)
    beta1 = following / norm
    p2 = tuple(r2[i] + beta1 * p1_raised[i] for i in range(3))
    alpha2 = following / square(p2, c, 1)
    steps = [alpha0 * one[i] + alpha1 * p1_raised[i] + alpha2 * p2[i] for i in range(3)]

    f0, f1, f2, af0, af1, af2 = [pixels[number] for number in range(6)]
    template_ref[...] = guess_tile[...] + steps[0] * f2 + steps[1] * f1 + steps[2] * f0
    residual = r2[0] * f2 + r2[1] * f1 + r2[2] * f0
    residual_ref[...] = residual - alpha2 * (p2[0] * af2 + p2[1] * af1 + p2[2] * af0)
    sums.wait_send()


def on_device(grid, right_side, initial_guess, kernel):
    n_rows, n_cols = grid
    middle = pltpu.VMEM((12, 16, LANES), F32)
    b_middle = pltpu.VMEM((8, 16, LANES), F32)
    side = pltpu.VMEM((2, 8, LANES), F32)
    halo = pltpu.VMEM((6, 8, LANES), F32)
    b_side = pltpu.VMEM((8, LANES), F32)
    b_halo = pltpu.VMEM((3, 8, LANES), F32)
    flat = pltpu.VMEM((FLAT, LANES), F32)
    weight = pltpu.VMEM((3 * LANES, 3 * LANES), BF16)
    tile = pltpu.VMEM((64, LANES), F32)
    dma = pltpu.SemaphoreType.DMA
    shape = jax.ShapeDtypeStruct((64, LANES), F32)
    vmem = pl.BlockSpec(memory_space=pltpu.VMEM)

    def body(*refs):
        image_kernel(grid, *refs)

    results = pl.pallas_call(
        body,
        out_shape=(shape, shape),
        in_specs=[pl.BlockSpec(memory_space=pltpu.HBM)] * 3,
        out_specs=(vmem, vmem),
        scratch_shapes=[
            middle, middle, b_middle, side, side, side, side, b_side, b_side,
            halo, halo, halo, halo, b_halo, b_halo,
            flat, flat, flat, flat, flat, flat, flat, flat, flat, flat, flat, flat, flat, flat, flat, flat, flat, flat, flat, flat,
            pltpu.VMEM((128, 128), F32), pltpu.VMEM((8, 144, 1024), BF16),
            weight, weight, weight, weight, weight, weight,
            tile, tile, tile, tile, tile, tile,
            pltpu.VMEM((n_rows * n_cols, 1, 128), F32), pltpu.VMEM((6, 64, LANES), F32), pltpu.SemaphoreType.REGULAR((3,)), tile, tile, pltpu.VMEM((31, 31), F32), dma((3,)),
            dma((8,)), dma((8,)), dma((8,)), dma((8,)), dma((8,)), dma((8,)),
            dma, dma,
        ],
        compiler_params=pltpu.CompilerParams(
            collective_id=0, has_side_effects=True, vmem_limit_bytes=24 * 1024 * 1024
        ),
    )(*(pltpu.with_memory_space_constraint(x, pltpu.HBM) for x in (right_side, initial_guess, kernel)))

    def store(template_ref, residual_ref, template_out, residual_out, sems):
        copies = (
            pltpu.make_async_copy(template_ref, template_out, sems.at[0]),
            pltpu.make_async_copy(residual_ref, residual_out, sems.at[1]),
        )
        for copy in copies:
            copy.start()
        for copy in copies:
            copy.wait()

    return pl.pallas_call(
        store,
        out_shape=(shape, shape),
        in_specs=[vmem] * 2,
        out_specs=(pl.BlockSpec(memory_space=pltpu.HBM),) * 2,
        scratch_shapes=[dma((2,))],
        compiler_params=pltpu.CompilerParams(vmem_limit_bytes=1024 * 1024),
    )(*results)


def solution(mesh):
    grid = (mesh.shape["row"], mesh.shape["col"])
    tiles = P("row", "col")
    return jax.shard_map(
        lambda *arrays: on_device(grid, *arrays),
        mesh=mesh,
        in_specs=(tiles, tiles, P()),
        out_specs=(tiles, tiles),
        check_vma=False,
    )
```

```python
import jax
import jax.numpy as jnp
from jax import lax
from jax.experimental import pallas as pl
from jax.experimental.pallas import tpu as pltpu
from jax.sharding import PartitionSpec as P

PENALTY = 0.05
F32, BF16 = jnp.float32, jnp.bfloat16
B = 16
LANES = B * B
PITCH = 24
ROWS = 13
FLAT = ROWS * PITCH
DIRECTIONS = ((-1, -1), (-1, 1), (1, -1), (1, 1), (0, -1), (0, 1), (-1, 0), (1, 0))
MESH = pl.DeviceIdType.MESH


def iota(shape, dim):
    return lax.broadcasted_iota(jnp.int32, shape, dim)


def roll(x, shift, axis):
    return pltpu.roll(x, shift % x.shape[axis], axis)


def rounded(x):
    return x.astype(BF16).astype(F32)


def put(pair, first, value):
    rows = pl.ds(first, value.shape[0])
    pair[0][rows, :] = value
    pair[1][rows, :] = value - rounded(value)


def swap_blocks(x):
    top, bottom = [], []
    for i in range(4):
        upper, lower = x[16 * i : 16 * i + 8], x[16 * i + 8 : 16 * i + 16]
        top += [upper[:, :128], upper[:, 128:]]
        bottom += [lower[:, :128], lower[:, 128:]]
    y = jnp.concatenate(top + bottom, axis=0)
    row, lane = iota(y.shape, 0), iota(y.shape, 1)
    for t in range(3):
        step = 1 << t
        row_bit, lane_bit = (row >> t) & 1, (lane >> (t + 4)) & 1
        from_below = roll(roll(y, -step, 0), B * step, 1)
        from_above = roll(roll(y, step, 0), -B * step, 1)
        y = jnp.where(row_bit == lane_bit, y, jnp.where(row_bit == 0, from_below, from_above))
    return jnp.concatenate([y[:64], y[64:]], axis=1)


def pick_lanes(x, lanes):
    return jnp.take_along_axis(x, lanes, axis=1, mode="promise_in_bounds")


def build_weights(taps_ref, shifted_ref, weights):
    taps = taps_ref[...]
    lane = iota((128, 128), 1)
    empty = (lane < 1) | (lane > 31)
    ahead = jnp.where(empty, 0.0, roll(taps, 1, 1)).T[0:48]
    flipped = jnp.where(empty, 0.0, pick_lanes(taps, jnp.clip(31 - lane, 0, 127))).T[0:48]
    group = iota((48, 128), 1) // B
    for number, source in enumerate((ahead, flipped)):
        pieces = []
        for tile in range(8):
            block = 8 * tile + group
            wanted = 46 - block if number == 0 else block - 16
            valid = (wanted >= 0) & (wanted <= 30)
            pieces.append(jnp.where(valid, pick_lanes(source, jnp.clip(wanted, 0, 30)), 0.0))
        base = jnp.concatenate(pieces, axis=1)
        column = iota(base.shape, 1) % B
        for t in range(4):
            base = jnp.where((column >> t) & 1 == 1, roll(base, 1 << t, 0), base)
        for shift in range(8):
            moved = roll(base, -B * shift, 1)
            high = moved.astype(BF16)
            shifted_ref[shift, 0:48] = high
            shifted_ref[shift, 48:96] = (moved - high.astype(F32)).astype(BF16)
        for part in range(2):
            weight = weights[2 * number + part]
            for di in (-1, 0, 1):
                for r in range(B):
                    start = 31 - 16 * di - r
                    lanes = 128 * (start // 8)
                    for dj in range(3):
                        rows = 48 * part + 16 * dj
                        weight[
                            LANES * (di + 1) + B * r : LANES * (di + 1) + B * r + B,
                            LANES * dj : LANES * dj + LANES,
                        ] = shifted_ref[start % 8, rows : rows + 16, lanes : lanes + LANES]


FIRST_UNIT = [(di, 0, low) for low in (False, True) for di in (-1, 0, 1)]
FIRST_UNIT += [(-1, -1, False), (-1, -1, True), (0, -1, True)]
SECOND_UNIT = [(di, 1, low) for low in (False, True) for di in (-1, 0, 1)]
SECOND_UNIT += [(0, -1, False), (1, -1, False), (1, -1, True)]


def multiply(field, high_weight, low_weight, runs, finish):
    count = sum(run[1] for run in runs)

    def rows(part, di):
        return jnp.concatenate([part[pl.ds(first + PITCH * di, length), :] for first, length in runs], axis=0)

    def body(middle, right, left0, left1):
        queues = []
        for unit, products in enumerate((FIRST_UNIT, SECOND_UNIT)):
            queue = []
            for number, (di, dj, low) in enumerate(products):
                queue.append((unit, number % 2, di, dj, low, ((left0, left1)[unit], middle, right)[dj + 1]))
            queues.append(queue)
        for step in range(max(map(len, queues))):
            for queue in queues:
                if step < len(queue):
                    unit, register, di, dj, low, total = queue[step]
                    weight = low_weight if low else high_weight
                    tile = weight[LANES * (di + 1) : LANES * (di + 2), LANES * (dj + 1) : LANES * (dj + 2)]
                    pltpu.matmul_push_rhs(tile, staging_register=register, mxu_index=unit)
                    pltpu.matmul_acc_lhs(total, rows(field[0], di), load_staged_rhs=register)
                    if not low:
                        pltpu.matmul_acc_lhs(total, rows(field[1], di))
        return finish(
            pltpu.matmul_pop(middle), pltpu.matmul_pop(right), pltpu.matmul_pop(left0) + pltpu.matmul_pop(left1)
        )

    totals = [pltpu.ACC(unit)((count, LANES), F32) for unit in (0, 1, 0, 1)]
    return pl.run_scoped(body, *totals)


def combine(middle, right, left):
    return middle + roll(right, -1, 0) + roll(left, 1, 0)


def correlate(field, high_weight, low_weight, first, count):
    return multiply(field, high_weight, low_weight, [(first, count)], combine)


def smooth(source, first, count):
    x = source[pl.ds(first, count), :]
    above = source[pl.ds(first - PITCH, count), :]
    below = source[pl.ds(first + PITCH, count), :]
    wide = source[pl.ds(first - 8, count + 16), :]
    before = roll(wide, 1, 0)[8 : 8 + count]
    after = roll(wide, -1, 0)[8 : 8 + count]
    lane = iota(x.shape, 1)
    column = lane % B
    upper = roll(jnp.where(lane >= LANES - B, above, x), B, 1)
    lower = roll(jnp.where(lane < B, below, x), -B, 1)
    leftward = jnp.where(column == 0, roll(before, -(B - 1), 1), roll(x, 1, 1))
    rightward = jnp.where(column == B - 1, roll(after, B - 1, 1), roll(x, -1, 1))
    return PENALTY * (4.0 * x - upper - lower - leftward - rightward)


def own(value, first):
    return jnp.concatenate(
        [value[PITCH * r + 8 - first : PITCH * r + 24 - first] for r in range(4, 8)], axis=0
    )


def pack_sides(middle, left_ref, right_ref):
    sublane = iota((8, LANES), 0)
    for pair in range(2):
        first, second = 4 + 2 * pair, 5 + 2 * pair
        left_ref[pair] = jnp.where(sublane < 4, middle[first, 0:8], roll(middle[second, 0:8], 4, 0))
        right_ref[pair] = jnp.where(sublane < 4, roll(middle[first, 8:16], 4, 0), middle[second, 8:16])


def unpack_middle(middle, flat, masked, rows):
    for r in rows:
        start = PITCH * r + 8
        put(flat, start, masked(middle[r], start, 16))


def unpack_sides(from_left, from_right, flat, masked):
    sublane = iota((8, LANES), 0)
    for r in range(ROWS):
        right = left = jnp.zeros((8, LANES), F32)
        if r >= 1:
            right = from_right[(r - 1) // 2]
            if (r - 1) % 2:
                right = roll(right, 4, 0)
        if r < 12:
            left = from_left[r // 2]
            if r % 2 == 0:
                left = roll(left, 4, 0)
        put(flat, PITCH * r, masked(jnp.where(sublane < 4, right, left), PITCH * r, 8))


def image_kernel(
    grid, b_ref, guess_ref, kernel_ref, template_ref, residual_ref,
    x_mid, v_mid, b_mid, x_left, x_right, v_left, v_right, b_left, b_right,
    x_from_left, x_from_right, v_from_left, v_from_right, b_from_left, b_from_right,
    xf, xf_low, vf, vf_low, bf, rf, rf_low, t1, t1_low, t2, t2_low, y_middle, y_right, y_left, mask_ref, taps_ref, shifted_ref, k_high, k_low, kt_high, kt_low,
    r0_own, v1_own, kr0_own, kv1_own, lr0_own, lv1_own,
    slots, pixels, far_sems, guess_tile, b_tile, taps_in, in_sems,
    x_send, x_recv, b_send, b_recv, v_send, v_recv, sum_send, sum_recv,
):
    n_rows, n_cols = grid
    loads = (
        pltpu.make_async_copy(guess_ref, guess_tile, in_sems.at[0]),
        pltpu.make_async_copy(b_ref, b_tile, in_sems.at[1]),
        pltpu.make_async_copy(kernel_ref, taps_in, in_sems.at[2]),
    )
    row, col = lax.axis_index("row"), lax.axis_index("col")

    def at(dr, dc):
        return lax.rem(row + dr + n_rows, n_rows), lax.rem(col + dc + n_cols, n_cols)

    for load in loads:
        load.start()
    barrier = pltpu.get_barrier_semaphore()
    def signal(semaphore, device):
        pl.semaphore_signal(semaphore, inc=1, device_id=device, device_id_type=MESH)

    def exists(dr, dc):
        inside = None
        for place, step, count in ((row, dr, n_rows), (col, dc, n_cols)):
            if step:
                test = place + step < count if step > 0 else place + step >= 0
                inside = test if inside is None else inside & test
        return inside

    for dr, dc in DIRECTIONS[:6]:
        pl.when(exists(dr, dc))(lambda dr=dr, dc=dc: signal(barrier, at(dr, dc)))
    for d in range(1, n_rows):
        signal(barrier, at(d, 0))
    greetings = n_rows - 1 + sum(exists(dr, dc).astype(jnp.int32) for dr, dc in DIRECTIONS[:6])

    def remote(source, target, send, recv, device):
        return pltpu.make_async_remote_copy(
            src_ref=source, dst_ref=target, send_sem=send, recv_sem=recv, device_id=device, device_id_type=MESH
        )

    def start(copies):
        for (dr, dc), copy in zip(DIRECTIONS, copies):
            pl.when(exists(dr, dc))(copy.start)

    def sent(copies):
        for (dr, dc), copy in zip(DIRECTIONS, copies):
            pl.when(exists(dr, dc))(copy.wait_send)

    def received(copies, numbers=range(8)):
        for number in numbers:
            dr, dc = DIRECTIONS[number]
            pl.when(exists(-dr, -dc))(copies[number].wait_recv)

    def field_copies(middle, left, right, from_left, from_right, send, recv, rows=4):
        copies = []
        for number, (dr, dc) in enumerate(DIRECTIONS):
            if dc == 0:
                source = middle.at[pl.ds(4 if dr == -1 else 8 - rows, rows)]
                target = middle.at[pl.ds(8 if dr == -1 else 4 - rows, rows)]
            else:
                source = right if dc == 1 else left
                target = (from_left if dc == 1 else from_right).at[pl.ds(2 - 2 * dr, 2)]
            copies.append(remote(source, target, send.at[number], recv.at[number], at(dr, dc)))
        return copies

    def spread(middle, first, x):
        for i in range(4):
            middle[first + i] = x[16 * i : 16 * i + 16]

    loads[0].wait()
    spread(x_mid, 4, swap_blocks(guess_tile[...]))
    pack_sides(x_mid, x_left, x_right)
    pl.semaphore_wait(barrier, greetings)

    x_copies = field_copies(x_mid, x_left, x_right, x_from_left, x_from_right, x_send, x_recv)
    start(x_copies)
    loads[1].wait()
    spread(b_mid, 2, swap_blocks(b_tile[...]))
    sublane = iota((8, LANES), 0)
    left_part = right_part = jnp.zeros((8, LANES), F32)
    for i in range(4):
        here = sublane // 2 == i
        left_part = jnp.where(here, roll(b_mid[2 + i, 0:8], 2 * i, 0), left_part)
        right_part = jnp.where(here, roll(b_mid[2 + i, 8:16], 2 * i + 2, 0), right_part)
    b_left[...] = left_part
    b_right[...] = right_part

    b_copies = []
    for number, (dr, dc) in enumerate(DIRECTIONS):
        if dc == 0:
            source = b_mid.at[pl.ds(2 if dr == -1 else 4, 2)]
            target = b_mid.at[pl.ds(6 if dr == -1 else 0, 2)]
        else:
            source = b_right if dc == 1 else b_left
            target = (b_from_left if dc == 1 else b_from_right).at[1 - dr]
        b_copies.append(remote(source, target, b_send.at[number], b_recv.at[number], at(dr, dc)))
    start(b_copies)

    taps_ref[...] = jnp.zeros_like(taps_ref)
    loads[2].wait()
    taps_ref[0:31, 0:31] = taps_in[...]
    build_weights(taps_ref, shifted_ref, (k_high, k_low, kt_high, kt_low))
    flat = iota((FLAT, LANES), 0)
    slot = flat % PITCH
    block_row = row * 4 + flat // PITCH - 4 - (slot < 4).astype(jnp.int32)
    block_col = col * 16 + slot - 8 + 24 * (slot < 4).astype(jnp.int32)
    inside = (block_row >= 0) & (block_row < 4 * n_rows) & (block_col >= 0) & (block_col < 16 * n_cols)
    mask_ref[...] = inside.astype(F32)

    def masked(value, first, count):
        return jnp.where(mask_ref[pl.ds(first, count), :] > 0.5, value, 0.0)

    distances = []
    while (2 << len(distances)) - 1 < n_cols - 1:
        distances.append(2 << len(distances))

    def greet(number):
        if number < len(distances):
            for d in (distances[number], -distances[number]):
                pl.when(exists(0, d))(lambda d=d: signal(far_sems.at[number], at(0, d)))

    def meet(number):
        if number < len(distances):
            d = distances[number]
            count = exists(0, d).astype(jnp.int32) + exists(0, -d).astype(jnp.int32)
            pl.semaphore_wait(far_sems.at[number], count)

    def take_b():
        received(b_copies)
        for r in range(2, 11):
            right = left = jnp.zeros((8, LANES), F32)
            if r >= 3:
                right = roll(b_from_right[(r - 1) // 4], -2 * ((r - 1) % 4), 0)
            if r < 10:
                left = roll(b_from_left[r // 4], 6 - 2 * (r % 4), 0)
            bf[PITCH * r : PITCH * r + 8] = jnp.where(sublane < 4, right, left)
            if r < 10:
                bf[PITCH * r + 8 : PITCH * r + 24] = b_mid[r - 2]

    parts_refs = (y_middle, y_right, y_left)

    def receive(copies, middle, from_left, from_right, field, greeting, top, bottom):
        def keep(runs):
            def finish(*parts):
                for part, value in zip(parts_refs, parts):
                    start = 0
                    for first, length in runs:
                        part[pl.ds(first, length), :] = value[start : start + length]
                        start += length

            return finish

        received(copies, range(6, 8))
        unpack_middle(middle, field, masked, range(top - 1, bottom + 1))
        runs = [(PITCH * r + 8, 16) for r in range(top, bottom)]
        multiply(field, k_high, k_low, runs, keep(runs))
        received(copies, range(6))
        greeting()
        unpack_sides(from_left, from_right, field, masked)
        runs = [(PITCH * r, 8) for r in range(top, bottom + 1)]
        multiply(field, k_high, k_low, runs, keep(runs))
        first, count = PITCH * top, PITCH * (bottom - top) + 8
        value = combine(*[part[pl.ds(first, count), :] for part in parts_refs])
        put((t1, t1_low), first, masked(value, first, count))

    blur, blur_back = (k_high, k_low), (kt_high, kt_low)
    blurred, second, blurred_second = (t1, t1_low), (rf, rf_low), (t2, t2_low)

    def stage(source, weights, target, runs, term=None, sign=1.0):
        terms = [None if term is None else term(keep, kept) for first, count, keep, kept in runs]
        value = multiply(source, *weights, [run[:2] for run in runs], combine)
        start = 0
        for (first, count, keep, kept), added in zip(runs, terms):
            piece = value[start + keep - first : start + keep - first + kept]
            start += count
            if added is not None:
                piece = added + sign * piece
            put(target, keep, masked(piece, keep, kept))

    receive(x_copies, x_mid, x_from_left, x_from_right, (xf, xf_low), lambda: greet(0), 1, 11)
    take_b()

    def remainder(keep, kept):
        return bf[pl.ds(keep, kept), :] - smooth(xf, keep, kept)

    stage(blurred, blur_back, second, [(48, 200, 48, 200)], remainder, -1.0)
    stage(second, blur, blurred_second, [(72, 152, 72, 152)])
    kr0 = own(t2[pl.ds(96, 104), :], 96)
    lr0 = own(smooth(rf, 96, 104), 96)
    v1 = own(correlate((t2, t2_low), kt_high, kt_low, 96, 104), 96) + lr0
    spread(v_mid, 4, v1)
    pack_sides(v_mid, v_left, v_right)
    v_copies = field_copies(v_mid, v_left, v_right, v_from_left, v_from_right, v_send, v_recv, 3)
    start(v_copies)
    far_copies = [
        remote(v_mid.at[pl.ds(7, 1)], v_mid.at[pl.ds(11, 1)], v_send.at[8], v_recv.at[8], at(-1, 0)),
        remote(v_mid.at[pl.ds(4, 1)], v_mid.at[pl.ds(0, 1)], v_send.at[9], v_recv.at[9], at(1, 0)),
    ]
    pl.when(exists(-1, 0))(far_copies[0].start)
    pl.when(exists(1, 0))(far_copies[1].start)
    meet(0)
    greet(1)
    r0_own[...] = own(rf[pl.ds(96, 104), :], 96)
    v1_own[...] = v1
    kr0_own[...] = kr0
    lr0_own[...] = lr0

    def meet_and_greet():
        meet(1)
        greet(2)

    receive(v_copies, v_mid, v_from_left, v_from_right, (vf, vf_low), meet_and_greet, 2, 10)
    smooth_pieces = []

    def image(keep, kept):
        smooth_pieces.append(smooth(vf, keep, kept))
        return smooth_pieces[-1]

    stage(blurred, blur_back, second, [(72, 152, 72, 152)], image)
    stage(second, blur, blurred_second, [(96, 104, 104, 88)])
    kv1, kv2 = own(t1[pl.ds(96, 104), :], 96), own(t2[pl.ds(96, 104), :], 96)
    lv1, lv2 = own(jnp.concatenate(smooth_pieces, axis=0), 72), own(smooth(rf, 96, 104), 96)
    v2 = own(rf[pl.ds(96, 104), :], 96)

    def powers(zero, one, two):
        return two, one - two, zero - 2.0 * one + two

    r0, v1 = r0_own[...], v1_own[...]
    p = powers(r0, v1, v2)
    kp = powers(kr0_own[...], kv1, kv2)
    lp = powers(lr0_own[...], lv1, lv2)

    def lanes_of(x):
        total = x[0:8]
        for i in range(1, 8):
            total = total + x[8 * i : 8 * i + 8]
        total = total[:, :128] + total[:, 128:]
        return jnp.sum(total, axis=0, keepdims=True)

    moments = [lanes_of(p[2] * p[2])]
    for i, j in ((2, 2), (1, 2), (1, 1), (0, 1), (0, 0)):
        moments.append(lanes_of(kp[i] * kp[j] + p[i] * lp[j]))
    slot8 = iota((8, 128), 0)
    packed = jnp.zeros((8, 128), F32)
    for i, moment in enumerate(moments):
        packed = jnp.where(slot8 == i, moment, packed)
    mine = iota((8, 128), 1) == slot8
    packed = jnp.sum(packed, axis=1, keepdims=True)
    packed = jnp.sum(jnp.where(mine, packed, 0.0), axis=0, keepdims=True)

    meet(2)
    me = row * n_cols + col
    slots[me] = packed

    def hops(offset):
        z, y, x = offset[0] // 2, offset[1] // 4, offset[1] % 4
        return -(min(z, 4 - z) + min(y, 4 - y) + min(x, 4 - x))

    rows_at = [at(d, 0)[0] for d in range(n_rows)]
    cols_at = [at(0, d)[1] for d in range(n_cols)]
    offsets = [(dr, dc) for dr in range(n_rows) for dc in range(n_cols)][1:]
    for dr, dc in sorted(offsets, key=hops):
        remote(slots.at[me], slots.at[me], sum_send, sum_recv, (rows_at[dr], cols_at[dc])).start()
    others = pl.ds(0, n_rows * n_cols - 1)
    sums = remote(slots.at[others], slots.at[others], sum_send, sum_recv, at(1, 0))
    for copies in (x_copies, b_copies, v_copies):
        sent(copies)
    pl.when(exists(-1, 0))(far_copies[0].wait_send)
    pl.when(exists(1, 0))(far_copies[1].wait_send)
    pl.when(exists(1, 0))(far_copies[0].wait_recv)
    pl.when(exists(-1, 0))(far_copies[1].wait_recv)
    unpack_middle(v_mid, (vf, vf_low), masked, (0, 11))
    stage((vf, vf_low), blur, blurred, [(24, 40, 24, 32), (232, 40, 240, 32)])
    stage(blurred, blur_back, second, [(48, 40, 48, 32), (208, 40, 216, 32)], image)
    stage(second, blur, blurred_second, [(72, 40, 72, 32), (184, 40, 192, 32)])
    v3 = own(correlate((t2, t2_low), kt_high, kt_low, 96, 104), 96) + lv2
    for number, value in enumerate(p + powers(v1, v2, v3)):
        pixels[number] = swap_blocks(value)
    sums.wait_recv()
    groups = [jnp.sum(slots[pl.ds(start, n_cols)], axis=0) for start in range(0, n_rows * n_cols, n_cols)]
    while len(groups) > 1:
        groups = [sum(groups[i : i + 2][1:], groups[i]) for i in range(0, len(groups), 2)]
    total = groups[0]
    total = jnp.sum(jnp.where(mine, jnp.broadcast_to(total, (8, 128)), 0.0), axis=1, keepdims=True)
    b0, c1, c2, c3, c4, c5 = [total[i : i + 1, :] for i in range(6)]
    c = (None, c1, c2, c3, c4, c5)
    b = (b0, c1 + c2, c2 + c3, c3 + c4, c4 + c5)

    def square(q, m, base):
        return (
            q[0] * q[0] * m[base]
            + 2.0 * (q[0] * q[1]) * m[base + 1]
            + (q[1] * q[1] + 2.0 * (q[0] * q[2])) * m[base + 2]
            + 2.0 * (q[1] * q[2]) * m[base + 3]
            + q[2] * q[2] * m[base + 4]
        )

    def raised(q):
        return q[0], q[0] + q[1], q[1]

    one = (1.0, 2.0, 1.0)
    norm = square(one, b, 0)
    alpha0 = norm / square(one, c, 1)
    r1 = (1.0, 1.0 - alpha0)
    following = square(raised(r1), b, 0)
    beta0 = following / norm
    norm = following
    p1 = (r1[0] + beta0, r1[1] + beta0)
    p1_raised = raised(p1)
    alpha1 = norm / square(p1_raised, c, 1)
    r1_raised = raised(r1)
    r2 = (r1_raised[0], r1_raised[1] - alpha1 * p1[0], r1_raised[2] - alpha1 * p1[1])
    following = square(r2, b, 0)
    beta1 = following / norm
    p2 = tuple(r2[i] + beta1 * p1_raised[i] for i in range(3))
    alpha2 = following / square(p2, c, 1)
    steps = [alpha0 * one[i] + alpha1 * p1_raised[i] + alpha2 * p2[i] for i in range(3)]

    f0, f1, f2, af0, af1, af2 = [pixels[number] for number in range(6)]
    template_ref[...] = guess_tile[...] + steps[0] * f2 + steps[1] * f1 + steps[2] * f0
    residual = r2[0] * f2 + r2[1] * f1 + r2[2] * f0
    residual_ref[...] = residual - alpha2 * (p2[0] * af2 + p2[1] * af1 + p2[2] * af0)
    sums.wait_send()


def on_device(grid, right_side, initial_guess, kernel):
    n_rows, n_cols = grid
    middle = pltpu.VMEM((12, 16, LANES), F32)
    b_middle = pltpu.VMEM((8, 16, LANES), F32)
    side = pltpu.VMEM((2, 8, LANES), F32)
    halo = pltpu.VMEM((6, 8, LANES), F32)
    b_side = pltpu.VMEM((8, LANES), F32)
    b_halo = pltpu.VMEM((3, 8, LANES), F32)
    flat = pltpu.VMEM((FLAT, LANES), F32)
    weight = pltpu.VMEM((3 * LANES, 3 * LANES), BF16)
    tile = pltpu.VMEM((64, LANES), F32)
    dma = pltpu.SemaphoreType.DMA
    shape = jax.ShapeDtypeStruct((64, LANES), F32)
    vmem = pl.BlockSpec(memory_space=pltpu.VMEM)

    def body(*refs):
        image_kernel(grid, *refs)

    results = pl.pallas_call(
        body,
        out_shape=(shape, shape),
        in_specs=[pl.BlockSpec(memory_space=pltpu.HBM)] * 3,
        out_specs=(vmem, vmem),
        scratch_shapes=[
            middle, middle, b_middle, side, side, side, side, b_side, b_side,
            halo, halo, halo, halo, b_halo, b_halo,
            flat, flat, flat, flat, flat, flat, flat, flat, flat, flat, flat, flat, flat, flat, flat,
            pltpu.VMEM((128, 128), F32), pltpu.VMEM((8, 96, 1024), BF16),
            weight, weight, weight, weight,
            tile, tile, tile, tile, tile, tile,
            pltpu.VMEM((n_rows * n_cols, 1, 128), F32), pltpu.VMEM((6, 64, LANES), F32), pltpu.SemaphoreType.REGULAR((3,)), tile, tile, pltpu.VMEM((31, 31), F32), dma((3,)),
            dma((8,)), dma((8,)), dma((8,)), dma((8,)), dma((10,)), dma((10,)),
            dma, dma,
        ],
        compiler_params=pltpu.CompilerParams(
            collective_id=0, has_side_effects=True, vmem_limit_bytes=16 * 1024 * 1024
        ),
    )(*(pltpu.with_memory_space_constraint(x, pltpu.HBM) for x in (right_side, initial_guess, kernel)))

    def store(template_ref, residual_ref, template_out, residual_out, sems):
        copies = (
            pltpu.make_async_copy(template_ref, template_out, sems.at[0]),
            pltpu.make_async_copy(residual_ref, residual_out, sems.at[1]),
        )
        for copy in copies:
            copy.start()
        for copy in copies:
            copy.wait()

    return pl.pallas_call(
        store,
        out_shape=(shape, shape),
        in_specs=[vmem] * 2,
        out_specs=(pl.BlockSpec(memory_space=pltpu.HBM),) * 2,
        scratch_shapes=[dma((2,))],
        compiler_params=pltpu.CompilerParams(vmem_limit_bytes=1024 * 1024),
    )(*results)


def solution(mesh):
    grid = (mesh.shape["row"], mesh.shape["col"])
    tiles = P("row", "col")
    return jax.shard_map(
        lambda *arrays: on_device(grid, *arrays),
        mesh=mesh,
        in_specs=(tiles, tiles, P()),
        out_specs=(tiles, tiles),
        check_vma=False,
    )
```
